128 devices in a mesh: gx: 8 (over z, core), gy: 16 (over y, x).
Axes of the slice: x: 4, y: 4, z: 4, core: 2. Of those that a mesh axis runs over, the one named last changes fastest.
Arguments:
- matrix_rows: float32 [16384, 1024], P(('gx', 'gy')), may hold values from -1.1 to 1.1
- tile_owner: int32 [2080], replicated, may hold values from 0 to 127, as said below
- tile_slot: int32 [2080], replicated, may hold values from 0 to 16, as said below
Outputs:
- packed_tiles: float32 [2176, 256, 256], P(('gx', 'gy'))
The draws below stay inside these ranges and needn't reach their ends.
Inputs may be any that keep to these rules, and one draw needn't show every extreme that they name: `tile_owner`: give tile (I, J) the class (c, r) as follows, with a = I // 8, b = J // 8, i = I % 8, j = J % 8: if a == b, c = a and r = i when i - j < 4, else r = j; if a > b and (a - b > 4, or a - b == 4 with i + j even), c = b and r = i; otherwise c = a and r = j. The owner of a class (c, r) tile is one of the devices c * 16 to c * 16 + 15. Every owner holds 16 or 17 tiles. At most 3 tiles of one class share an owner, and in every draw some owner holds exactly 3 tiles of one class. `tile_slot`: the tiles of one owner take the slots 0 to their count - 1, each once.
All inputs are finite; a program needn't handle non-finite values.
Results may differ from the reference program's by a relative error of at most 0.0003.
Values sent between devices are 32-bit elements; how exact they have to be, the bound alone decides.
A program may use at most 128 MiB of HBM per device.

```python
import jax
import jax.numpy as jnp
import numpy as np
from jax import lax

WIDTH = 1024
TILE = 256
ORDER = 16384
TILE_COUNT = 64
HALF_TILES = 8
LOWER_COUNT = 2080
SLOTS = 17
N_GX = 8
N_GY = 16
DEVICES = 128


def tile_classes():
    lower_i, lower_j = np.tril_indices(TILE_COUNT)
    group_a = lower_i // HALF_TILES
    group_b = lower_j // HALF_TILES
    inner_i = lower_i % HALF_TILES
    inner_j = lower_j % HALF_TILES
    same = group_a == group_b
    within_row = inner_i - inner_j < HALF_TILES // 2
    gap = group_a - group_b
    across_row = (gap > N_GX // 2) | (gap == N_GX // 2) & ((inner_i + inner_j) % 2 == 0)
    rowwise = np.where(same, within_row, across_row)
    class_x = np.where(same | ~rowwise, group_a, group_b)
    class_r = np.where(rowwise, inner_i, inner_j)
    return (class_x.astype(np.int32), class_r.astype(np.int32))


def owner_table(key):
    class_x, class_r = tile_classes()
    set_id = jnp.asarray(class_x * HALF_TILES + class_r, jnp.int32)
    row_of = jnp.asarray(class_x, jnp.int32)
    set_rank = jax.random.permutation(jax.random.fold_in(key, 11), TILE_COUNT).astype(jnp.int32)
    tile_rank = jax.random.permutation(jax.random.fold_in(key, 12), LOWER_COUNT).astype(jnp.int32)
    score = (row_of * TILE_COUNT + set_rank[set_id]) * LOWER_COUNT + tile_rank
    order = jnp.argsort(score, stable=True).astype(jnp.int32)
    position = jnp.zeros((LOWER_COUNT,), jnp.int32).at[order].set(jnp.arange(LOWER_COUNT, dtype=jnp.int32))
    per_row = LOWER_COUNT // N_GX
    inside_row = position % per_row
    row_keys = jax.random.split(jax.random.fold_in(key, 13), N_GX)
    owner_order = jax.vmap(lambda one: jax.random.permutation(one, N_GY))(row_keys).astype(jnp.int32)
    owners = row_of * N_GY + owner_order[row_of, inside_row % N_GY]
    slot_index = inside_row // N_GY
    return (owners.astype(jnp.int32), slot_index.astype(jnp.int32))


def draw_tile_owner(key, part):
    return owner_table(key)[0]


def draw_tile_slot(key, part):
    return owner_table(key)[1]


def shard_levels(own_key, dims, shards, smallest, largest):
    def one(dim, shards_of):
        heights = jax.random.uniform(jax.random.fold_in(jax.random.fold_in(own_key, 6), dim), (shards_of,), jnp.float32, smallest / len(shards), largest / len(shards))
        return jnp.repeat(jnp.exp(heights), dims[dim] // shards_of).reshape((-1,) + (1,) * (len(dims) - dim - 1))

    level = one(*shards[0])
    for cut in shards[1:]:
        level = level * one(*cut)
    return level


def normal_values(stream_key, extent, width, limit, pieces=(), kind=jnp.bfloat16):
    gain = shard_levels(stream_key, extent, pieces, -0.22, 0.18) if pieces else 1.0
    values = jax.random.normal(stream_key, extent, jnp.float32) * width * gain
    return jnp.minimum(jnp.maximum(values, -limit), limit).astype(kind)


def setup_inputs(seed: int = 0) -> dict:
    splits = jax.random.split(jax.random.key(seed), 4)
    matrix_rows = normal_values(splits[0], (ORDER, WIDTH), 0.177, 1.1, ((0, 128),), jnp.float32)
    tile_owner = draw_tile_owner(jax.random.fold_in(splits[3], 71), 0)
    tile_slot = draw_tile_slot(jax.random.fold_in(splits[3], 71), 0)
    return dict(matrix_rows=matrix_rows, tile_owner=tile_owner, tile_slot=tile_slot)


def reference(matrix_rows, tile_owner, tile_slot):
    lower_i, lower_j = np.tril_indices(TILE_COUNT)
    row_table = jnp.asarray(lower_i, jnp.int32)
    col_table = jnp.asarray(lower_j, jnp.int32)
    blocks = matrix_rows.reshape(TILE_COUNT, TILE, WIDTH)
    inside = lax.broadcasted_iota(jnp.int32, (TILE, TILE), 0)
    across = lax.broadcasted_iota(jnp.int32, (TILE, TILE), 1)

    def one_tile(index):
        row_tile = row_table[index]
        col_tile = col_table[index]
        product = lax.dot_general(blocks[row_tile], blocks[col_tile], (((1,), (1,)), ((), ())),
                                  precision=lax.Precision.HIGHEST, preferred_element_type=jnp.float32)
        upper = jnp.logical_and(row_tile == col_tile, inside < across)
        return jnp.where(upper, jnp.float32(0.0), product)

    tiles = lax.map(one_tile, jnp.arange(LOWER_COUNT, dtype=jnp.int32))
    packed = jnp.zeros((DEVICES, SLOTS, TILE, TILE), jnp.float32)
    packed = packed.at[tile_owner, tile_slot].set(tiles)
    return packed.reshape(DEVICES * SLOTS, TILE, TILE)
```

```python
import functools

import jax
import jax.numpy as jnp
import numpy as np
from jax import lax
from jax.experimental import pallas as pl
from jax.experimental.pallas import tpu as pltpu
from jax.sharding import PartitionSpec as P

MESH = pl.DeviceIdType.MESH
SIDE = 4
PLANE = SIDE * SIDE
GROUPS = 8
HALF_TILES = 8
STEPS = 5
CAP = 3
CHUNK = 128
TILE = 256
TILE_COUNT = 64


def exchange_kernel(
    step_tab, col_tab, diag_tab, a_ref, in_ref,
    g, ghi, glo, rf, rhi, rlo, outs,
    a1_send, a1_recv, a2_send, a2_recv, b1_send, b1_recv, b2_send, b2_recv,
    z_send, z_recv, p_send, p_recv, x_send, x_recv, l_sem,
):
    gx = lax.axis_index("gx")
    gy = lax.axis_index("gy")
    core = gx % 2
    y = gy // SIDE
    x = gy % SIDE
    u = jnp.where(core == 0, x, y)
    v = jnp.where(core == 0, y, x)
    stride_u = jnp.where(core == 0, 1, SIDE)
    stride_v = jnp.where(core == 0, SIDE, 1)

    def at(du, dv):
        return (u + du + SIDE) % SIDE * stride_u + (v + dv + SIDE) % SIDE * stride_v

    ahead = (gx + 2) % GROUPS
    behind = (gx + 6) % GROUPS
    partner = gx + 1 - 2 * core

    barrier = pltpu.get_barrier_semaphore()

    def greet(i, carry):
        pl.semaphore_signal(
            barrier, inc=1, device_id={"gx": gx, "gy": (gy + i) % PLANE}, device_id_type=MESH
        )
        return carry

    lax.fori_loop(1, PLANE, greet, 0)
    for other in (ahead, behind, partner):
        pl.semaphore_signal(barrier, inc=1, device_id={"gx": other, "gy": gy}, device_id_type=MESH)
    pl.semaphore_wait(barrier, PLANE + 2)

    def whole(c):
        return g.at[c // 2, pl.ds(pl.multiple_of(c % 2 * CHUNK, CHUNK), CHUNK)]

    def half(c, h):
        start = pl.multiple_of(c % 2 * CHUNK + h * (CHUNK // 2), CHUNK // 2)
        return g.at[c // 2, pl.ds(start, CHUNK // 2)]

    def remote(src, dst, send, recv, to_gx, to_gy):
        return pltpu.make_async_remote_copy(
            src_ref=src, dst_ref=dst, send_sem=send, recv_sem=recv,
            device_id={"gx": to_gx, "gy": to_gy}, device_id_type=MESH,
        )

    me = gy
    a1 = [remote(a_ref, whole(me), a1_send.at[d], a1_recv.at[d], gx, at(1 - 2 * d, 0)) for d in (0, 1)]
    z1 = remote(a_ref, rf.at[1], z_send.at[0], z_recv.at[0], ahead, gy)
    offs = (0, -1, 1, 2)
    b1 = []
    for n, du in enumerate(offs):
        src = a_ref if n == 0 else whole(at(du, 0))
        b1.append([
            remote(src, whole(at(du, 0)), b1_send.at[n, d], b1_recv.at[n, d], gx, at(0, 1 - 2 * d))
            for d in (0, 1)
        ])
    a1[0].start()
    a1[1].start()
    b1[0][0].start()
    b1[0][1].start()
    z1.start()

    def split_g(c):
        block = c // 2
        rows = pl.ds(pl.multiple_of(c % 2 * CHUNK, CHUNK), CHUNK)
        value = g[block, rows, :]
        high = value.astype(jnp.bfloat16)
        ghi[block, rows, :] = high
        glo[block, rows, :] = (value - high.astype(jnp.float32)).astype(jnp.bfloat16)

    def split_r(n, value):
        high = value.astype(jnp.bfloat16)
        rhi[n] = high
        rlo[n] = (value - high.astype(jnp.float32)).astype(jnp.bfloat16)

    own = a_ref[...]
    split_r(0, own)
    block, rows = me // 2, pl.ds(pl.multiple_of(me % 2 * CHUNK, CHUNK), CHUNK)
    ghi[block, rows, :] = rhi[0]
    glo[block, rows, :] = rlo[0]

    a2 = []
    for d in (0, 1):
        src_c = at(-1 + 2 * d, 0)
        a1[d].wait_recv()
        copy = remote(half(src_c, d), half(src_c, d), a2_send.at[d], a2_recv.at[d], gx, at(1 - 2 * d, 0))
        copy.start()
        a2.append(copy)
        b1[1 + d][0].start()
        b1[1 + d][1].start()
        split_g(src_c)

    z1.wait_recv()
    z2 = remote(rf.at[1], rf.at[3], z_send.at[1], z_recv.at[1], ahead, gy)
    z2.start()

    b2 = []

    def forward_v(n):
        for d in (0, 1):
            c = at(offs[n], -1 + 2 * d)
            b1[n][d].wait_recv()
            copy = remote(half(c, d), half(c, d), b2_send.at[n, d], b2_recv.at[n, d], gx, at(0, 1 - 2 * d))
            copy.start()
            b2.append(copy)
            split_g(c)

    forward_v(0)
    for d in (0, 1):
        a2[d].wait_recv()
    b1[3][0].start()
    b1[3][1].start()
    split_g(at(2, 0))

    @pl.when(core == 0)
    def _():
        remote(a_ref, rf.at[0], p_send.at[0], p_recv.at[0], partner, gy).start()

    @pl.when(core == 1)
    def _():
        remote(rf.at[1], rf.at[0], p_send.at[0], p_recv.at[0], partner, gy).start()

    split_r(2, rf[1])
    forward_v(1)
    z2.wait_recv()

    @pl.when(core == 0)
    def _():
        remote(rf.at[1], rf.at[2], p_send.at[1], p_recv.at[1], partner, gy).start()

    @pl.when(core == 1)
    def _():
        remote(rf.at[3], rf.at[2], p_send.at[1], p_recv.at[1], partner, gy).start()

    split_r(4, rf[3])
    forward_v(2)
    p1 = remote(a_ref, rf.at[0], p_send.at[0], p_recv.at[0], partner, gy)
    p2 = remote(a_ref, rf.at[2], p_send.at[1], p_recv.at[1], partner, gy)
    p1.wait_recv()
    split_r(1, rf[0])
    p2.wait_recv()
    split_r(3, rf[2])
    forward_v(3)
    for n in range(4):
        for d in (0, 1):
            b2[2 * n + d].wait_recv()
        split_g(at(offs[n], 2))

    row_in = lax.broadcasted_iota(jnp.int32, (CHUNK, TILE), 0) + gy % 2 * CHUNK
    col_in = lax.broadcasted_iota(jnp.int32, (CHUNK, TILE), 1)
    upper = row_in < col_in

    def dot(p, q):
        return lax.dot_general(p, q, (((1,), (1,)), ((), ())), preferred_element_type=jnp.float32)

    def one_owner(i, carry):
        order = (PLANE // 2 + 1 + i) % PLANE
        to = (gy + order) % PLANE

        def one_slot(k, inner):
            entry = to * CAP + k
            s = step_tab[entry]
            j = col_tab[entry]
            rh = rhi[s]
            gh = ghi[j]
            value = dot(rh, gh) + dot(rh, glo[j]) + dot(rlo[s], gh)
            masked = jnp.logical_and(upper, diag_tab[entry] > 0)
            outs[order, k] = jnp.where(masked, jnp.float32(0.0), value)
            return inner

        lax.fori_loop(0, CAP, one_slot, 0)

        @pl.when(order > 0)
        def _():
            remote(outs.at[order], in_ref.at[gy], x_send.at[order], x_recv.at[order], gx, to).start()

        return carry

    lax.fori_loop(0, PLANE, one_owner, 0)
    local = pltpu.make_async_copy(outs.at[0], in_ref.at[gy], l_sem)
    local.start()

    for copy in a1 + a2 + b2 + [z1, z2, p1, p2] + [c for pair in b1 for c in pair]:
        copy.wait_send()
    local.wait()

    def finish(i, carry):
        source = (gy + PLANE - i) % PLANE
        copy = remote(outs.at[i], in_ref.at[source], x_send.at[i], x_recv.at[i], gx, (gy + i) % PLANE)
        copy.wait_send()
        copy.wait_recv()
        return carry

    lax.fori_loop(1, PLANE, finish, 0)


def exchange(matrix_rows, step_tab, col_tab, diag_tab):
    width = matrix_rows.shape[1]
    smem = pl.BlockSpec(memory_space=pltpu.SMEM)
    dma = pltpu.SemaphoreType.DMA
    return pl.pallas_call(
        exchange_kernel,
        out_shape=jax.ShapeDtypeStruct((PLANE, CAP, CHUNK, TILE), jnp.float32),
        in_specs=[smem, smem, smem, pl.BlockSpec(memory_space=pltpu.VMEM)],
        out_specs=pl.BlockSpec(memory_space=pl.ANY),
        scratch_shapes=[
            pltpu.VMEM((HALF_TILES, TILE, width), jnp.float32),
            pltpu.VMEM((HALF_TILES, TILE, width), jnp.bfloat16),
            pltpu.VMEM((HALF_TILES, TILE, width), jnp.bfloat16),
            pltpu.VMEM((4, CHUNK, width), jnp.float32),
            pltpu.VMEM((STEPS, CHUNK, width), jnp.bfloat16),
            pltpu.VMEM((STEPS, CHUNK, width), jnp.bfloat16),
            pltpu.VMEM((PLANE, CAP, CHUNK, TILE), jnp.float32),
            dma((2,)), dma((2,)), dma((2,)), dma((2,)),
            dma((4, 2)), dma((4, 2)), dma((4, 2)), dma((4, 2)),
            dma((2,)), dma((2,)), dma((2,)), dma((2,)),
            dma((PLANE,)), dma((PLANE,)), dma(()),
        ],
        compiler_params=pltpu.CompilerParams(
            collective_id=0, has_side_effects=True, vmem_limit_bytes=48 * 1024 * 1024
        ),
        name="exchange",
    )(step_tab, col_tab, diag_tab, matrix_rows)


def assemble_kernel(src_tab, rank_tab, kind_tab, upper_ref, lower_ref, out_ref):
    kind = kind_tab[pl.program_id(0)]

    @pl.when(kind == 0)
    def _():
        out_ref[...] = jnp.zeros_like(out_ref)

    @pl.when(kind == 1)
    def _():
        out_ref[0, :CHUNK, :] = upper_ref[0, 0]
        out_ref[0, CHUNK:, :] = lower_ref[0, 0]

    @pl.when(kind == 2)
    def _():
        out_ref[0, :, :CHUNK] = upper_ref[0, 0].T
        out_ref[0, :, CHUNK:] = lower_ref[0, 0].T


def assemble(incoming, class_r, rank, kind):
    slots = class_r.shape[0]

    def piece(h):
        return pl.BlockSpec(
            (1, 1, CHUNK, TILE), lambda q, src, rk, kd: (2 * src[q] + h, rk[q], 0, 0)
        )

    return pl.pallas_call(
        assemble_kernel,
        out_shape=jax.ShapeDtypeStruct((slots, TILE, TILE), jnp.float32),
        grid_spec=pltpu.PrefetchScalarGridSpec(
            num_scalar_prefetch=3,
            grid=(slots,),
            in_specs=[piece(0), piece(1)],
            out_specs=pl.BlockSpec((1, TILE, TILE), lambda q, src, rk, kd: (q, 0, 0)),
        ),
        name="assemble",
    )(class_r, rank, kind, incoming, incoming)


def send_tables(x_index, y_index, tile_owner):
    own_r = y_index // 2
    quarter = HALF_TILES // 2
    middle = GROUPS // 2 - 1
    offsets = jnp.arange(quarter + 1, dtype=jnp.int32)
    first_cols = (own_r - offsets) % HALF_TILES
    first_valid = jnp.logical_or(offsets < quarter, own_r < quarter)
    flag = (x_index >= GROUPS // 2).astype(jnp.int32)
    last_cols = 2 * jnp.arange(quarter, dtype=jnp.int32) + (own_r + flag) % 2
    middle_cols = jnp.asarray(np.tile(np.arange(HALF_TILES, dtype=np.int32), middle))
    col_of = jnp.concatenate([first_cols, middle_cols, last_cols])
    valid = jnp.concatenate([first_valid, jnp.ones((middle * HALF_TILES + quarter,), bool)])
    step_of = jnp.asarray(np.concatenate([
        np.zeros(quarter + 1, np.int32),
        np.repeat(np.arange(1, middle + 1, dtype=np.int32), HALF_TILES),
        np.full(quarter, middle + 1, np.int32),
    ]))
    source_x = (x_index - step_of) % GROUPS
    rowwise = jnp.where(step_of == 0, col_of <= own_r, source_x > x_index)
    near = source_x * HALF_TILES + own_r
    far = x_index * HALF_TILES + col_of
    row_tile = jnp.where(rowwise, near, far)
    col_tile = jnp.where(rowwise, far, near)
    tile_index = jnp.where(valid, row_tile * (row_tile + 1) // 2 + col_tile, 0)
    target = jnp.where(valid, tile_owner[tile_index] % PLANE, PLANE)
    earlier = (target[:, None] == target[None, :]) & (tile_index[None, :] < tile_index[:, None])
    earlier = earlier & valid[None, :]
    rank = jnp.sum(earlier.astype(jnp.int32), axis=1)
    place = jnp.where(valid, target * CAP + rank, PLANE * CAP)
    hit = place[None, :] == jnp.arange(PLANE * CAP, dtype=jnp.int32)[:, None]
    packed = step_of * 16 + col_of * 2 + (row_tile == col_tile).astype(jnp.int32)
    chosen = jnp.sum(jnp.where(hit, packed[None, :], 0), axis=1)
    return chosen // 16, chosen // 2 % HALF_TILES, chosen % 2


def receive_tables(my_index, slot_count, tile_owner, tile_slot):
    lower_i, lower_j = np.tril_indices(TILE_COUNT)
    code = jnp.asarray(lower_i * TILE_COUNT + lower_j, jnp.int32)
    wanted = jnp.arange(slot_count, dtype=jnp.int32)
    hit = (tile_owner == my_index)[None, :] & (tile_slot[None, :] == wanted[:, None])
    found = jnp.max(jnp.where(hit, code[None, :], -1), axis=1)
    present = found >= 0
    clipped = jnp.maximum(found, 0)
    row_tile = clipped // TILE_COUNT
    col_tile = clipped % TILE_COUNT
    group_a = row_tile // HALF_TILES
    group_b = col_tile // HALF_TILES
    inner_i = row_tile % HALF_TILES
    inner_j = col_tile % HALF_TILES
    gap = group_a - group_b
    across = (gap > GROUPS // 2) | ((gap == GROUPS // 2) & ((inner_i + inner_j) % 2 == 0))
    rowwise = jnp.where(gap == 0, inner_i - inner_j < HALF_TILES // 2, across)
    class_r = jnp.where(rowwise, inner_i, inner_j)
    before = (class_r[:, None] == class_r[None, :]) & (clipped[None, :] < clipped[:, None])
    before = before & present[None, :]
    rank = jnp.minimum(jnp.sum(before.astype(jnp.int32), axis=1), CAP - 1)
    kind = jnp.where(present, jnp.where(rowwise, 1, 2), 0)
    return class_r, rank, kind


def per_device(matrix_rows, tile_owner, tile_slot):
    x_index = lax.axis_index("gx")
    y_index = lax.axis_index("gy")
    devices = GROUPS * PLANE
    slot_count = (tile_owner.shape[0] + devices - 1) // devices
    step_tab, col_tab, diag_tab = send_tables(x_index, y_index, tile_owner)
    class_r, rank, kind = receive_tables(x_index * PLANE + y_index, slot_count, tile_owner, tile_slot)
    incoming = exchange(matrix_rows, step_tab, col_tab, diag_tab)
    return assemble(incoming, class_r, rank, kind)


def solution(mesh):
    placed = (P(("gx", "gy"), None), P(), P())
    return jax.shard_map(
        per_device,
        mesh=mesh,
        in_specs=placed,
        out_specs=P(("gx", "gy"), None, None),
        check_vma=False,
    )
```

```python
import jax
import jax.numpy as jnp
import numpy as np
from jax import lax
from jax.experimental import pallas as pl
from jax.experimental.pallas import tpu as pltpu
from jax.sharding import PartitionSpec as P

MESH = pl.DeviceIdType.MESH
SIDE = 4
PLANE = SIDE * SIDE
GROUPS = 8
HALF_TILES = 8
STEPS = 5
CAP = 3
CHUNK = 128
HALF = CHUNK // 2
TILE = 256
TILE_COUNT = 64
ENTRIES = 33
ORDER = (
    (2, 2), (1, 0), (3, 0), (0, 2), (1, 1), (3, 3), (2, 0), (0, 1),
    (0, 3), (1, 2), (3, 2), (1, 3), (3, 1), (2, 1), (2, 3), (0, 0),
)


def entry_of(e, gx, r):
    quarter = HALF_TILES // 2
    middle = GROUPS // 2 - 1
    if e <= quarter:
        s, col = 0, (r - e + HALF_TILES) % HALF_TILES
        valid = r < quarter if e == quarter else None
        rowwise = col <= r
        source = gx
    elif e <= quarter + middle * HALF_TILES:
        s, col = 1 + (e - quarter - 1) // HALF_TILES, (e - quarter - 1) % HALF_TILES
        valid = None
        source = (gx - s + GROUPS) % GROUPS
        rowwise = source > gx
    else:
        s = middle + 1
        last = e - quarter - 1 - middle * HALF_TILES
        col = 2 * last + (r + jnp.where(gx >= GROUPS // 2, 1, 0)) % 2
        valid = None
        source = (gx - s + GROUPS) % GROUPS
        rowwise = source > gx
    near = source * HALF_TILES + r
    far = gx * HALF_TILES + col
    row_tile = jnp.where(rowwise, near, far)
    col_tile = jnp.where(rowwise, far, near)
    return s, col, valid, rowwise, row_tile, col_tile


def exchange_kernel(
    owner_smem, owner_ref, slot_ref, code_ref, a_ref, in_ref, table_ref,
    g, ghi, glo, rf, rhi, rlo, outs, target_tab, entry_tab, send_tab, found_tab,
    a1_send, a1_recv, a2_send, a2_recv, b1_send, b1_recv, b2_send, b2_recv,
    z_send, z_recv, p_send, p_recv, x_send, x_recv, l_sem,
):
    gx = lax.axis_index("gx")
    gy = lax.axis_index("gy")
    core = gx % 2
    y = gy // SIDE
    x = gy % SIDE
    u = jnp.where(core == 0, x, y)
    v = jnp.where(core == 0, y, x)
    stride_u = jnp.where(core == 0, 1, SIDE)
    stride_v = jnp.where(core == 0, SIDE, 1)

    def at(du, dv):
        return (u + du + SIDE) % SIDE * stride_u + (v + dv + SIDE) % SIDE * stride_v

    ahead = (gx + 2) % GROUPS
    behind = (gx + 6) % GROUPS
    partner = gx + 1 - 2 * core

    barrier = pltpu.get_barrier_semaphore()

    def greet(i, carry):
        pl.semaphore_signal(
            barrier, inc=1, device_id={"gx": gx, "gy": (gy + i) % PLANE}, device_id_type=MESH
        )
        return carry

    lax.fori_loop(1, PLANE, greet, 0)
    for other in (ahead, behind, partner):
        pl.semaphore_signal(barrier, inc=1, device_id={"gx": other, "gy": gy}, device_id_type=MESH)
    pl.semaphore_wait(barrier, PLANE + 2)

    def half(c, h):
        start = pl.multiple_of(c % 2 * CHUNK + h * HALF, HALF)
        return g.at[c // 2, pl.ds(start, HALF)]

    def own_half(h):
        return a_ref.at[pl.ds(h * HALF, HALF)]

    def remote(src, dst, send, recv, to_gx, to_gy):
        return pltpu.make_async_remote_copy(
            src_ref=src, dst_ref=dst, send_sem=send, recv_sem=recv,
            device_id={"gx": to_gx, "gy": to_gy}, device_id_type=MESH,
        )

    copies = []

    def start(copy):
        copy.start()
        copies.append(copy)

    me = gy
    a1 = [[
        remote(own_half(h), half(me, h), a1_send.at[d, p], a1_recv.at[d, p], gx, at(1 - 2 * d, 0))
        for p, h in enumerate((d, 1 - d))
    ] for d in (0, 1)]
    a2 = [
        remote(
            half(at(-1 + 2 * d, 0), d), half(at(-1 + 2 * d, 0), d),
            a2_send.at[d], a2_recv.at[d], gx, at(1 - 2 * d, 0),
        )
        for d in (0, 1)
    ]
    offs = (0, -1, 1, 2)
    b1 = [[[
        remote(
            own_half(h) if n == 0 else half(at(du, 0), h), half(at(du, 0), h),
            b1_send.at[n, d, p], b1_recv.at[n, d, p], gx, at(0, 1 - 2 * d),
        )
        for p, h in enumerate((d, 1 - d))
    ] for d in (0, 1)] for n, du in enumerate(offs)]
    b2 = [[
        remote(
            half(at(du, -1 + 2 * d), d), half(at(du, -1 + 2 * d), d),
            b2_send.at[n, d], b2_recv.at[n, d], gx, at(0, 1 - 2 * d),
        )
        for d in (0, 1)
    ] for n, du in enumerate(offs)]
    z1 = remote(a_ref, rf.at[1], z_send.at[0], z_recv.at[0], ahead, gy)
    z2 = remote(rf.at[1], rf.at[3], z_send.at[1], z_recv.at[1], ahead, gy)
    for p in (0, 1):
        for d in (0, 1):
            start(a1[d][p])
    start(z1)
    for p in (0, 1):
        for d in (0, 1):
            start(b1[0][d][p])

    def split_g(c):
        block = c // 2
        rows = pl.ds(pl.multiple_of(c % 2 * CHUNK, CHUNK), CHUNK)
        value = g[block, rows, :]
        high = value.astype(jnp.bfloat16)
        ghi[block, rows, :] = high
        glo[block, rows, :] = (value - high.astype(jnp.float32)).astype(jnp.bfloat16)

    def split_r(n, value):
        high = value.astype(jnp.bfloat16)
        rhi[n] = high
        rlo[n] = (value - high.astype(jnp.float32)).astype(jnp.bfloat16)

    own_r = gy // 2
    for e in range(ENTRIES):
        s, col, valid, rowwise, row_tile, col_tile = entry_of(e, gx, own_r)
        owner = owner_smem[row_tile * (row_tile + 1) // 2 + col_tile] % PLANE
        target_tab[e] = owner if valid is None else jnp.where(valid, owner, -1)
        diag = jnp.where(row_tile == col_tile, 2, 0)
        entry_tab[e] = s * 32 + col * 4 + diag + jnp.where(rowwise, 1, 0)

    def fill(to, carry):
        kept = [jnp.int32(0)] * CAP
        for e in range(ENTRIES):
            hit = target_tab[e] == to
            fresh = entry_tab[e]
            kept = [jnp.where(hit, b, a) for a, b in zip(kept, [fresh] + kept[:-1])]
        for k in range(CAP):
            send_tab[to * CAP + k] = kept[k]
        return carry

    lax.fori_loop(0, PLANE, fill, 0)

    split_r(0, a_ref[...])
    block, rows = me // 2, pl.ds(pl.multiple_of(me % 2 * CHUNK, CHUNK), CHUNK)
    ghi[block, rows, :] = rhi[0]
    glo[block, rows, :] = rlo[0]

    for d in (0, 1):
        a1[d][0].wait_recv()
        start(a2[d])
    for d in (0, 1):
        a1[d][1].wait_recv()
        for p in (0, 1):
            for e in (0, 1):
                start(b1[1 + d][e][p])
        split_g(at(-1 + 2 * d, 0))

    z1.wait_recv()
    start(z2)

    def forward_v(n):
        for d in (0, 1):
            b1[n][d][0].wait_recv()
            start(b2[n][d])

    def take_v(n):
        for d in (0, 1):
            b1[n][d][1].wait_recv()
            split_g(at(offs[n], -1 + 2 * d))

    mine = owner_ref[...] == gx * PLANE + gy
    slots = table_ref.shape[0]

    def find(q, carry):
        hit = jnp.logical_and(mine, slot_ref[...] == q)
        found = jnp.max(jnp.where(hit, code_ref[...], -1))
        row_tile = jnp.maximum(found, 0) // TILE_COUNT
        col_tile = jnp.maximum(found, 0) % TILE_COUNT
        group_a, inner_i = row_tile // HALF_TILES, row_tile % HALF_TILES
        group_b, inner_j = col_tile // HALF_TILES, col_tile % HALF_TILES
        gap = group_a - group_b
        even = (inner_i + inner_j) % 2 == 0
        across = jnp.logical_or(gap > GROUPS // 2, jnp.logical_and(gap == GROUPS // 2, even))
        within = inner_i - inner_j < HALF_TILES // 2
        rowwise = jnp.logical_or(jnp.logical_and(gap == 0, within), jnp.logical_and(gap > 0, across))
        class_r = jnp.where(rowwise, inner_i, inner_j)
        col = jnp.where(rowwise, inner_j, inner_i)
        s = (gx - jnp.where(rowwise, group_a, group_b) + GROUPS) % GROUPS
        place = s * HALF_TILES + jnp.where(s == 0, (class_r - col + HALF_TILES) % HALF_TILES, col)
        found_tab[q] = jnp.where(found >= 0, class_r * 64 + place, -1)
        table_ref[q] = jnp.where(found >= 0, jnp.where(rowwise, 1, 2), 0) + class_r * 4
        return carry

    lax.fori_loop(0, slots, find, 0)

    def count(q, carry):
        own = found_tab[q]
        later = jnp.int32(0)
        for other in range(slots):
            code = found_tab[other]
            same = jnp.logical_and(code // 64 == own // 64, code > own)
            later = later + jnp.where(same, 1, 0)
        table_ref[q] = table_ref[q] + 32 * jnp.minimum(later, CAP - 1)
        return carry

    forward_v(0)
    for d in (0, 1):
        a2[d].wait_recv()
        start(b1[3][d][0])
    for d in (0, 1):
        start(b1[3][d][1])
    split_g(at(2, 0))

    @pl.when(core == 0)
    def _():
        remote(a_ref, rf.at[0], p_send.at[0], p_recv.at[0], partner, gy).start()

    @pl.when(core == 1)
    def _():
        remote(rf.at[1], rf.at[0], p_send.at[0], p_recv.at[0], partner, gy).start()

    take_v(0)
    lax.fori_loop(0, slots, count, 0)
    split_r(2, rf[1])
    forward_v(1)
    z2.wait_recv()

    @pl.when(core == 0)
    def _():
        remote(rf.at[1], rf.at[2], p_send.at[1], p_recv.at[1], partner, gy).start()

    @pl.when(core == 1)
    def _():
        remote(rf.at[3], rf.at[2], p_send.at[1], p_recv.at[1], partner, gy).start()

    take_v(1)
    split_r(4, rf[3])
    forward_v(2)
    p1 = remote(a_ref, rf.at[0], p_send.at[0], p_recv.at[0], partner, gy)
    p2 = remote(a_ref, rf.at[2], p_send.at[1], p_recv.at[1], partner, gy)
    p1.wait_recv()
    split_r(1, rf[0])
    take_v(2)
    forward_v(3)
    p2.wait_recv()
    split_r(3, rf[2])
    take_v(3)
    for n in range(4):
        for d in (0, 1):
            b2[n][d].wait_recv()
        split_g(at(offs[n], 2))

    row_in = lax.broadcasted_iota(jnp.int32, (CHUNK, TILE), 0) + gy % 2 * CHUNK
    col_in = lax.broadcasted_iota(jnp.int32, (CHUNK, TILE), 1)
    upper = row_in < col_in

    def dot(p, q):
        return lax.dot_general(p, q, (((1,), (1,)), ((), ())), preferred_element_type=jnp.float32)

    def one_piece(i, carry):
        k = i // PLANE
        n = i % PLANE
        first = jnp.int32(0)
        second = jnp.int32(0)
        for m, (one, two) in enumerate(ORDER):
            first = jnp.where(n == m, one, first)
            second = jnp.where(n == m, two, second)
        dy = jnp.where(core == 0, first, second)
        dx = jnp.where(core == 0, second, first)
        to = (y + dy) % SIDE * SIDE + (x + dx) % SIDE
        order = dy * SIDE + dx
        entry = send_tab[to * CAP + k]
        s = entry // 32
        j = entry // 4 % HALF_TILES
        rh = rhi[s]
        gh = ghi[j]
        value = dot(rh, gh) + dot(rh, glo[j]) + dot(rlo[s], gh)
        masked = jnp.logical_and(upper, entry // 2 % 2 > 0)
        value = jnp.where(masked, jnp.float32(0.0), value)
        rowwise = jnp.full((CHUNK, CHUNK), entry % 2, jnp.int32) > 0
        for c in range(2):
            part = value[:, c * CHUNK:(c + 1) * CHUNK]
            outs[order, k, c] = jnp.where(rowwise, part, part.T)

        @pl.when(order > 0)
        def _():
            remote(
                outs.at[order, k], in_ref.at[gy, k], x_send.at[order, k], x_recv.at[order, k], gx, to
            ).start()

        return carry

    lax.fori_loop(0, PLANE * CAP, one_piece, 0)
    local = pltpu.make_async_copy(outs.at[0], in_ref.at[gy], l_sem)
    local.start()

    for copy in copies + [p1, p2]:
        copy.wait_send()
    local.wait()

    def finish(i, carry):
        k = i % CAP
        order = i // CAP
        copy = remote(
            outs.at[order, k], in_ref.at[gy, k], x_send.at[order, k], x_recv.at[order, k], gx, partner_of(order)
        )
        copy.wait_send()
        copy.wait_recv()
        return carry

    def partner_of(order):
        return (y + order // SIDE) % SIDE * SIDE + (x + order % SIDE) % SIDE

    lax.fori_loop(CAP, PLANE * CAP, finish, 0)


def exchange(matrix_rows, tile_owner, tile_slot, slots):
    width = matrix_rows.shape[1]
    count = tile_owner.shape[0]
    lower_i, lower_j = np.tril_indices(TILE_COUNT)
    code = jnp.asarray(lower_i * TILE_COUNT + lower_j, jnp.int32).reshape(1, count)
    smem = pl.BlockSpec(memory_space=pltpu.SMEM)
    vmem = pl.BlockSpec(memory_space=pltpu.VMEM)
    dma = pltpu.SemaphoreType.DMA
    return pl.pallas_call(
        exchange_kernel,
        out_shape=(
            jax.ShapeDtypeStruct((PLANE, CAP, 2, CHUNK, CHUNK), jnp.float32),
            jax.ShapeDtypeStruct((slots,), jnp.int32),
        ),
        in_specs=[smem, vmem, vmem, vmem, vmem],
        out_specs=(pl.BlockSpec(memory_space=pl.ANY), smem),
        scratch_shapes=[
            pltpu.VMEM((HALF_TILES, TILE, width), jnp.float32),
            pltpu.VMEM((HALF_TILES, TILE, width), jnp.bfloat16),
            pltpu.VMEM((HALF_TILES, TILE, width), jnp.bfloat16),
            pltpu.VMEM((4, CHUNK, width), jnp.float32),
            pltpu.VMEM((STEPS, CHUNK, width), jnp.bfloat16),
            pltpu.VMEM((STEPS, CHUNK, width), jnp.bfloat16),
            pltpu.VMEM((PLANE, CAP, 2, CHUNK, CHUNK), jnp.float32),
            pltpu.SMEM((ENTRIES,), jnp.int32),
            pltpu.SMEM((ENTRIES,), jnp.int32),
            pltpu.SMEM((PLANE * CAP,), jnp.int32),
            pltpu.SMEM((slots,), jnp.int32),
            dma((2, 2)), dma((2, 2)), dma((2,)), dma((2,)),
            dma((4, 2, 2)), dma((4, 2, 2)), dma((4, 2)), dma((4, 2)),
            dma((2,)), dma((2,)), dma((2,)), dma((2,)),
            dma((PLANE, CAP)), dma((PLANE, CAP)), dma(()),
        ],
        compiler_params=pltpu.CompilerParams(
            collective_id=0, has_side_effects=True, vmem_limit_bytes=48 * 1024 * 1024
        ),
        name="exchange",
    )(tile_owner, tile_owner.reshape(1, count), tile_slot.reshape(1, count), code, matrix_rows)


def assemble_kernel(table, in_ref, out_ref, tiles, in_sem, out_sem):
    slots = tiles.shape[0]

    def pieces(q, act):
        entry = table[q]
        across = entry % 4 == 1
        source = entry // 4 % HALF_TILES * 2
        rank = entry // 32
        for h in range(2):
            for c in range(2):
                row = pl.multiple_of(jnp.where(across, h, c) * CHUNK, CHUNK)
                col = pl.multiple_of(jnp.where(across, c, h) * CHUNK, CHUNK)
                act(pltpu.make_async_copy(
                    in_ref.at[source + h, rank, c],
                    tiles.at[q, pl.ds(row, CHUNK), pl.ds(col, CHUNK)],
                    in_sem.at[q, 2 * h + c],
                ))

    def fetch(q, carry):
        present = table[q] % 4 > 0

        @pl.when(present)
        def _():
            pieces(q, lambda copy: copy.start())

        @pl.when(jnp.logical_not(present))
        def _():
            tiles[q] = jnp.zeros((TILE, TILE), jnp.float32)

        return carry

    def put(q, carry):
        @pl.when(table[q] % 4 > 0)
        def _():
            pieces(q, lambda copy: copy.wait())

        pltpu.make_async_copy(tiles.at[q], out_ref.at[q], out_sem.at[q]).start()
        return carry

    def finish(q, carry):
        pltpu.make_async_copy(tiles.at[q], out_ref.at[q], out_sem.at[q]).wait()
        return carry

    lax.fori_loop(0, slots, fetch, 0)
    lax.fori_loop(0, slots, put, 0)
    lax.fori_loop(0, slots, finish, 0)


def assemble(table, incoming):
    slots = table.shape[0]
    return pl.pallas_call(
        assemble_kernel,
        out_shape=jax.ShapeDtypeStruct((slots, TILE, TILE), jnp.float32),
        in_specs=[pl.BlockSpec(memory_space=pltpu.SMEM), pl.BlockSpec(memory_space=pl.ANY)],
        out_specs=pl.BlockSpec(memory_space=pl.ANY),
        scratch_shapes=[
            pltpu.VMEM((slots, TILE, TILE), jnp.float32),
            pltpu.SemaphoreType.DMA((slots, 4)),
            pltpu.SemaphoreType.DMA((slots,)),
        ],
        name="assemble",
    )(table, incoming)


def per_device(matrix_rows, tile_owner, tile_slot):
    devices = GROUPS * PLANE
    slots = (tile_owner.shape[0] + devices - 1) // devices
    incoming, table = exchange(matrix_rows, tile_owner, tile_slot, slots)
    return assemble(table, incoming)


def solution(mesh):
    placed = (P(("gx", "gy"), None), P(), P())
    return jax.shard_map(
        per_device,
        mesh=mesh,
        in_specs=placed,
        out_specs=P(("gx", "gy"), None, None),
        check_vma=False,
    )
```

```python
import jax
import jax.numpy as jnp
import numpy as np
from jax import lax
from jax.experimental import pallas as pl
from jax.experimental.pallas import tpu as pltpu
from jax.sharding import PartitionSpec as P

MESH = pl.DeviceIdType.MESH
SIDE = 4
PLANE = SIDE * SIDE
GROUPS = 8
HALF_TILES = 8
STEPS = 5
CAP = 3
CHUNK = 128
HALF = CHUNK // 2
TILE = 256
TILE_COUNT = 64
ENTRIES = 33
ORDER = ((3, 2), (0, 1), (1, 1), (0, 2), (3, 3), (0, 3), (1, 0), (0, 0))
SERVED = len(ORDER)
PIECES = 2 * SERVED


def entry_of(e, gx, r):
    quarter = HALF_TILES // 2
    middle = GROUPS // 2 - 1
    if e <= quarter:
        s, col = 0, (r - e + HALF_TILES) % HALF_TILES
        valid = r < quarter if e == quarter else None
        rowwise = col <= r
        source = gx
    elif e <= quarter + middle * HALF_TILES:
        s, col = 1 + (e - quarter - 1) // HALF_TILES, (e - quarter - 1) % HALF_TILES
        valid = None
        source = (gx - s + GROUPS) % GROUPS
        rowwise = source > gx
    else:
        s = middle + 1
        last = e - quarter - 1 - middle * HALF_TILES
        col = 2 * last + (r + jnp.where(gx >= GROUPS // 2, 1, 0)) % 2
        valid = None
        source = (gx - s + GROUPS) % GROUPS
        rowwise = source > gx
    near = source * HALF_TILES + r
    far = gx * HALF_TILES + col
    row_tile = jnp.where(rowwise, near, far)
    col_tile = jnp.where(rowwise, far, near)
    return s, col, valid, rowwise, row_tile, col_tile


def exchange_kernel(
    owner_smem, owner_any, slot_any, code_any, a_any, in_ref, table_ref,
    a_ref, owner_ref, slot_ref, code_ref,
    g, ghi, glo, rf, qf, stage, rhi, rlo, outs, target_tab, entry_tab, send_tab, found_tab,
    a1_send, a1_recv, a2_send, a2_recv, b1_send, b1_recv, b2_send, b2_recv,
    z_send, z_recv, p_send, p_recv, q_send, q_recv, x_send, x_recv, l_sem,
):
    gx = lax.axis_index("gx")
    gy = lax.axis_index("gy")
    core = gx % 2
    y = gy // SIDE
    x = gy % SIDE
    u = jnp.where(core == 0, x, y)
    v = jnp.where(core == 0, y, x)
    stride_u = jnp.where(core == 0, 1, SIDE)
    stride_v = jnp.where(core == 0, SIDE, 1)

    def at(du, dv):
        return (u + du + SIDE) % SIDE * stride_u + (v + dv + SIDE) % SIDE * stride_v

    ahead = (gx + 2) % GROUPS
    behind = (gx + 6) % GROUPS
    partner = gx + 1 - 2 * core
    crossed = (gx + 7 + 2 * core) % GROUPS
    after = (gx + 1) % GROUPS

    loads = [
        pltpu.make_async_copy(src, dst, l_sem.at[n])
        for n, (src, dst) in enumerate(
            ((a_any, a_ref), (owner_any, owner_ref), (slot_any, slot_ref), (code_any, code_ref))
        )
    ]
    for load in loads:
        load.start()

    barrier = pltpu.get_barrier_semaphore()
    for du, dv in ((1, 0), (3, 0), (0, 1), (0, 3)):
        pl.semaphore_signal(
            barrier, inc=1, device_id={"gx": gx, "gy": at(du, dv)}, device_id_type=MESH
        )
    for other in (ahead, behind, partner, crossed):
        pl.semaphore_signal(barrier, inc=1, device_id={"gx": other, "gy": gy}, device_id_type=MESH)
    loads[0].wait()
    pl.semaphore_wait(barrier, 8)

    def rows_of(c, h, size):
        return pl.ds(pl.multiple_of(c % 2 * CHUNK + h * HALF, HALF), size)

    def half(c, h):
        return g.at[c // 2, rows_of(c, h, HALF)]

    def whole(c):
        return g.at[c // 2, rows_of(c, 0, CHUNK)]

    def own_half(h):
        return a_ref.at[pl.ds(h * HALF, HALF)]

    def remote(src, dst, send, recv, to_gx, to_gy):
        return pltpu.make_async_remote_copy(
            src_ref=src, dst_ref=dst, send_sem=send, recv_sem=recv,
            device_id={"gx": to_gx, "gy": to_gy}, device_id_type=MESH,
        )

    copies = []

    def start(copy):
        copy.start()
        copies.append(copy)

    me = gy
    a1 = [[
        remote(own_half(h), half(me, h), a1_send.at[d, p], a1_recv.at[d, p], gx, at(1 - 2 * d, 0))
        for p, h in enumerate((d, 1 - d))
    ] for d in (0, 1)]
    a2 = [
        remote(
            half(at(-1 + 2 * d, 0), d), half(at(-1 + 2 * d, 0), d),
            a2_send.at[d], a2_recv.at[d], gx, at(1 - 2 * d, 0),
        )
        for d in (0, 1)
    ]
    offs = (0, -1, 1, 2)
    b1 = [[[
        remote(
            own_half(h) if n == 0 else half(at(du, 0), h), half(at(du, 0), h),
            b1_send.at[n, d, p], b1_recv.at[n, d, p], gx, at(0, 1 - 2 * d),
        )
        for p, h in enumerate((d, 1 - d))
    ] for d in (0, 1)] for n, du in enumerate(offs)]
    b2 = [[
        remote(
            half(at(du, -1 + 2 * d), d), half(at(du, -1 + 2 * d), d),
            b2_send.at[n, d], b2_recv.at[n, d], gx, at(0, 1 - 2 * d),
        )
        for d in (0, 1)
    ] for n, du in enumerate(offs)]

    def along_z(n, src, dst, to):
        return remote(src, dst, z_send.at[n], z_recv.at[n], to, gy)

    z_near = along_z(0, a_ref, rf.at[1], ahead)
    z_back = along_z(1, a_ref, stage.at[0], behind)
    z_far = along_z(2, stage.at[0], rf.at[3], behind)

    def along_q(n, src, dst, to):
        return remote(src, dst, q_send.at[n], q_recv.at[n], to, gy)

    opposite = at(2, 0)
    q_near = along_q(1, whole(opposite), qf.at[1], ahead)
    q_back = along_q(4, whole(opposite), stage.at[1], behind)
    q_far = along_q(3, stage.at[1], qf.at[3], behind)
    q_next = along_q(0, whole(at(0, 2)), qf.at[0], after)
    q_third = along_q(2, qf.at[0], qf.at[2], ahead)

    def to_partner(n, src, dst):
        return remote(src, rf.at[dst], p_send.at[n], p_recv.at[n], partner, gy)

    for p in (0, 1):
        for d in (0, 1):
            start(a1[d][p])
    start(z_near)
    start(z_back)
    for p in (0, 1):
        for d in (0, 1):
            start(b1[0][d][p])

    @pl.when(core == 0)
    def _():
        to_partner(0, a_ref, 0).start()

    def split(value):
        high = value.astype(jnp.bfloat16)
        return high, (value - high.astype(jnp.float32)).astype(jnp.bfloat16)

    def split_g(c):
        block = c // 2
        rows = rows_of(c, 0, CHUNK)
        high, low = split(g[block, rows, :])
        ghi[block, rows, :] = high
        glo[block, rows, :] = low

    def split_r(n, value):
        high, low = split(value)
        rhi[n] = high
        rlo[n] = low

    for cls, chunk in enumerate((gy, opposite)):
        class_r = chunk // 2
        for e in range(ENTRIES):
            s, col, valid, rowwise, row_tile, col_tile = entry_of(e, gx, class_r)
            owner = owner_smem[row_tile * (row_tile + 1) // 2 + col_tile] % PLANE
            target_tab[cls * ENTRIES + e] = owner if valid is None else jnp.where(valid, owner, -1)
            diag = jnp.where(row_tile == col_tile, 2, 0)
            step = s + STEPS * cls
            entry_tab[cls * ENTRIES + e] = step * 32 + col * 4 + diag + jnp.where(rowwise, 1, 0)

    def served(n):
        du = jnp.int32(0)
        dv = jnp.int32(0)
        for m, (one, two) in enumerate(ORDER):
            du = jnp.where(n == m, one, du)
            dv = jnp.where(n == m, two, dv)
        return at(du, dv)

    def fill(p, carry):
        to = served(p // 2)
        base = p % 2 * ENTRIES
        kept = [jnp.int32(0)] * CAP
        for e in range(ENTRIES):
            hit = target_tab[base + e] == to
            fresh = entry_tab[base + e]
            kept = [jnp.where(hit, b, a) for a, b in zip(kept, [fresh] + kept[:-1])]
        for k in range(CAP):
            send_tab[p * CAP + k] = kept[k]
        return carry

    lax.fori_loop(0, PIECES, fill, 0)

    split_r(0, a_ref[...])
    block, rows = me // 2, rows_of(me, 0, CHUNK)
    ghi[block, rows, :] = rhi[0]
    glo[block, rows, :] = rlo[0]

    for d in (0, 1):
        a1[d][0].wait_recv()
        start(a2[d])
    z_back.wait_recv()
    start(z_far)
    for d in (0, 1):
        a1[d][1].wait_recv()
        for p in (0, 1):
            for e in (0, 1):
                start(b1[1 + d][e][p])
        split_g(at(-1 + 2 * d, 0))
    z_near.wait_recv()

    @pl.when(core == 0)
    def _():
        to_partner(1, rf.at[1], 2).start()

    @pl.when(core == 1)
    def _():
        to_partner(0, rf.at[1], 0).start()

    def forward_v(n):
        for d in (0, 1):
            b1[n][d][0].wait_recv()
            start(b2[n][d])

    def take_v(n):
        for d in (0, 1):
            b1[n][d][1].wait_recv()
            split_g(at(offs[n], -1 + 2 * d))

    def take_far(n):
        for d in (0, 1):
            b2[n][d].wait_recv()
        if n == 0:
            start(q_next)
        split_g(at(offs[n], 2))

    forward_v(0)
    for d in (0, 1):
        a2[d].wait_recv()
        start(b1[3][d][0])
    for d in (0, 1):
        start(b1[3][d][1])
    start(q_near)
    start(q_back)
    split_g(opposite)
    high, low = split(whole(opposite)[...])
    rhi[STEPS] = high
    rlo[STEPS] = low

    for load in loads[1:]:
        load.wait()
    mine = owner_ref[...] == gx * PLANE + gy
    slots = table_ref.shape[0]

    def find(q, carry):
        hit = jnp.logical_and(mine, slot_ref[...] == q)
        found = jnp.max(jnp.where(hit, code_ref[...], -1))
        row_tile = jnp.maximum(found, 0) // TILE_COUNT
        col_tile = jnp.maximum(found, 0) % TILE_COUNT
        group_a, inner_i = row_tile // HALF_TILES, row_tile % HALF_TILES
        group_b, inner_j = col_tile // HALF_TILES, col_tile % HALF_TILES
        gap = group_a - group_b
        even = (inner_i + inner_j) % 2 == 0
        across = jnp.logical_or(gap > GROUPS // 2, jnp.logical_and(gap == GROUPS // 2, even))
        within = inner_i - inner_j < HALF_TILES // 2
        rowwise = jnp.logical_or(jnp.logical_and(gap == 0, within), jnp.logical_and(gap > 0, across))
        class_r = jnp.where(rowwise, inner_i, inner_j)
        col = jnp.where(rowwise, inner_j, inner_i)
        s = (gx - jnp.where(rowwise, group_a, group_b) + GROUPS) % GROUPS
        place = s * HALF_TILES + jnp.where(s == 0, (class_r - col + HALF_TILES) % HALF_TILES, col)
        found_tab[q] = jnp.where(found >= 0, class_r * 64 + place, -1)
        table_ref[q] = jnp.where(found >= 0, jnp.where(rowwise, 1, 2), 0) + class_r * 4
        return carry

    lax.fori_loop(0, slots, find, 0)

    def count(q, carry):
        own = found_tab[q]
        later = jnp.int32(0)
        for other in range(slots):
            code = found_tab[other]
            same = jnp.logical_and(code // 64 == own // 64, code > own)
            later = later + jnp.where(same, 1, 0)
        table_ref[q] = table_ref[q] + 32 * jnp.minimum(later, CAP - 1)
        return carry

    take_v(0)
    take_far(0)
    forward_v(1)
    z_far.wait_recv()

    @pl.when(core == 1)
    def _():
        to_partner(1, rf.at[3], 2).start()

    q_back.wait_recv()
    start(q_far)
    lax.fori_loop(0, slots, count, 0)
    take_v(1)
    split_r(2, rf[1])
    forward_v(2)
    q_next.wait_recv()
    start(q_third)
    split_r(4, rf[3])
    p1 = to_partner(0, a_ref, 0)
    p2 = to_partner(1, a_ref, 2)
    p1.wait_recv()
    split_r(1, rf[0])
    take_v(2)
    p2.wait_recv()
    split_r(3, rf[2])
    forward_v(3)
    split_r(STEPS + 1, qf[0])
    q_near.wait_recv()
    split_r(STEPS + 2, qf[1])
    take_far(1)
    take_far(2)
    take_v(3)
    q_far.wait_recv()
    split_r(STEPS + 4, qf[3])
    take_far(3)
    q_third.wait_recv()
    split_r(STEPS + 3, qf[2])

    row_in = lax.broadcasted_iota(jnp.int32, (CHUNK, TILE), 0)
    col_in = lax.broadcasted_iota(jnp.int32, (CHUNK, TILE), 1)

    def dot(p, q):
        return lax.dot_general(p, q, (((1,), (1,)), ((), ())), preferred_element_type=jnp.float32)

    def one_piece(i, carry):
        k = i // PIECES
        p = i % PIECES
        to = served(p // 2)
        chunk = jnp.where(p % 2 == 0, gy, opposite)
        entry = send_tab[p * CAP + k]
        s = entry // 32
        j = entry // 4 % HALF_TILES
        rh = rhi[s]
        gh = ghi[j]
        value = dot(rh, gh) + dot(rh, glo[j]) + dot(rlo[s], gh)
        upper = row_in + chunk % 2 * CHUNK < col_in
        masked = jnp.logical_and(upper, entry // 2 % 2 > 0)
        value = jnp.where(masked, jnp.float32(0.0), value)
        rowwise = jnp.full((CHUNK, CHUNK), entry % 2, jnp.int32) > 0
        for c in range(2):
            part = value[:, c * CHUNK:(c + 1) * CHUNK]
            outs[p, k, c] = jnp.where(rowwise, part, part.T)

        @pl.when(p < PIECES - 2)
        def _():
            remote(
                outs.at[p, k], in_ref.at[chunk, k], x_send.at[p, k], x_recv.at[chunk, k], gx, to
            ).start()

        return carry

    lax.fori_loop(0, PIECES * CAP, one_piece, 0)
    local = [
        pltpu.make_async_copy(outs.at[PIECES - 2 + n], in_ref.at[c], l_sem.at[n])
        for n, c in enumerate((gy, opposite))
    ]
    for copy in local:
        copy.start()
    for copy in copies + [p1, p2]:
        copy.wait_send()
    for copy in local:
        copy.wait()

    def sent(i, carry):
        remote(
            outs.at[i // CAP, i % CAP], in_ref.at[0, 0], x_send.at[i // CAP, i % CAP], x_recv.at[0, 0], ahead, gy
        ).wait_send()
        return carry

    lax.fori_loop(0, (PIECES - 2) * CAP, sent, 0)

    def arrived(i, carry):
        du = i // CAP // SIDE
        chunk = at(du, i // CAP % SIDE)

        @pl.when(jnp.logical_or(i // CAP % SIDE > 0, du % 2 > 0))
        def _():
            remote(
                outs.at[0, 0], in_ref.at[chunk, i % CAP], x_send.at[0, 0], x_recv.at[chunk, i % CAP], ahead, gy
            ).wait_recv()

        return carry

    lax.fori_loop(0, PLANE * CAP, arrived, 0)


def exchange(matrix_rows, tile_owner, tile_slot, slots):
    rows, width = matrix_rows.shape
    count = tile_owner.shape[0]
    lower_i, lower_j = np.tril_indices(TILE_COUNT)
    code = jnp.asarray(lower_i * TILE_COUNT + lower_j, jnp.int32)
    smem = pl.BlockSpec(memory_space=pltpu.SMEM)
    hbm = pl.BlockSpec(memory_space=pl.ANY)
    dma = pltpu.SemaphoreType.DMA
    return pl.pallas_call(
        exchange_kernel,
        out_shape=(
            jax.ShapeDtypeStruct((PLANE, CAP, 2, CHUNK, CHUNK), jnp.float32),
            jax.ShapeDtypeStruct((slots,), jnp.int32),
        ),
        in_specs=[smem, hbm, hbm, hbm, hbm],
        out_specs=(hbm, smem),
        scratch_shapes=[
            pltpu.VMEM((rows, width), jnp.float32),
            pltpu.VMEM((count,), jnp.int32),
            pltpu.VMEM((count,), jnp.int32),
            pltpu.VMEM((count,), jnp.int32),
            pltpu.VMEM((HALF_TILES, TILE, width), jnp.float32),
            pltpu.VMEM((HALF_TILES, TILE, width), jnp.bfloat16),
            pltpu.VMEM((HALF_TILES, TILE, width), jnp.bfloat16),
            pltpu.VMEM((4, CHUNK, width), jnp.float32),
            pltpu.VMEM((4, CHUNK, width), jnp.float32),
            pltpu.VMEM((2, CHUNK, width), jnp.float32),
            pltpu.VMEM((2 * STEPS, CHUNK, width), jnp.bfloat16),
            pltpu.VMEM((2 * STEPS, CHUNK, width), jnp.bfloat16),
            pltpu.VMEM((PIECES, CAP, 2, CHUNK, CHUNK), jnp.float32),
            pltpu.SMEM((2 * ENTRIES,), jnp.int32),
            pltpu.SMEM((2 * ENTRIES,), jnp.int32),
            pltpu.SMEM((PIECES * CAP,), jnp.int32),
            pltpu.SMEM((slots,), jnp.int32),
            dma((2, 2)), dma((2, 2)), dma((2,)), dma((2,)),
            dma((4, 2, 2)), dma((4, 2, 2)), dma((4, 2)), dma((4, 2)),
            dma((3,)), dma((3,)), dma((2,)), dma((2,)), dma((5,)), dma((5,)),
            dma((PIECES, CAP)), dma((PLANE, CAP)), dma((4,)),
        ],
        compiler_params=pltpu.CompilerParams(
            collective_id=0, has_side_effects=True, vmem_limit_bytes=56 * 1024 * 1024
        ),
        name="exchange",
    )(tile_owner, tile_owner, tile_slot, code, matrix_rows)


def assemble_kernel(table, in_ref, out_ref, tiles, in_sem, out_sem):
    slots = tiles.shape[0]

    def pieces(q, act):
        entry = table[q]
        across = entry % 4 == 1
        source = entry // 4 % HALF_TILES * 2
        rank = entry // 32
        for h in range(2):
            for c in range(2):
                row = pl.multiple_of(jnp.where(across, h, c) * CHUNK, CHUNK)
                col = pl.multiple_of(jnp.where(across, c, h) * CHUNK, CHUNK)
                act(pltpu.make_async_copy(
                    in_ref.at[source + h, rank, c],
                    tiles.at[q, pl.ds(row, CHUNK), pl.ds(col, CHUNK)],
                    in_sem.at[q, 2 * h + c],
                ))

    def fetch(q, carry):
        present = table[q] % 4 > 0

        @pl.when(present)
        def _():
            pieces(q, lambda copy: copy.start())

        @pl.when(jnp.logical_not(present))
        def _():
            tiles[q] = jnp.zeros((TILE, TILE), jnp.float32)

        return carry

    def put(q, carry):
        @pl.when(table[q] % 4 > 0)
        def _():
            pieces(q, lambda copy: copy.wait())

        pltpu.make_async_copy(tiles.at[q], out_ref.at[q], out_sem.at[q]).start()
        return carry

    def finish(q, carry):
        pltpu.make_async_copy(tiles.at[q], out_ref.at[q], out_sem.at[q]).wait()
        return carry

    lax.fori_loop(0, slots, fetch, 0)
    lax.fori_loop(0, slots, put, 0)
    lax.fori_loop(0, slots, finish, 0)


def assemble(table, incoming):
    slots = table.shape[0]
    return pl.pallas_call(
        assemble_kernel,
        out_shape=jax.ShapeDtypeStruct((slots, TILE, TILE), jnp.float32),
        in_specs=[pl.BlockSpec(memory_space=pltpu.SMEM), pl.BlockSpec(memory_space=pl.ANY)],
        out_specs=pl.BlockSpec(memory_space=pl.ANY),
        scratch_shapes=[
            pltpu.VMEM((slots, TILE, TILE), jnp.float32),
            pltpu.SemaphoreType.DMA((slots, 4)),
            pltpu.SemaphoreType.DMA((slots,)),
        ],
        name="assemble",
    )(table, incoming)


def per_device(matrix_rows, tile_owner, tile_slot):
    devices = GROUPS * PLANE
    slots = (tile_owner.shape[0] + devices - 1) // devices
    incoming, table = exchange(matrix_rows, tile_owner, tile_slot, slots)
    return assemble(table, incoming)


def solution(mesh):
    placed = (P(("gx", "gy"), None), P(), P())
    return jax.shard_map(
        per_device,
        mesh=mesh,
        in_specs=placed,
        out_specs=P(("gx", "gy"), None, None),
        check_vma=False,
    )
```

```python
import jax
import jax.numpy as jnp
import numpy as np
from jax import lax
from jax.experimental import pallas as pl
from jax.experimental.pallas import tpu as pltpu
from jax.sharding import PartitionSpec as P

MESH = pl.DeviceIdType.MESH
SIDE = 4
PLANE = SIDE * SIDE
GROUPS = 8
HALF_TILES = 8
STEPS = 5
CAP = 3
CHUNK = 128
HALF = CHUNK // 2
TILE = 256
TILE_COUNT = 64
ENTRIES = 33
ORDER = ((2, 0), (0, 1), (1, 9), (0, 3), (3, 9), (1, 0), (3, 0), (0, 0))
SERVED = len(ORDER)
PIECES = 2 * SERVED


def entry_of(e, gx, r):
    quarter = HALF_TILES // 2
    middle = GROUPS // 2 - 1
    if e <= quarter:
        s, col = 0, (r - e + HALF_TILES) % HALF_TILES
        valid = r < quarter if e == quarter else None
        rowwise = col <= r
        source = gx
    elif e <= quarter + middle * HALF_TILES:
        s, col = 1 + (e - quarter - 1) // HALF_TILES, (e - quarter - 1) % HALF_TILES
        valid = None
        source = (gx - s + GROUPS) % GROUPS
        rowwise = source > gx
    else:
        s = middle + 1
        last = e - quarter - 1 - middle * HALF_TILES
        col = 2 * last + (r + jnp.where(gx >= GROUPS // 2, 1, 0)) % 2
        valid = None
        source = (gx - s + GROUPS) % GROUPS
        rowwise = source > gx
    near = source * HALF_TILES + r
    far = gx * HALF_TILES + col
    row_tile = jnp.where(rowwise, near, far)
    col_tile = jnp.where(rowwise, far, near)
    return s, col, valid, rowwise, row_tile, col_tile


def exchange_kernel(
    owner_smem, owner_any, slot_any, code_any, a_any, in_ref, table_ref,
    a_ref, owner_ref, slot_ref, code_ref,
    g, ghi, glo, rf, qf, stage, rhi, rlo, outs, target_tab, entry_tab, send_tab, found_tab,
    a1_send, a1_recv, a2_send, a2_recv, b1_send, b1_recv, b2_send, b2_recv,
    z_send, z_recv, p_send, p_recv, q_send, q_recv, x_send, x_recv, l_sem,
):
    gx = lax.axis_index("gx")
    gy = lax.axis_index("gy")
    core = gx % 2
    y = gy // SIDE
    x = gy % SIDE
    u = jnp.where(core == 0, x, y)
    v = jnp.where(core == 0, y, x)
    stride_u = jnp.where(core == 0, 1, SIDE)
    stride_v = jnp.where(core == 0, SIDE, 1)

    def at(du, dv):
        return (u + du + SIDE) % SIDE * stride_u + (v + dv + SIDE) % SIDE * stride_v

    ahead = (gx + 2) % GROUPS
    behind = (gx + 6) % GROUPS
    partner = gx + 1 - 2 * core

    loads = [
        pltpu.make_async_copy(src, dst, l_sem.at[n])
        for n, (src, dst) in enumerate(
            ((a_any, a_ref), (owner_any, owner_ref), (slot_any, slot_ref), (code_any, code_ref))
        )
    ]
    for load in loads:
        load.start()

    barrier = pltpu.get_barrier_semaphore()
    for du, dv in ((1, 0), (3, 0), (0, 1), (0, 3)):
        pl.semaphore_signal(
            barrier, inc=1, device_id={"gx": gx, "gy": at(du, dv)}, device_id_type=MESH
        )
    for other in (ahead, behind, partner):
        pl.semaphore_signal(barrier, inc=1, device_id={"gx": other, "gy": gy}, device_id_type=MESH)
    loads[0].wait()
    pl.semaphore_wait(barrier, 7)

    def rows_of(c, h, size):
        return pl.ds(pl.multiple_of(c % 2 * CHUNK + h * HALF, HALF), size)

    def half(c, h):
        return g.at[c // 2, rows_of(c, h, HALF)]

    def whole(c):
        return g.at[c // 2, rows_of(c, 0, CHUNK)]

    def own_half(h):
        return a_ref.at[pl.ds(h * HALF, HALF)]

    def remote(src, dst, send, recv, to_gx, to_gy):
        return pltpu.make_async_remote_copy(
            src_ref=src, dst_ref=dst, send_sem=send, recv_sem=recv,
            device_id={"gx": to_gx, "gy": to_gy}, device_id_type=MESH,
        )

    copies = []

    def start(copy):
        copy.start()
        copies.append(copy)

    me = gy
    a1 = [[
        remote(own_half(h), half(me, h), a1_send.at[d, p], a1_recv.at[d, p], gx, at(1 - 2 * d, 0))
        for p, h in enumerate((d, 1 - d))
    ] for d in (0, 1)]
    a2 = [
        remote(
            half(at(-1 + 2 * d, 0), d), half(at(-1 + 2 * d, 0), d),
            a2_send.at[d], a2_recv.at[d], gx, at(1 - 2 * d, 0),
        )
        for d in (0, 1)
    ]
    offs = (0, -1, 1, 2)
    b1 = [[[
        remote(
            own_half(h) if n == 0 else half(at(du, 0), h), half(at(du, 0), h),
            b1_send.at[n, d, p], b1_recv.at[n, d, p], gx, at(0, 1 - 2 * d),
        )
        for p, h in enumerate((d, 1 - d))
    ] for d in (0, 1)] for n, du in enumerate(offs)]
    b2 = [[
        remote(
            half(at(du, -1 + 2 * d), d), half(at(du, -1 + 2 * d), d),
            b2_send.at[n, d], b2_recv.at[n, d], gx, at(0, 1 - 2 * d),
        )
        for d in (0, 1)
    ] for n, du in enumerate(offs)]

    def along_z(n, src, dst, to):
        return remote(src, dst, z_send.at[n], z_recv.at[n], to, gy)

    z_near = along_z(0, a_ref, rf.at[1], ahead)
    z_back = along_z(1, a_ref, stage.at[0], behind)
    z_far = along_z(2, stage.at[0], rf.at[3], behind)

    def along_q(n, src, dst, to):
        return remote(src, dst, q_send.at[n], q_recv.at[n], to, gy)

    opposite = at(2, 2)
    q_near = along_q(0, whole(opposite), qf.at[1], ahead)
    q_back = along_q(1, whole(opposite), stage.at[1], behind)
    q_far = along_q(2, stage.at[1], qf.at[3], behind)

    def to_partner(n, src, dst):
        return remote(src, dst, p_send.at[n], p_recv.at[n], partner, gy)

    p_of = [to_partner(n, a_ref, dst) for n, dst in enumerate((rf.at[0], rf.at[2], qf.at[0], qf.at[2]))]

    for p in (0, 1):
        for d in (0, 1):
            start(a1[d][p])
    start(z_near)
    start(z_back)

    @pl.when(core == 0)
    def _():
        to_partner(0, a_ref, rf.at[0]).start()

    def split(value):
        high = value.astype(jnp.bfloat16)
        return high, (value - high.astype(jnp.float32)).astype(jnp.bfloat16)

    def split_g(c):
        block = c // 2
        rows = rows_of(c, 0, CHUNK)
        high, low = split(g[block, rows, :])
        ghi[block, rows, :] = high
        glo[block, rows, :] = low

    def split_r(n, value):
        high, low = split(value)
        rhi[n] = high
        rlo[n] = low

    for cls, chunk in enumerate((gy, opposite)):
        class_r = chunk // 2
        for e in range(ENTRIES):
            s, col, valid, rowwise, row_tile, col_tile = entry_of(e, gx, class_r)
            owner = owner_smem[row_tile * (row_tile + 1) // 2 + col_tile] % PLANE
            target_tab[cls * ENTRIES + e] = owner if valid is None else jnp.where(valid, owner, -1)
            diag = jnp.where(row_tile == col_tile, 2, 0)
            step = s + STEPS * cls
            entry_tab[cls * ENTRIES + e] = step * 32 + col * 4 + diag + jnp.where(rowwise, 1, 0)

    def served(n, cls):
        du = jnp.int32(0)
        dv = jnp.int32(0)
        for m, (one, two) in enumerate(ORDER):
            du = jnp.where(n == m, one, du)
            dv = jnp.where(n == m, two, dv)
        side = jnp.where((u + 2 * cls) % SIDE < 2, 1, 3)
        return at(du, jnp.where(dv == 9, side, dv))

    def fill(p, carry):
        to = served(p // 2, p % 2)
        base = p % 2 * ENTRIES
        kept = [jnp.int32(0)] * CAP
        for e in range(ENTRIES):
            hit = target_tab[base + e] == to
            fresh = entry_tab[base + e]
            kept = [jnp.where(hit, b, a) for a, b in zip(kept, [fresh] + kept[:-1])]
        for k in range(CAP):
            send_tab[p * CAP + k] = kept[k]
        return carry

    split_r(0, a_ref[...])
    block, rows = me // 2, rows_of(me, 0, CHUNK)
    ghi[block, rows, :] = rhi[0]
    glo[block, rows, :] = rlo[0]

    for d in (0, 1):
        a1[d][0].wait_recv()
        start(a2[d])
    for d in (0, 1):
        start(b1[0][d][0])
    for d in (0, 1):
        a1[d][1].wait_recv()
        split_g(at(-1 + 2 * d, 0))
    for d in (0, 1):
        a2[d].wait_recv()
        start(b1[3][d][0])
    split_g(at(2, 0))
    lax.fori_loop(0, PIECES, fill, 0)

    def forward_v(n):
        for d in (0, 1):
            b1[n][d][0].wait_recv()
            start(b2[n][d])

    def take_v(n):
        for d in (0, 1):
            b1[n][d][1].wait_recv()
            split_g(at(offs[n], -1 + 2 * d))

    def take_far(n):
        for d in (0, 1):
            b2[n][d].wait_recv()
        split_g(at(offs[n], 2))

    forward_v(3)
    forward_v(0)
    for n, p in ((1, 0), (2, 0), (3, 1), (0, 1)):
        for d in (0, 1):
            start(b1[n][d][p])
    z_back.wait_recv()
    start(z_far)
    z_near.wait_recv()

    @pl.when(core == 0)
    def _():
        to_partner(1, rf.at[1], rf.at[2]).start()

    @pl.when(core == 1)
    def _():
        to_partner(0, rf.at[1], rf.at[0]).start()

    for d in (0, 1):
        b2[3][d].wait_recv()
    start(q_near)
    start(q_back)

    @pl.when(core == 0)
    def _():
        to_partner(2, whole(opposite), qf.at[0]).start()

    split_g(opposite)
    high, low = split(whole(opposite)[...])
    rhi[STEPS] = high
    rlo[STEPS] = low
    split_r(2, rf[1])

    for load in loads[1:]:
        load.wait()
    mine = owner_ref[...] == gx * PLANE + gy
    slots = table_ref.shape[0]

    def find(q, carry):
        hit = jnp.logical_and(mine, slot_ref[...] == q)
        found = jnp.max(jnp.where(hit, code_ref[...], -1))
        row_tile = jnp.maximum(found, 0) // TILE_COUNT
        col_tile = jnp.maximum(found, 0) % TILE_COUNT
        group_a, inner_i = row_tile // HALF_TILES, row_tile % HALF_TILES
        group_b, inner_j = col_tile // HALF_TILES, col_tile % HALF_TILES
        gap = group_a - group_b
        even = (inner_i + inner_j) % 2 == 0
        across = jnp.logical_or(gap > GROUPS // 2, jnp.logical_and(gap == GROUPS // 2, even))
        within = inner_i - inner_j < HALF_TILES // 2
        rowwise = jnp.logical_or(jnp.logical_and(gap == 0, within), jnp.logical_and(gap > 0, across))
        class_r = jnp.where(rowwise, inner_i, inner_j)
        col = jnp.where(rowwise, inner_j, inner_i)
        s = (gx - jnp.where(rowwise, group_a, group_b) + GROUPS) % GROUPS
        place = s * HALF_TILES + jnp.where(s == 0, (class_r - col + HALF_TILES) % HALF_TILES, col)
        found_tab[q] = jnp.where(found >= 0, class_r * 64 + place, -1)
        table_ref[q] = jnp.where(found >= 0, jnp.where(rowwise, 1, 2), 0) + class_r * 4
        return carry

    lax.fori_loop(0, slots, find, 0)

    def count(q, carry):
        own = found_tab[q]
        later = jnp.int32(0)
        for other in range(slots):
            code = found_tab[other]
            same = jnp.logical_and(code // 64 == own // 64, code > own)
            later = later + jnp.where(same, 1, 0)
        table_ref[q] = table_ref[q] + 32 * jnp.minimum(later, CAP - 1)
        return carry

    for n in (1, 2):
        forward_v(n)
    for n in (1, 2):
        for d in (0, 1):
            start(b1[n][d][1])
    z_far.wait_recv()

    @pl.when(core == 1)
    def _():
        to_partner(1, rf.at[3], rf.at[2]).start()

    q_back.wait_recv()
    start(q_far)
    q_near.wait_recv()

    @pl.when(core == 0)
    def _():
        to_partner(3, qf.at[1], qf.at[2]).start()

    @pl.when(core == 1)
    def _():
        to_partner(2, qf.at[1], qf.at[0]).start()

    lax.fori_loop(0, slots, count, 0)
    take_far(0)
    split_r(4, rf[3])
    split_r(STEPS + 2, qf[1])
    p_of[0].wait_recv()
    split_r(1, rf[0])
    p_of[1].wait_recv()
    split_r(3, rf[2])
    take_v(3)
    take_v(0)
    p_of[2].wait_recv()
    split_r(STEPS + 1, qf[0])
    q_far.wait_recv()

    @pl.when(core == 1)
    def _():
        to_partner(3, qf.at[3], qf.at[2]).start()

    split_r(STEPS + 4, qf[3])
    take_far(1)
    take_far(2)
    p_of[3].wait_recv()
    split_r(STEPS + 3, qf[2])
    take_v(1)
    take_v(2)

    row_in = lax.broadcasted_iota(jnp.int32, (CHUNK, TILE), 0)
    col_in = lax.broadcasted_iota(jnp.int32, (CHUNK, TILE), 1)

    def dot(p, q):
        return lax.dot_general(p, q, (((1,), (1,)), ((), ())), preferred_element_type=jnp.float32)

    def one_piece(i, carry):
        k = i // PIECES
        p = i % PIECES
        to = served(p // 2, p % 2)
        chunk = jnp.where(p % 2 == 0, gy, opposite)
        entry = send_tab[p * CAP + k]
        s = entry // 32
        j = entry // 4 % HALF_TILES
        rh = rhi[s]
        gh = ghi[j]
        value = dot(rh, gh) + dot(rh, glo[j]) + dot(rlo[s], gh)
        upper = row_in + chunk % 2 * CHUNK < col_in
        masked = jnp.logical_and(upper, entry // 2 % 2 > 0)
        value = jnp.where(masked, jnp.float32(0.0), value)
        rowwise = jnp.full((CHUNK, CHUNK), entry % 2, jnp.int32) > 0
        for c in range(2):
            part = value[:, c * CHUNK:(c + 1) * CHUNK]
            outs[p, k, c] = jnp.where(rowwise, part, part.T)

        @pl.when(p < PIECES - 2)
        def _():
            remote(
                outs.at[p, k], in_ref.at[chunk, k], x_send.at[p, k], x_recv.at[chunk, k], gx, to
            ).start()

        return carry

    lax.fori_loop(0, PIECES * CAP, one_piece, 0)
    local = [
        pltpu.make_async_copy(outs.at[PIECES - 2 + n], in_ref.at[c], l_sem.at[n])
        for n, c in enumerate((gy, opposite))
    ]
    for copy in local:
        copy.start()
    for copy in copies + p_of:
        copy.wait_send()
    for copy in local:
        copy.wait()

    def sent(i, carry):
        remote(
            outs.at[i // CAP, i % CAP], in_ref.at[0, 0], x_send.at[i // CAP, i % CAP], x_recv.at[0, 0], ahead, gy
        ).wait_send()
        return carry

    lax.fori_loop(0, (PIECES - 2) * CAP, sent, 0)

    def arrived(i, carry):
        du = i // CAP // SIDE
        dv = i // CAP % SIDE
        chunk = at(du, dv)

        @pl.when(jnp.logical_or(du != dv, du % 2 > 0))
        def _():
            remote(
                outs.at[0, 0], in_ref.at[chunk, i % CAP], x_send.at[0, 0], x_recv.at[chunk, i % CAP], ahead, gy
            ).wait_recv()

        return carry

    lax.fori_loop(0, PLANE * CAP, arrived, 0)


def exchange(matrix_rows, tile_owner, tile_slot, slots):
    rows, width = matrix_rows.shape
    count = tile_owner.shape[0]
    lower_i, lower_j = np.tril_indices(TILE_COUNT)
    code = jnp.asarray(lower_i * TILE_COUNT + lower_j, jnp.int32)
    smem = pl.BlockSpec(memory_space=pltpu.SMEM)
    hbm = pl.BlockSpec(memory_space=pl.ANY)
    dma = pltpu.SemaphoreType.DMA
    return pl.pallas_call(
        exchange_kernel,
        out_shape=(
            jax.ShapeDtypeStruct((PLANE, CAP, 2, CHUNK, CHUNK), jnp.float32),
            jax.ShapeDtypeStruct((slots,), jnp.int32),
        ),
        in_specs=[smem, hbm, hbm, hbm, hbm],
        out_specs=(hbm, smem),
        scratch_shapes=[
            pltpu.VMEM((rows, width), jnp.float32),
            pltpu.VMEM((count,), jnp.int32),
            pltpu.VMEM((count,), jnp.int32),
            pltpu.VMEM((count,), jnp.int32),
            pltpu.VMEM((HALF_TILES, TILE, width), jnp.float32),
            pltpu.VMEM((HALF_TILES, TILE, width), jnp.bfloat16),
            pltpu.VMEM((HALF_TILES, TILE, width), jnp.bfloat16),
            pltpu.VMEM((4, CHUNK, width), jnp.float32),
            pltpu.VMEM((4, CHUNK, width), jnp.float32),
            pltpu.VMEM((2, CHUNK, width), jnp.float32),
            pltpu.VMEM((2 * STEPS, CHUNK, width), jnp.bfloat16),
            pltpu.VMEM((2 * STEPS, CHUNK, width), jnp.bfloat16),
            pltpu.VMEM((PIECES, CAP, 2, CHUNK, CHUNK), jnp.float32),
            pltpu.SMEM((2 * ENTRIES,), jnp.int32),
            pltpu.SMEM((2 * ENTRIES,), jnp.int32),
            pltpu.SMEM((PIECES * CAP,), jnp.int32),
            pltpu.SMEM((slots,), jnp.int32),
            dma((2, 2)), dma((2, 2)), dma((2,)), dma((2,)),
            dma((4, 2, 2)), dma((4, 2, 2)), dma((4, 2)), dma((4, 2)),
            dma((3,)), dma((3,)), dma((4,)), dma((4,)), dma((3,)), dma((3,)),
            dma((PIECES, CAP)), dma((PLANE, CAP)), dma((4,)),
        ],
        compiler_params=pltpu.CompilerParams(
            collective_id=0, has_side_effects=True, vmem_limit_bytes=56 * 1024 * 1024
        ),
        name="exchange",
    )(tile_owner, tile_owner, tile_slot, code, matrix_rows)


def assemble_kernel(table, in_ref, out_ref, tiles, in_sem, out_sem):
    slots = tiles.shape[0]

    def pieces(q, act):
        entry = table[q]
        across = entry % 4 == 1
        source = entry // 4 % HALF_TILES * 2
        rank = entry // 32
        for h in range(2):
            for c in range(2):
                row = pl.multiple_of(jnp.where(across, h, c) * CHUNK, CHUNK)
                col = pl.multiple_of(jnp.where(across, c, h) * CHUNK, CHUNK)
                act(pltpu.make_async_copy(
                    in_ref.at[source + h, rank, c],
                    tiles.at[q, pl.ds(row, CHUNK), pl.ds(col, CHUNK)],
                    in_sem.at[q, 2 * h + c],
                ))

    def fetch(q, carry):
        present = table[q] % 4 > 0

        @pl.when(present)
        def _():
            pieces(q, lambda copy: copy.start())

        @pl.when(jnp.logical_not(present))
        def _():
            tiles[q] = jnp.zeros((TILE, TILE), jnp.float32)

        return carry

    def put(q, carry):
        @pl.when(table[q] % 4 > 0)
        def _():
            pieces(q, lambda copy: copy.wait())

        pltpu.make_async_copy(tiles.at[q], out_ref.at[q], out_sem.at[q]).start()
        return carry

    def finish(q, carry):
        pltpu.make_async_copy(tiles.at[q], out_ref.at[q], out_sem.at[q]).wait()
        return carry

    lax.fori_loop(0, slots, fetch, 0)
    lax.fori_loop(0, slots, put, 0)
    lax.fori_loop(0, slots, finish, 0)


def assemble(table, incoming):
    slots = table.shape[0]
    return pl.pallas_call(
        assemble_kernel,
        out_shape=jax.ShapeDtypeStruct((slots, TILE, TILE), jnp.float32),
        in_specs=[pl.BlockSpec(memory_space=pltpu.SMEM), pl.BlockSpec(memory_space=pl.ANY)],
        out_specs=pl.BlockSpec(memory_space=pl.ANY),
        scratch_shapes=[
            pltpu.VMEM((slots, TILE, TILE), jnp.float32),
            pltpu.SemaphoreType.DMA((slots, 4)),
            pltpu.SemaphoreType.DMA((slots,)),
        ],
        name="assemble",
    )(table, incoming)


def per_device(matrix_rows, tile_owner, tile_slot):
    devices = GROUPS * PLANE
    slots = (tile_owner.shape[0] + devices - 1) // devices
    incoming, table = exchange(matrix_rows, tile_owner, tile_slot, slots)
    return assemble(table, incoming)


def solution(mesh):
    placed = (P(("gx", "gy"), None), P(), P())
    return jax.shard_map(
        per_device,
        mesh=mesh,
        in_specs=placed,
        out_specs=P(("gx", "gy"), None, None),
        check_vma=False,
    )
```

```python
import jax
import jax.numpy as jnp
import numpy as np
from jax import lax
from jax.experimental import pallas as pl
from jax.experimental.pallas import tpu as pltpu
from jax.sharding import PartitionSpec as P

MESH = pl.DeviceIdType.MESH
SIDE = 4
PLANE = SIDE * SIDE
GROUPS = 8
HALF_TILES = 8
STEPS = 5
CAP = 3
CHUNK = 128
HALF = CHUNK // 2
TILE = 256
TILE_COUNT = 64
ENTRIES = 33
ORDER = ((2, 0), (0, 1), (1, 9), (0, 3), (3, 9), (1, 0), (3, 0), (0, 0))
SERVED = len(ORDER)
PIECES = 2 * SERVED


def entry_of(e, gx, r):
    quarter = HALF_TILES // 2
    middle = GROUPS // 2 - 1
    if e <= quarter:
        s, col = 0, (r - e + HALF_TILES) % HALF_TILES
        valid = r < quarter if e == quarter else None
        rowwise = col <= r
        source = gx
    elif e <= quarter + middle * HALF_TILES:
        s, col = 1 + (e - quarter - 1) // HALF_TILES, (e - quarter - 1) % HALF_TILES
        valid = None
        source = (gx - s + GROUPS) % GROUPS
        rowwise = source > gx
    else:
        s = middle + 1
        last = e - quarter - 1 - middle * HALF_TILES
        col = 2 * last + (r + jnp.where(gx >= GROUPS // 2, 1, 0)) % 2
        valid = None
        source = (gx - s + GROUPS) % GROUPS
        rowwise = source > gx
    near = source * HALF_TILES + r
    far = gx * HALF_TILES + col
    row_tile = jnp.where(rowwise, near, far)
    col_tile = jnp.where(rowwise, far, near)
    return s, col, valid, rowwise, row_tile, col_tile


def exchange_kernel(
    owner_smem, owner_any, slot_any, code_any, a_any, in_ref, table_ref,
    a_ref, owner_ref, slot_ref, code_ref,
    g, ghi, glo, rf, qf, rhi, rlo, outs, target_tab, entry_tab, send_tab, found_tab,
    a1_send, a1_recv, a2_send, a2_recv, b1_send, b1_recv, b2_send, b2_recv,
    z_send, z_recv, p_send, p_recv, q_send, q_recv, x_send, x_recv, l_sem,
):
    gx = lax.axis_index("gx")
    gy = lax.axis_index("gy")
    core = gx % 2
    y = gy // SIDE
    x = gy % SIDE
    u = jnp.where(core == 0, x, y)
    v = jnp.where(core == 0, y, x)
    stride_u = jnp.where(core == 0, 1, SIDE)
    stride_v = jnp.where(core == 0, SIDE, 1)

    def at(du, dv):
        return (u + du + SIDE) % SIDE * stride_u + (v + dv + SIDE) % SIDE * stride_v

    ahead = (gx + 2) % GROUPS
    behind = (gx + 6) % GROUPS
    beyond = (gx + 4) % GROUPS
    partner = gx + 1 - 2 * core

    loads = [
        pltpu.make_async_copy(src, dst, l_sem.at[n])
        for n, (src, dst) in enumerate(
            ((a_any, a_ref), (owner_any, owner_ref), (slot_any, slot_ref), (code_any, code_ref))
        )
    ]
    for load in loads:
        load.start()

    barrier = pltpu.get_barrier_semaphore()
    for du, dv in ((1, 0), (3, 0), (0, 1), (0, 3)):
        pl.semaphore_signal(
            barrier, inc=1, device_id={"gx": gx, "gy": at(du, dv)}, device_id_type=MESH
        )
    for other in (ahead, behind, beyond, partner):
        pl.semaphore_signal(barrier, inc=1, device_id={"gx": other, "gy": gy}, device_id_type=MESH)
    loads[0].wait()
    pl.semaphore_wait(barrier, 8)

    def rows_of(c, h, size):
        return pl.ds(pl.multiple_of(c % 2 * CHUNK + h * HALF, HALF), size)

    def half(c, h):
        return g.at[c // 2, rows_of(c, h, HALF)]

    def whole(c):
        return g.at[c // 2, rows_of(c, 0, CHUNK)]

    def own_half(h):
        return a_ref.at[pl.ds(h * HALF, HALF)]

    def remote(src, dst, send, recv, to_gx, to_gy):
        return pltpu.make_async_remote_copy(
            src_ref=src, dst_ref=dst, send_sem=send, recv_sem=recv,
            device_id={"gx": to_gx, "gy": to_gy}, device_id_type=MESH,
        )

    copies = []

    def start(copy):
        copy.start()
        copies.append(copy)

    me = gy
    a1 = [[
        remote(own_half(h), half(me, h), a1_send.at[d, p], a1_recv.at[d, p], gx, at(1 - 2 * d, 0))
        for p, h in enumerate((d, 1 - d))
    ] for d in (0, 1)]
    a2 = [
        remote(
            half(at(-1 + 2 * d, 0), d), half(at(-1 + 2 * d, 0), d),
            a2_send.at[d], a2_recv.at[d], gx, at(1 - 2 * d, 0),
        )
        for d in (0, 1)
    ]
    offs = (0, -1, 1, 2)
    b1 = [[[
        remote(
            own_half(h) if n == 0 else half(at(du, 0), h), half(at(du, 0), h),
            b1_send.at[n, d, p], b1_recv.at[n, d, p], gx, at(0, 1 - 2 * d),
        )
        for p, h in enumerate((d, 1 - d))
    ] for d in (0, 1)] for n, du in enumerate(offs)]
    b2 = [[
        remote(
            half(at(du, -1 + 2 * d), d), half(at(du, -1 + 2 * d), d),
            b2_send.at[n, d], b2_recv.at[n, d], gx, at(0, 1 - 2 * d),
        )
        for d in (0, 1)
    ] for n, du in enumerate(offs)]

    def along_z(n, src, dst, to):
        return remote(src, dst, z_send.at[n], z_recv.at[n], to, gy)

    z_near = along_z(0, a_ref, rf.at[1], ahead)
    z_far = along_z(1, a_ref, rf.at[3], beyond)

    def along_q(n, src, dst, to):
        return remote(src, dst, q_send.at[n], q_recv.at[n], to, gy)

    opposite = at(2, 2)
    q_near = along_q(0, whole(opposite), qf.at[1], ahead)
    q_far = along_q(1, whole(opposite), qf.at[3], beyond)

    def to_partner(n, src, dst):
        return remote(src, dst, p_send.at[n], p_recv.at[n], partner, gy)

    p_of = [to_partner(n, a_ref, dst) for n, dst in enumerate((rf.at[0], rf.at[2], qf.at[0], qf.at[2]))]

    for p in (0, 1):
        for d in (0, 1):
            start(a1[d][p])
    start(z_near)
    start(z_far)

    @pl.when(core == 0)
    def _():
        to_partner(0, a_ref, rf.at[0]).start()

    def split(value):
        high = value.astype(jnp.bfloat16)
        return high, (value - high.astype(jnp.float32)).astype(jnp.bfloat16)

    def split_g(c):
        block = c // 2
        rows = rows_of(c, 0, CHUNK)
        high, low = split(g[block, rows, :])
        ghi[block, rows, :] = high
        glo[block, rows, :] = low

    def split_r(n, value):
        high, low = split(value)
        rhi[n] = high
        rlo[n] = low

    for cls, chunk in enumerate((gy, opposite)):
        class_r = chunk // 2
        for e in range(ENTRIES):
            s, col, valid, rowwise, row_tile, col_tile = entry_of(e, gx, class_r)
            owner = owner_smem[row_tile * (row_tile + 1) // 2 + col_tile] % PLANE
            target_tab[cls * ENTRIES + e] = owner if valid is None else jnp.where(valid, owner, -1)
            diag = jnp.where(row_tile == col_tile, 2, 0)
            step = s + STEPS * cls
            entry_tab[cls * ENTRIES + e] = step * 32 + col * 4 + diag + jnp.where(rowwise, 1, 0)

    def served(n, cls):
        du = jnp.int32(0)
        dv = jnp.int32(0)
        for m, (one, two) in enumerate(ORDER):
            du = jnp.where(n == m, one, du)
            dv = jnp.where(n == m, two, dv)
        side = jnp.where((u + 2 * cls) % SIDE < 2, 1, 3)
        return at(du, jnp.where(dv == 9, side, dv))

    def fill(p, carry):
        to = served(p // 2, p % 2)
        base = p % 2 * ENTRIES
        kept = [jnp.int32(0)] * CAP
        for e in range(ENTRIES):
            hit = target_tab[base + e] == to
            fresh = entry_tab[base + e]
            kept = [jnp.where(hit, b, a) for a, b in zip(kept, [fresh] + kept[:-1])]
        for k in range(CAP):
            send_tab[p * CAP + k] = kept[k]
        return carry

    split_r(0, a_ref[...])
    block, rows = me // 2, rows_of(me, 0, CHUNK)
    ghi[block, rows, :] = rhi[0]
    glo[block, rows, :] = rlo[0]

    def take_v(n):
        for d in (0, 1):
            b1[n][d][1].wait_recv()
            split_g(at(offs[n], -1 + 2 * d))

    def take_far(n):
        for d in (0, 1):
            b2[n][d].wait_recv()
        split_g(at(offs[n], 2))

    for d in (0, 1):
        a1[d][0].wait_recv()
        start(a2[d])
    for d in (0, 1):
        a1[d][1].wait_recv()
        start(b1[0][d][0])
    for d in (0, 1):
        split_g(at(-1 + 2 * d, 0))
    for d in (0, 1):
        a2[d].wait_recv()
        start(b1[3][d][0])
    for d in (0, 1):
        b1[0][d][0].wait_recv()
        start(b1[0][d][1])
    split_g(at(2, 0))
    for d in (0, 1):
        b1[3][d][0].wait_recv()
        start(b2[3][d])
    for d in (0, 1):
        b1[0][d][1].wait_recv()
        start(b2[0][d])
        start(b1[1][d][0])
        start(b1[2][d][0])
    for d in (0, 1):
        split_g(at(0, -1 + 2 * d))
    for d in (0, 1):
        b2[3][d].wait_recv()
    start(q_near)
    start(q_far)

    @pl.when(core == 0)
    def _():
        to_partner(2, whole(opposite), qf.at[0]).start()

    for n in (3, 1, 2):
        for d in (0, 1):
            start(b1[n][d][1])
    split_g(opposite)
    high, low = split(whole(opposite)[...])
    rhi[STEPS] = high
    rlo[STEPS] = low
    z_near.wait_recv()

    @pl.when(core == 0)
    def _():
        to_partner(1, rf.at[1], rf.at[2]).start()

    @pl.when(core == 1)
    def _():
        to_partner(0, rf.at[1], rf.at[0]).start()

    split_r(2, rf[1])
    z_far.wait_recv()

    @pl.when(core == 1)
    def _():
        to_partner(1, rf.at[3], rf.at[2]).start()

    split_r(4, rf[3])
    lax.fori_loop(0, PIECES, fill, 0)

    for load in loads[1:]:
        load.wait()
    mine = owner_ref[...] == gx * PLANE + gy
    slots = table_ref.shape[0]

    def find(q, carry):
        hit = jnp.logical_and(mine, slot_ref[...] == q)
        found = jnp.max(jnp.where(hit, code_ref[...], -1))
        row_tile = jnp.maximum(found, 0) // TILE_COUNT
        col_tile = jnp.maximum(found, 0) % TILE_COUNT
        group_a, inner_i = row_tile // HALF_TILES, row_tile % HALF_TILES
        group_b, inner_j = col_tile // HALF_TILES, col_tile % HALF_TILES
        gap = group_a - group_b
        even = (inner_i + inner_j) % 2 == 0
        across = jnp.logical_or(gap > GROUPS // 2, jnp.logical_and(gap == GROUPS // 2, even))
        within = inner_i - inner_j < HALF_TILES // 2
        rowwise = jnp.logical_or(jnp.logical_and(gap == 0, within), jnp.logical_and(gap > 0, across))
        class_r = jnp.where(rowwise, inner_i, inner_j)
        col = jnp.where(rowwise, inner_j, inner_i)
        s = (gx - jnp.where(rowwise, group_a, group_b) + GROUPS) % GROUPS
        place = s * HALF_TILES + jnp.where(s == 0, (class_r - col + HALF_TILES) % HALF_TILES, col)
        found_tab[q] = jnp.where(found >= 0, class_r * 64 + place, -1)
        table_ref[q] = jnp.where(found >= 0, jnp.where(rowwise, 1, 2), 0) + class_r * 4
        return carry

    lax.fori_loop(0, slots, find, 0)

    def count(q, carry):
        own = found_tab[q]
        later = jnp.int32(0)
        for other in range(slots):
            code = found_tab[other]
            same = jnp.logical_and(code // 64 == own // 64, code > own)
            later = later + jnp.where(same, 1, 0)
        table_ref[q] = table_ref[q] + 32 * jnp.minimum(later, CAP - 1)
        return carry

    for n in (1, 2):
        for d in (0, 1):
            b1[n][d][0].wait_recv()
            start(b2[n][d])
    lax.fori_loop(0, slots, count, 0)
    take_far(0)
    p_of[0].wait_recv()
    split_r(1, rf[0])
    p_of[1].wait_recv()
    split_r(3, rf[2])
    take_v(3)
    q_near.wait_recv()

    @pl.when(core == 0)
    def _():
        to_partner(3, qf.at[1], qf.at[2]).start()

    @pl.when(core == 1)
    def _():
        to_partner(2, qf.at[1], qf.at[0]).start()

    split_r(STEPS + 2, qf[1])
    take_v(1)
    take_v(2)
    p_of[2].wait_recv()
    split_r(STEPS + 1, qf[0])
    take_far(1)
    take_far(2)
    q_far.wait_recv()

    @pl.when(core == 1)
    def _():
        to_partner(3, qf.at[3], qf.at[2]).start()

    split_r(STEPS + 4, qf[3])
    p_of[3].wait_recv()
    split_r(STEPS + 3, qf[2])

    row_in = lax.broadcasted_iota(jnp.int32, (CHUNK, TILE), 0)
    col_in = lax.broadcasted_iota(jnp.int32, (CHUNK, TILE), 1)

    def dot(p, q):
        return lax.dot_general(p, q, (((1,), (1,)), ((), ())), preferred_element_type=jnp.float32)

    def one_piece(i, carry):
        k = i // PIECES
        p = i % PIECES
        to = served(p // 2, p % 2)
        chunk = jnp.where(p % 2 == 0, gy, opposite)
        entry = send_tab[p * CAP + k]
        s = entry // 32
        j = entry // 4 % HALF_TILES
        rh = rhi[s]
        gh = ghi[j]
        value = dot(rh, gh) + dot(rh, glo[j]) + dot(rlo[s], gh)
        upper = row_in + chunk % 2 * CHUNK < col_in
        masked = jnp.logical_and(upper, entry // 2 % 2 > 0)
        value = jnp.where(masked, jnp.float32(0.0), value)
        rowwise = jnp.full((CHUNK, CHUNK), entry % 2, jnp.int32) > 0
        for c in range(2):
            part = value[:, c * CHUNK:(c + 1) * CHUNK]
            outs[p, k, c] = jnp.where(rowwise, part, part.T)

        @pl.when(p < PIECES - 2)
        def _():
            remote(
                outs.at[p, k], in_ref.at[chunk, k], x_send.at[p, k], x_recv.at[chunk, k], gx, to
            ).start()

        return carry

    lax.fori_loop(0, PIECES * CAP, one_piece, 0)
    local = [
        pltpu.make_async_copy(outs.at[PIECES - 2 + n], in_ref.at[c], l_sem.at[n])
        for n, c in enumerate((gy, opposite))
    ]
    for copy in local:
        copy.start()
    for copy in copies + p_of:
        copy.wait_send()
    for copy in local:
        copy.wait()

    def sent(i, carry):
        remote(
            outs.at[i // CAP, i % CAP], in_ref.at[0, 0], x_send.at[i // CAP, i % CAP], x_recv.at[0, 0], ahead, gy
        ).wait_send()
        return carry

    lax.fori_loop(0, (PIECES - 2) * CAP, sent, 0)

    def arrived(i, carry):
        du = i // CAP // SIDE
        dv = i // CAP % SIDE
        chunk = at(du, dv)

        @pl.when(jnp.logical_or(du != dv, du % 2 > 0))
        def _():
            remote(
                outs.at[0, 0], in_ref.at[chunk, i % CAP], x_send.at[0, 0], x_recv.at[chunk, i % CAP], ahead, gy
            ).wait_recv()

        return carry

    lax.fori_loop(0, PLANE * CAP, arrived, 0)


def exchange(matrix_rows, tile_owner, tile_slot, slots):
    rows, width = matrix_rows.shape
    count = tile_owner.shape[0]
    lower_i, lower_j = np.tril_indices(TILE_COUNT)
    code = jnp.asarray(lower_i * TILE_COUNT + lower_j, jnp.int32)
    smem = pl.BlockSpec(memory_space=pltpu.SMEM)
    hbm = pl.BlockSpec(memory_space=pl.ANY)
    dma = pltpu.SemaphoreType.DMA
    return pl.pallas_call(
        exchange_kernel,
        out_shape=(
            jax.ShapeDtypeStruct((PLANE, CAP, 2, CHUNK, CHUNK), jnp.float32),
            jax.ShapeDtypeStruct((slots,), jnp.int32),
        ),
        in_specs=[smem, hbm, hbm, hbm, hbm],
        out_specs=(hbm, smem),
        scratch_shapes=[
            pltpu.VMEM((rows, width), jnp.float32),
            pltpu.VMEM((count,), jnp.int32),
            pltpu.VMEM((count,), jnp.int32),
            pltpu.VMEM((count,), jnp.int32),
            pltpu.VMEM((HALF_TILES, TILE, width), jnp.float32),
            pltpu.VMEM((HALF_TILES, TILE, width), jnp.bfloat16),
            pltpu.VMEM((HALF_TILES, TILE, width), jnp.bfloat16),
            pltpu.VMEM((4, CHUNK, width), jnp.float32),
            pltpu.VMEM((4, CHUNK, width), jnp.float32),
            pltpu.VMEM((2 * STEPS, CHUNK, width), jnp.bfloat16),
            pltpu.VMEM((2 * STEPS, CHUNK, width), jnp.bfloat16),
            pltpu.VMEM((PIECES, CAP, 2, CHUNK, CHUNK), jnp.float32),
            pltpu.SMEM((2 * ENTRIES,), jnp.int32),
            pltpu.SMEM((2 * ENTRIES,), jnp.int32),
            pltpu.SMEM((PIECES * CAP,), jnp.int32),
            pltpu.SMEM((slots,), jnp.int32),
            dma((2, 2)), dma((2, 2)), dma((2,)), dma((2,)),
            dma((4, 2, 2)), dma((4, 2, 2)), dma((4, 2)), dma((4, 2)),
            dma((2,)), dma((2,)), dma((4,)), dma((4,)), dma((2,)), dma((2,)),
            dma((PIECES, CAP)), dma((PLANE, CAP)), dma((4,)),
        ],
        compiler_params=pltpu.CompilerParams(
            collective_id=0, has_side_effects=True, vmem_limit_bytes=56 * 1024 * 1024
        ),
        name="exchange",
    )(tile_owner, tile_owner, tile_slot, code, matrix_rows)


def assemble_kernel(table, in_ref, out_ref, tiles, in_sem, out_sem):
    slots = tiles.shape[0]

    def pieces(q, act):
        entry = table[q]
        across = entry % 4 == 1
        source = entry // 4 % HALF_TILES * 2
        rank = entry // 32
        for h in range(2):
            for c in range(2):
                row = pl.multiple_of(jnp.where(across, h, c) * CHUNK, CHUNK)
                col = pl.multiple_of(jnp.where(across, c, h) * CHUNK, CHUNK)
                act(pltpu.make_async_copy(
                    in_ref.at[source + h, rank, c],
                    tiles.at[q, pl.ds(row, CHUNK), pl.ds(col, CHUNK)],
                    in_sem.at[q, 2 * h + c],
                ))

    def fetch(q, carry):
        present = table[q] % 4 > 0

        @pl.when(present)
        def _():
            pieces(q, lambda copy: copy.start())

        @pl.when(jnp.logical_not(present))
        def _():
            tiles[q] = jnp.zeros((TILE, TILE), jnp.float32)

        return carry

    def put(q, carry):
        @pl.when(table[q] % 4 > 0)
        def _():
            pieces(q, lambda copy: copy.wait())

        pltpu.make_async_copy(tiles.at[q], out_ref.at[q], out_sem.at[q]).start()
        return carry

    def finish(q, carry):
        pltpu.make_async_copy(tiles.at[q], out_ref.at[q], out_sem.at[q]).wait()
        return carry

    lax.fori_loop(0, slots, fetch, 0)
    lax.fori_loop(0, slots, put, 0)
    lax.fori_loop(0, slots, finish, 0)


def assemble(table, incoming):
    slots = table.shape[0]
    return pl.pallas_call(
        assemble_kernel,
        out_shape=jax.ShapeDtypeStruct((slots, TILE, TILE), jnp.float32),
        in_specs=[pl.BlockSpec(memory_space=pltpu.SMEM), pl.BlockSpec(memory_space=pl.ANY)],
        out_specs=pl.BlockSpec(memory_space=pl.ANY),
        scratch_shapes=[
            pltpu.VMEM((slots, TILE, TILE), jnp.float32),
            pltpu.SemaphoreType.DMA((slots, 4)),
            pltpu.SemaphoreType.DMA((slots,)),
        ],
        name="assemble",
    )(table, incoming)


def per_device(matrix_rows, tile_owner, tile_slot):
    devices = GROUPS * PLANE
    slots = (tile_owner.shape[0] + devices - 1) // devices
    incoming, table = exchange(matrix_rows, tile_owner, tile_slot, slots)
    return assemble(table, incoming)


def solution(mesh):
    placed = (P(("gx", "gy"), None), P(), P())
    return jax.shard_map(
        per_device,
        mesh=mesh,
        in_specs=placed,
        out_specs=P(("gx", "gy"), None, None),
        check_vma=False,
    )
```

```python
import jax
import jax.numpy as jnp
import numpy as np
from jax import lax
from jax.experimental import pallas as pl
from jax.experimental.pallas import tpu as pltpu
from jax.sharding import PartitionSpec as P

MESH = pl.DeviceIdType.MESH
SIDE = 4
PLANE = SIDE * SIDE
GROUPS = 8
HALF_TILES = 8
STEPS = 5
CAP = 3
CHUNK = 128
HALF = CHUNK // 2
TILE = 256
TILE_COUNT = 64
ENTRIES = 33
ORDER = ((2, 0), (0, 1), (1, 9), (0, 3), (3, 9), (1, 0), (3, 0), (0, 0))
SERVED = len(ORDER)
PIECES = 2 * SERVED


def entry_of(e, gx, r):
    quarter = HALF_TILES // 2
    middle = GROUPS // 2 - 1
    if e <= quarter:
        s, col = 0, (r - e + HALF_TILES) % HALF_TILES
        valid = r < quarter if e == quarter else None
        rowwise = col <= r
        source = gx
    elif e <= quarter + middle * HALF_TILES:
        s, col = 1 + (e - quarter - 1) // HALF_TILES, (e - quarter - 1) % HALF_TILES
        valid = None
        source = (gx - s + GROUPS) % GROUPS
        rowwise = source > gx
    else:
        s = middle + 1
        last = e - quarter - 1 - middle * HALF_TILES
        col = 2 * last + (r + jnp.where(gx >= GROUPS // 2, 1, 0)) % 2
        valid = None
        source = (gx - s + GROUPS) % GROUPS
        rowwise = source > gx
    near = source * HALF_TILES + r
    far = gx * HALF_TILES + col
    row_tile = jnp.where(rowwise, near, far)
    col_tile = jnp.where(rowwise, far, near)
    return s, col, valid, rowwise, row_tile, col_tile


def exchange_kernel(
    owner_smem, owner_any, slot_any, code_any, a_any, in_ref, table_ref,
    a_ref, owner_ref, slot_ref, code_ref,
    g, ghi, glo, rf, qf, rhi, rlo, outs, target_tab, entry_tab, send_tab, found_tab,
    a1_send, a1_recv, a2_send, a2_recv, b1_send, b1_recv, b2_send, b2_recv,
    z_send, z_recv, p_send, p_recv, q_send, q_recv, x_send, x_recv, l_sem,
):
    gx = lax.axis_index("gx")
    gy = lax.axis_index("gy")
    core = gx % 2
    y = gy // SIDE
    x = gy % SIDE
    u = jnp.where(core == 0, x, y)
    v = jnp.where(core == 0, y, x)
    stride_u = jnp.where(core == 0, 1, SIDE)
    stride_v = jnp.where(core == 0, SIDE, 1)

    def at(du, dv):
        return (u + du + SIDE) % SIDE * stride_u + (v + dv + SIDE) % SIDE * stride_v

    ahead = (gx + 2) % GROUPS
    behind = (gx + 6) % GROUPS
    beyond = (gx + 4) % GROUPS
    partner = gx + 1 - 2 * core

    loads = [
        pltpu.make_async_copy(src, dst, l_sem.at[n])
        for n, (src, dst) in enumerate(
            ((a_any, a_ref), (owner_any, owner_ref), (slot_any, slot_ref), (code_any, code_ref))
        )
    ]
    for load in loads:
        load.start()

    barrier = pltpu.get_barrier_semaphore()
    for du, dv in ((1, 0), (3, 0), (0, 1), (0, 3)):
        pl.semaphore_signal(
            barrier, inc=1, device_id={"gx": gx, "gy": at(du, dv)}, device_id_type=MESH
        )
    for other in (ahead, behind, beyond, partner):
        pl.semaphore_signal(barrier, inc=1, device_id={"gx": other, "gy": gy}, device_id_type=MESH)
    loads[0].wait()
    pl.semaphore_wait(barrier, 8)

    def rows_of(c, h, size):
        return pl.ds(pl.multiple_of(c % 2 * CHUNK + h * HALF, HALF), size)

    def half(c, h):
        return g.at[c // 2, rows_of(c, h, HALF)]

    def whole(c):
        return g.at[c // 2, rows_of(c, 0, CHUNK)]

    def own_half(h):
        return a_ref.at[pl.ds(h * HALF, HALF)]

    def remote(src, dst, send, recv, to_gx, to_gy):
        return pltpu.make_async_remote_copy(
            src_ref=src, dst_ref=dst, send_sem=send, recv_sem=recv,
            device_id={"gx": to_gx, "gy": to_gy}, device_id_type=MESH,
        )

    copies = []

    def start(copy):
        copy.start()
        copies.append(copy)

    me = gy
    a1 = [[
        remote(own_half(h), half(me, h), a1_send.at[d, p], a1_recv.at[d, p], gx, at(1 - 2 * d, 0))
        for p, h in enumerate((d, 1 - d))
    ] for d in (0, 1)]
    a2 = [
        remote(
            half(at(-1 + 2 * d, 0), d), half(at(-1 + 2 * d, 0), d),
            a2_send.at[d], a2_recv.at[d], gx, at(1 - 2 * d, 0),
        )
        for d in (0, 1)
    ]
    offs = (0, -1, 1, 2)
    b1 = [[[
        remote(
            own_half(h) if n == 0 else half(at(du, 0), h), half(at(du, 0), h),
            b1_send.at[n, d, p], b1_recv.at[n, d, p], gx, at(0, 1 - 2 * d),
        )
        for p, h in enumerate((d, 1 - d))
    ] for d in (0, 1)] for n, du in enumerate(offs)]
    b2 = [[
        remote(
            half(at(du, -1 + 2 * d), d), half(at(du, -1 + 2 * d), d),
            b2_send.at[n, d], b2_recv.at[n, d], gx, at(0, 1 - 2 * d),
        )
        for d in (0, 1)
    ] for n, du in enumerate(offs)]

    def along_z(n, src, dst, to):
        return remote(src, dst, z_send.at[n], z_recv.at[n], to, gy)

    z_near = along_z(0, a_ref, rf.at[1], ahead)
    z_far = along_z(1, a_ref, rf.at[3], beyond)

    def along_q(n, src, dst, to):
        return remote(src, dst, q_send.at[n], q_recv.at[n], to, gy)

    opposite = at(2, 2)
    q_near = along_q(0, whole(opposite), qf.at[1], ahead)
    q_far = along_q(1, whole(opposite), qf.at[3], beyond)

    def to_partner(n, src, dst):
        return remote(src, dst, p_send.at[n], p_recv.at[n], partner, gy)

    p_of = [to_partner(n, a_ref, dst) for n, dst in enumerate((rf.at[0], rf.at[2], qf.at[0], qf.at[2]))]

    for p in (0, 1):
        for d in (0, 1):
            start(a1[d][p])
    for p in (0, 1):
        for d in (0, 1):
            start(b1[0][d][p])
    start(z_near)
    start(z_far)

    @pl.when(core == 0)
    def _():
        to_partner(0, a_ref, rf.at[0]).start()

    def split(value):
        high = value.astype(jnp.bfloat16)
        return high, (value - high.astype(jnp.float32)).astype(jnp.bfloat16)

    def split_g(c):
        block = c // 2
        rows = rows_of(c, 0, CHUNK)
        high, low = split(g[block, rows, :])
        ghi[block, rows, :] = high
        glo[block, rows, :] = low

    def split_r(n, value):
        high, low = split(value)
        rhi[n] = high
        rlo[n] = low

    for cls, chunk in enumerate((gy, opposite)):
        class_r = chunk // 2
        for e in range(ENTRIES):
            s, col, valid, rowwise, row_tile, col_tile = entry_of(e, gx, class_r)
            owner = owner_smem[row_tile * (row_tile + 1) // 2 + col_tile] % PLANE
            target_tab[cls * ENTRIES + e] = owner if valid is None else jnp.where(valid, owner, -1)
            diag = jnp.where(row_tile == col_tile, 2, 0)
            step = s + STEPS * cls
            entry_tab[cls * ENTRIES + e] = step * 32 + col * 4 + diag + jnp.where(rowwise, 1, 0)

    def served(n, cls):
        du = jnp.int32(0)
        dv = jnp.int32(0)
        for m, (one, two) in enumerate(ORDER):
            du = jnp.where(n == m, one, du)
            dv = jnp.where(n == m, two, dv)
        side = jnp.where((u + 2 * cls) % SIDE < 2, 1, 3)
        return at(du, jnp.where(dv == 9, side, dv))

    def fill(p, carry):
        to = served(p // 2, p % 2)
        base = p % 2 * ENTRIES
        kept = [jnp.int32(0)] * CAP
        for e in range(ENTRIES):
            hit = target_tab[base + e] == to
            fresh = entry_tab[base + e]
            kept = [jnp.where(hit, b, a) for a, b in zip(kept, [fresh] + kept[:-1])]
        for k in range(CAP):
            send_tab[p * CAP + k] = kept[k]
        return carry

    lax.fori_loop(0, PIECES, fill, 0)
    split_r(0, a_ref[...])
    block, rows = me // 2, rows_of(me, 0, CHUNK)
    ghi[block, rows, :] = rhi[0]
    glo[block, rows, :] = rlo[0]

    for load in loads[1:]:
        load.wait()
    mine = owner_ref[...] == gx * PLANE + gy
    slots = table_ref.shape[0]

    def find(q, carry):
        hit = jnp.logical_and(mine, slot_ref[...] == q)
        found = jnp.max(jnp.where(hit, code_ref[...], -1))
        row_tile = jnp.maximum(found, 0) // TILE_COUNT
        col_tile = jnp.maximum(found, 0) % TILE_COUNT
        group_a, inner_i = row_tile // HALF_TILES, row_tile % HALF_TILES
        group_b, inner_j = col_tile // HALF_TILES, col_tile % HALF_TILES
        gap = group_a - group_b
        even = (inner_i + inner_j) % 2 == 0
        across = jnp.logical_or(gap > GROUPS // 2, jnp.logical_and(gap == GROUPS // 2, even))
        within = inner_i - inner_j < HALF_TILES // 2
        rowwise = jnp.logical_or(jnp.logical_and(gap == 0, within), jnp.logical_and(gap > 0, across))
        class_r = jnp.where(rowwise, inner_i, inner_j)
        col = jnp.where(rowwise, inner_j, inner_i)
        s = (gx - jnp.where(rowwise, group_a, group_b) + GROUPS) % GROUPS
        place = s * HALF_TILES + jnp.where(s == 0, (class_r - col + HALF_TILES) % HALF_TILES, col)
        found_tab[q] = jnp.where(found >= 0, class_r * 64 + place, -1)
        table_ref[q] = jnp.where(found >= 0, jnp.where(rowwise, 1, 2), 0) + class_r * 4
        return carry

    def count(q, carry):
        own = found_tab[q]
        later = jnp.int32(0)
        for other in range(slots):
            code = found_tab[other]
            same = jnp.logical_and(code // 64 == own // 64, code > own)
            later = later + jnp.where(same, 1, 0)
        table_ref[q] = table_ref[q] + 32 * jnp.minimum(later, CAP - 1)
        return carry

    def take_v(n):
        for d in (0, 1):
            b1[n][d][1].wait_recv()
            split_g(at(offs[n], -1 + 2 * d))

    def take_far(n):
        for d in (0, 1):
            b2[n][d].wait_recv()
        split_g(at(offs[n], 2))

    for d in (0, 1):
        a1[d][0].wait_recv()
        start(a2[d])
    for d in (0, 1):
        a1[d][1].wait_recv()
    for p in (0, 1):
        for d in (0, 1):
            start(b1[1][d][p])
    for d in (0, 1):
        split_g(at(-1 + 2 * d, 0))
    for d in (0, 1):
        a2[d].wait_recv()
        start(b1[3][d][0])
    for d in (0, 1):
        start(b1[3][d][1])
    for d in (0, 1):
        b1[0][d][0].wait_recv()
        start(b2[0][d])
    split_g(at(2, 0))
    for d in (0, 1):
        b1[3][d][0].wait_recv()
        start(b2[3][d])
    for p in (0, 1):
        for d in (0, 1):
            start(b1[2][d][p])
    for d in (0, 1):
        b1[1][d][0].wait_recv()
        start(b2[1][d])
    z_near.wait_recv()

    @pl.when(core == 0)
    def _():
        to_partner(1, rf.at[1], rf.at[2]).start()

    @pl.when(core == 1)
    def _():
        to_partner(0, rf.at[1], rf.at[0]).start()

    take_v(0)
    split_r(2, rf[1])
    z_far.wait_recv()

    @pl.when(core == 1)
    def _():
        to_partner(1, rf.at[3], rf.at[2]).start()

    split_r(4, rf[3])
    take_far(0)
    for d in (0, 1):
        b2[3][d].wait_recv()
    start(q_near)
    start(q_far)

    @pl.when(core == 0)
    def _():
        to_partner(2, whole(opposite), qf.at[0]).start()

    for d in (0, 1):
        b1[2][d][0].wait_recv()
        start(b2[2][d])
    split_g(opposite)
    high, low = split(whole(opposite)[...])
    rhi[STEPS] = high
    rlo[STEPS] = low
    lax.fori_loop(0, slots, find, 0)
    take_v(1)
    take_v(3)
    p_of[0].wait_recv()
    split_r(1, rf[0])
    p_of[1].wait_recv()
    split_r(3, rf[2])
    lax.fori_loop(0, slots, count, 0)
    take_v(2)
    take_far(1)
    take_far(2)

    row_in = lax.broadcasted_iota(jnp.int32, (CHUNK, TILE), 0)
    col_in = lax.broadcasted_iota(jnp.int32, (CHUNK, TILE), 1)

    def dot(p, q):
        return lax.dot_general(p, q, (((1,), (1,)), ((), ())), preferred_element_type=jnp.float32)

    def one_piece(i, carry):
        k = i // SERVED % CAP
        p = i % SERVED * 2 + i // (SERVED * CAP)
        to = served(p // 2, p % 2)
        chunk = jnp.where(p % 2 == 0, gy, opposite)
        entry = send_tab[p * CAP + k]
        s = entry // 32
        j = entry // 4 % HALF_TILES
        rh = rhi[s]
        gh = ghi[j]
        value = dot(rh, gh) + dot(rh, glo[j]) + dot(rlo[s], gh)
        upper = row_in + chunk % 2 * CHUNK < col_in
        masked = jnp.logical_and(upper, entry // 2 % 2 > 0)
        value = jnp.where(masked, jnp.float32(0.0), value)
        rowwise = jnp.full((CHUNK, CHUNK), entry % 2, jnp.int32) > 0
        for c in range(2):
            part = value[:, c * CHUNK:(c + 1) * CHUNK]
            outs[p, k, c] = jnp.where(rowwise, part, part.T)

        @pl.when(p < PIECES - 2)
        def _():
            remote(
                outs.at[p, k], in_ref.at[chunk, k], x_send.at[p, k], x_recv.at[chunk, k], gx, to
            ).start()

        return carry

    lax.fori_loop(0, SERVED, one_piece, 0)
    q_near.wait_recv()

    @pl.when(core == 0)
    def _():
        to_partner(3, qf.at[1], qf.at[2]).start()

    @pl.when(core == 1)
    def _():
        to_partner(2, qf.at[1], qf.at[0]).start()

    split_r(STEPS + 2, qf[1])
    lax.fori_loop(SERVED, SERVED * CAP, one_piece, 0)
    q_far.wait_recv()

    @pl.when(core == 1)
    def _():
        to_partner(3, qf.at[3], qf.at[2]).start()

    split_r(STEPS + 4, qf[3])
    p_of[2].wait_recv()
    split_r(STEPS + 1, qf[0])
    p_of[3].wait_recv()
    split_r(STEPS + 3, qf[2])
    lax.fori_loop(SERVED * CAP, PIECES * CAP, one_piece, 0)
    local = [
        pltpu.make_async_copy(outs.at[PIECES - 2 + n], in_ref.at[c], l_sem.at[n])
        for n, c in enumerate((gy, opposite))
    ]
    for copy in local:
        copy.start()
    for copy in copies + p_of:
        copy.wait_send()
    for copy in local:
        copy.wait()

    def sent(i, carry):
        remote(
            outs.at[i // CAP, i % CAP], in_ref.at[0, 0], x_send.at[i // CAP, i % CAP], x_recv.at[0, 0], ahead, gy
        ).wait_send()
        return carry

    lax.fori_loop(0, (PIECES - 2) * CAP, sent, 0)

    def arrived(i, carry):
        du = i // CAP // SIDE
        dv = i // CAP % SIDE
        chunk = at(du, dv)

        @pl.when(jnp.logical_or(du != dv, du % 2 > 0))
        def _():
            remote(
                outs.at[0, 0], in_ref.at[chunk, i % CAP], x_send.at[0, 0], x_recv.at[chunk, i % CAP], ahead, gy
            ).wait_recv()

        return carry

    lax.fori_loop(0, PLANE * CAP, arrived, 0)


def exchange(matrix_rows, tile_owner, tile_slot, slots):
    rows, width = matrix_rows.shape
    count = tile_owner.shape[0]
    lower_i, lower_j = np.tril_indices(TILE_COUNT)
    code = jnp.asarray(lower_i * TILE_COUNT + lower_j, jnp.int32)
    smem = pl.BlockSpec(memory_space=pltpu.SMEM)
    hbm = pl.BlockSpec(memory_space=pl.ANY)
    dma = pltpu.SemaphoreType.DMA
    return pl.pallas_call(
        exchange_kernel,
        out_shape=(
            jax.ShapeDtypeStruct((PLANE, CAP, 2, CHUNK, CHUNK), jnp.float32),
            jax.ShapeDtypeStruct((slots,), jnp.int32),
        ),
        in_specs=[smem, hbm, hbm, hbm, hbm],
        out_specs=(hbm, smem),
        scratch_shapes=[
            pltpu.VMEM((rows, width), jnp.float32),
            pltpu.VMEM((count,), jnp.int32),
            pltpu.VMEM((count,), jnp.int32),
            pltpu.VMEM((count,), jnp.int32),
            pltpu.VMEM((HALF_TILES, TILE, width), jnp.float32),
            pltpu.VMEM((HALF_TILES, TILE, width), jnp.bfloat16),
            pltpu.VMEM((HALF_TILES, TILE, width), jnp.bfloat16),
            pltpu.VMEM((4, CHUNK, width), jnp.float32),
            pltpu.VMEM((4, CHUNK, width), jnp.float32),
            pltpu.VMEM((2 * STEPS, CHUNK, width), jnp.bfloat16),
            pltpu.VMEM((2 * STEPS, CHUNK, width), jnp.bfloat16),
            pltpu.VMEM((PIECES, CAP, 2, CHUNK, CHUNK), jnp.float32),
            pltpu.SMEM((2 * ENTRIES,), jnp.int32),
            pltpu.SMEM((2 * ENTRIES,), jnp.int32),
            pltpu.SMEM((PIECES * CAP,), jnp.int32),
            pltpu.SMEM((slots,), jnp.int32),
            dma((2, 2)), dma((2, 2)), dma((2,)), dma((2,)),
            dma((4, 2, 2)), dma((4, 2, 2)), dma((4, 2)), dma((4, 2)),
            dma((2,)), dma((2,)), dma((4,)), dma((4,)), dma((2,)), dma((2,)),
            dma((PIECES, CAP)), dma((PLANE, CAP)), dma((4,)),
        ],
        compiler_params=pltpu.CompilerParams(
            collective_id=0, has_side_effects=True, vmem_limit_bytes=56 * 1024 * 1024
        ),
        name="exchange",
    )(tile_owner, tile_owner, tile_slot, code, matrix_rows)


def assemble_kernel(table, in_ref, out_ref, tiles, in_sem, out_sem):
    slots = tiles.shape[0]

    def pieces(q, act):
        entry = table[q]
        across = entry % 4 == 1
        source = entry // 4 % HALF_TILES * 2
        rank = entry // 32
        for h in range(2):
            for c in range(2):
                row = pl.multiple_of(jnp.where(across, h, c) * CHUNK, CHUNK)
                col = pl.multiple_of(jnp.where(across, c, h) * CHUNK, CHUNK)
                act(pltpu.make_async_copy(
                    in_ref.at[source + h, rank, c],
                    tiles.at[q, pl.ds(row, CHUNK), pl.ds(col, CHUNK)],
                    in_sem.at[q, 2 * h + c],
                ))

    def fetch(q, carry):
        present = table[q] % 4 > 0

        @pl.when(present)
        def _():
            pieces(q, lambda copy: copy.start())

        @pl.when(jnp.logical_not(present))
        def _():
            tiles[q] = jnp.zeros((TILE, TILE), jnp.float32)

        return carry

    def put(q, carry):
        @pl.when(table[q] % 4 > 0)
        def _():
            pieces(q, lambda copy: copy.wait())

        pltpu.make_async_copy(tiles.at[q], out_ref.at[q], out_sem.at[q]).start()
        return carry

    def finish(q, carry):
        pltpu.make_async_copy(tiles.at[q], out_ref.at[q], out_sem.at[q]).wait()
        return carry

    lax.fori_loop(0, slots, fetch, 0)
    lax.fori_loop(0, slots, put, 0)
    lax.fori_loop(0, slots, finish, 0)


def assemble(table, incoming):
    slots = table.shape[0]
    return pl.pallas_call(
        assemble_kernel,
        out_shape=jax.ShapeDtypeStruct((slots, TILE, TILE), jnp.float32),
        in_specs=[pl.BlockSpec(memory_space=pltpu.SMEM), pl.BlockSpec(memory_space=pl.ANY)],
        out_specs=pl.BlockSpec(memory_space=pl.ANY),
        scratch_shapes=[
            pltpu.VMEM((slots, TILE, TILE), jnp.float32),
            pltpu.SemaphoreType.DMA((slots, 4)),
            pltpu.SemaphoreType.DMA((slots,)),
        ],
        name="assemble",
    )(table, incoming)


def per_device(matrix_rows, tile_owner, tile_slot):
    devices = GROUPS * PLANE
    slots = (tile_owner.shape[0] + devices - 1) // devices
    incoming, table = exchange(matrix_rows, tile_owner, tile_slot, slots)
    return assemble(table, incoming)


def solution(mesh):
    placed = (P(("gx", "gy"), None), P(), P())
    return jax.shard_map(
        per_device,
        mesh=mesh,
        in_specs=placed,
        out_specs=P(("gx", "gy"), None, None),
        check_vma=False,
    )
```

```python
import jax
import jax.numpy as jnp
import numpy as np
from jax import lax
from jax.experimental import pallas as pl
from jax.experimental.pallas import tpu as pltpu
from jax.sharding import PartitionSpec as P

MESH = pl.DeviceIdType.MESH
SIDE = 4
PLANE = SIDE * SIDE
GROUPS = 8
HALF_TILES = 8
STEPS = 5
CAP = 3
CHUNK = 128
HALF = CHUNK // 2
TILE = 256
TILE_COUNT = 64
ENTRIES = 33
ORDER = ((2, 0), (0, 1), (1, 9), (0, 3), (3, 9), (1, 0), (3, 0), (0, 0))
SERVED = len(ORDER)
PIECES = 2 * SERVED


def entry_of(e, gx, r):
    quarter = HALF_TILES // 2
    middle = GROUPS // 2 - 1
    if e <= quarter:
        s, col = 0, (r - e + HALF_TILES) % HALF_TILES
        valid = r < quarter if e == quarter else None
        rowwise = col <= r
        source = gx
    elif e <= quarter + middle * HALF_TILES:
        s, col = 1 + (e - quarter - 1) // HALF_TILES, (e - quarter - 1) % HALF_TILES
        valid = None
        source = (gx - s + GROUPS) % GROUPS
        rowwise = source > gx
    else:
        s = middle + 1
        last = e - quarter - 1 - middle * HALF_TILES
        col = 2 * last + (r + jnp.where(gx >= GROUPS // 2, 1, 0)) % 2
        valid = None
        source = (gx - s + GROUPS) % GROUPS
        rowwise = source > gx
    near = source * HALF_TILES + r
    far = gx * HALF_TILES + col
    row_tile = jnp.where(rowwise, near, far)
    col_tile = jnp.where(rowwise, far, near)
    return s, col, valid, rowwise, row_tile, col_tile


def exchange_kernel(
    owner_smem, owner_any, slot_any, code_any, a_any, in_ref, table_ref,
    a_ref, owner_ref, slot_ref, code_ref,
    g, ghi, glo, rf, qf, rhi, rlo, outs, target_tab, entry_tab, send_tab, found_tab,
    a1_send, a1_recv, a2_send, a2_recv, b1_send, b1_recv, b2_send, b2_recv,
    z_send, z_recv, p_send, p_recv, q_send, q_recv, x_send, x_recv, l_sem,
):
    gx = lax.axis_index("gx")
    gy = lax.axis_index("gy")
    core = gx % 2
    y = gy // SIDE
    x = gy % SIDE
    u = jnp.where(core == 0, x, y)
    v = jnp.where(core == 0, y, x)
    stride_u = jnp.where(core == 0, 1, SIDE)
    stride_v = jnp.where(core == 0, SIDE, 1)

    def at(du, dv):
        return (u + du + SIDE) % SIDE * stride_u + (v + dv + SIDE) % SIDE * stride_v

    ahead = (gx + 2) % GROUPS
    behind = (gx + 6) % GROUPS
    partner = gx + 1 - 2 * core

    loads = [
        pltpu.make_async_copy(src, dst, l_sem.at[n])
        for n, (src, dst) in enumerate(
            ((a_any, a_ref), (owner_any, owner_ref), (slot_any, slot_ref), (code_any, code_ref))
        )
    ]
    for load in loads:
        load.start()

    barrier = pltpu.get_barrier_semaphore()
    for du, dv in ((1, 0), (3, 0), (0, 1), (0, 3)):
        pl.semaphore_signal(
            barrier, inc=1, device_id={"gx": gx, "gy": at(du, dv)}, device_id_type=MESH
        )
    for other in (ahead, behind, partner):
        pl.semaphore_signal(barrier, inc=1, device_id={"gx": other, "gy": gy}, device_id_type=MESH)
    loads[0].wait()
    pl.semaphore_wait(barrier, 7)

    def rows_of(c, h, size):
        return pl.ds(pl.multiple_of(c % 2 * CHUNK + h * HALF, HALF), size)

    def half(c, h):
        return g.at[c // 2, rows_of(c, h, HALF)]

    def whole(c):
        return g.at[c // 2, rows_of(c, 0, CHUNK)]

    def part(ref, n, h):
        return ref.at[n, pl.ds(h * HALF, HALF)]

    def own_half(h):
        return a_ref.at[pl.ds(h * HALF, HALF)]

    def remote(src, dst, send, recv, to_gx, to_gy):
        return pltpu.make_async_remote_copy(
            src_ref=src, dst_ref=dst, send_sem=send, recv_sem=recv,
            device_id={"gx": to_gx, "gy": to_gy}, device_id_type=MESH,
        )

    copies = []

    def start(copy):
        copy.start()
        copies.append(copy)

    me = gy
    a1 = [[
        remote(own_half(h), half(me, h), a1_send.at[d, p], a1_recv.at[d, p], gx, at(1 - 2 * d, 0))
        for p, h in enumerate((d, 1 - d))
    ] for d in (0, 1)]
    a2 = [
        remote(
            half(at(-1 + 2 * d, 0), d), half(at(-1 + 2 * d, 0), d),
            a2_send.at[d], a2_recv.at[d], gx, at(1 - 2 * d, 0),
        )
        for d in (0, 1)
    ]
    offs = (0, -1, 1, 2)
    b1 = [[[
        remote(
            own_half(h) if n == 0 else half(at(du, 0), h), half(at(du, 0), h),
            b1_send.at[n, d, p], b1_recv.at[n, d, p], gx, at(0, 1 - 2 * d),
        )
        for p, h in enumerate((d, 1 - d))
    ] for d in (0, 1)] for n, du in enumerate(offs)]
    b2 = [[
        remote(
            half(at(du, -1 + 2 * d), d), half(at(du, -1 + 2 * d), d),
            b2_send.at[n, d], b2_recv.at[n, d], gx, at(0, 1 - 2 * d),
        )
        for d in (0, 1)
    ] for n, du in enumerate(offs)]

    def along_z(n, src, dst, to):
        return remote(src, dst, z_send.at[n], z_recv.at[n], to, gy)

    z_near = along_z(0, a_ref, rf.at[1], ahead)
    z_far = along_z(1, rf.at[1], rf.at[3], ahead)

    def along_q(n, src, dst, to):
        return remote(src, dst, q_send.at[n], q_recv.at[n], to, gy)

    opposite = at(2, 2)
    q_near = [along_q(h, half(opposite, h), part(qf, 1, h), ahead) for h in (0, 1)]
    q_far = [along_q(2 + h, part(qf, 1, h), part(qf, 3, h), ahead) for h in (0, 1)]

    def to_partner(n, src, dst):
        return remote(src, dst, p_send.at[n], p_recv.at[n], partner, gy)

    p_of = [to_partner(n, a_ref, dst) for n, dst in enumerate((rf.at[0], rf.at[2], qf.at[0], qf.at[2]))]

    for p in (0, 1):
        for d in (0, 1):
            start(a1[d][p])
    for p in (0, 1):
        for d in (0, 1):
            start(b1[0][d][p])
    start(z_near)

    @pl.when(core == 0)
    def _():
        to_partner(0, a_ref, rf.at[0]).start()

    def split(value):
        high = value.astype(jnp.bfloat16)
        return high, (value - high.astype(jnp.float32)).astype(jnp.bfloat16)

    def split_g(c):
        block = c // 2
        rows = rows_of(c, 0, CHUNK)
        high, low = split(g[block, rows, :])
        ghi[block, rows, :] = high
        glo[block, rows, :] = low

    def split_r(n, value):
        high, low = split(value)
        rhi[n] = high
        rlo[n] = low

    for cls, chunk in enumerate((gy, opposite)):
        class_r = chunk // 2
        for e in range(ENTRIES):
            s, col, valid, rowwise, row_tile, col_tile = entry_of(e, gx, class_r)
            owner = owner_smem[row_tile * (row_tile + 1) // 2 + col_tile] % PLANE
            target_tab[cls * ENTRIES + e] = owner if valid is None else jnp.where(valid, owner, -1)
            diag = jnp.where(row_tile == col_tile, 2, 0)
            step = s + STEPS * cls
            entry_tab[cls * ENTRIES + e] = step * 32 + col * 4 + diag + jnp.where(rowwise, 1, 0)

    def served(n, cls):
        du = jnp.int32(0)
        dv = jnp.int32(0)
        for m, (one, two) in enumerate(ORDER):
            du = jnp.where(n == m, one, du)
            dv = jnp.where(n == m, two, dv)
        side = jnp.where((u + 2 * cls) % SIDE < 2, 1, 3)
        return at(du, jnp.where(dv == 9, side, dv))

    def fill(p, carry):
        to = served(p // 2, p % 2)
        base = p % 2 * ENTRIES
        kept = [jnp.int32(0)] * CAP
        for e in range(ENTRIES):
            hit = target_tab[base + e] == to
            fresh = entry_tab[base + e]
            kept = [jnp.where(hit, b, a) for a, b in zip(kept, [fresh] + kept[:-1])]
        for k in range(CAP):
            send_tab[p * CAP + k] = kept[k]
        return carry

    lax.fori_loop(0, PIECES, fill, 0)
    split_r(0, a_ref[...])
    block, rows = me // 2, rows_of(me, 0, CHUNK)
    ghi[block, rows, :] = rhi[0]
    glo[block, rows, :] = rlo[0]

    for load in loads[1:]:
        load.wait()
    mine = owner_ref[...] == gx * PLANE + gy
    slots = table_ref.shape[0]

    def find(q, carry):
        hit = jnp.logical_and(mine, slot_ref[...] == q)
        found = jnp.max(jnp.where(hit, code_ref[...], -1))
        row_tile = jnp.maximum(found, 0) // TILE_COUNT
        col_tile = jnp.maximum(found, 0) % TILE_COUNT
        group_a, inner_i = row_tile // HALF_TILES, row_tile % HALF_TILES
        group_b, inner_j = col_tile // HALF_TILES, col_tile % HALF_TILES
        gap = group_a - group_b
        even = (inner_i + inner_j) % 2 == 0
        across = jnp.logical_or(gap > GROUPS // 2, jnp.logical_and(gap == GROUPS // 2, even))
        within = inner_i - inner_j < HALF_TILES // 2
        rowwise = jnp.logical_or(jnp.logical_and(gap == 0, within), jnp.logical_and(gap > 0, across))
        class_r = jnp.where(rowwise, inner_i, inner_j)
        col = jnp.where(rowwise, inner_j, inner_i)
        s = (gx - jnp.where(rowwise, group_a, group_b) + GROUPS) % GROUPS
        place = s * HALF_TILES + jnp.where(s == 0, (class_r - col + HALF_TILES) % HALF_TILES, col)
        found_tab[q] = jnp.where(found >= 0, class_r * 64 + place, -1)
        table_ref[q] = jnp.where(found >= 0, jnp.where(rowwise, 1, 2), 0) + class_r * 4
        return carry

    def count(q, carry):
        own = found_tab[q]
        later = jnp.int32(0)
        for other in range(slots):
            code = found_tab[other]
            same = jnp.logical_and(code // 64 == own // 64, code > own)
            later = later + jnp.where(same, 1, 0)
        table_ref[q] = table_ref[q] + 32 * jnp.minimum(later, CAP - 1)
        return carry

    def take_v(n):
        for d in (0, 1):
            b1[n][d][1].wait_recv()
            split_g(at(offs[n], -1 + 2 * d))

    def take_far(n):
        for d in (0, 1):
            b2[n][d].wait_recv()
        split_g(at(offs[n], 2))

    for d in (0, 1):
        a1[d][0].wait_recv()
        start(a2[d])
    for d in (0, 1):
        a1[d][1].wait_recv()
    for d in (0, 1):
        start(b1[1][d][0])
    for d in (0, 1):
        split_g(at(-1 + 2 * d, 0))
    for d in (0, 1):
        a2[d].wait_recv()
        start(b1[3][d][0])
    for d in (0, 1):
        b1[0][d][0].wait_recv()
        start(b2[0][d])
    for d in (0, 1):
        start(b1[3][d][1])
    split_g(at(2, 0))
    for d in (0, 1):
        b1[3][d][0].wait_recv()
        start(b2[3][d])
    for d in (0, 1):
        start(b1[1][d][1])
    for p in (0, 1):
        for d in (0, 1):
            start(b1[2][d][p])
    for d in (0, 1):
        b1[1][d][0].wait_recv()
        start(b2[1][d])
    z_near.wait_recv()
    start(z_far)

    @pl.when(core == 0)
    def _():
        to_partner(1, rf.at[1], rf.at[2]).start()

    @pl.when(core == 1)
    def _():
        to_partner(0, rf.at[1], rf.at[0]).start()

    take_v(0)
    split_r(2, rf[1])
    z_far.wait_recv()

    @pl.when(core == 1)
    def _():
        to_partner(1, rf.at[3], rf.at[2]).start()

    split_r(4, rf[3])
    take_far(0)
    for d in (0, 1):
        b2[3][d].wait_recv()
    for h in (0, 1):
        start(q_near[h])

    @pl.when(core == 0)
    def _():
        to_partner(2, whole(opposite), qf.at[0]).start()

    for d in (0, 1):
        b1[2][d][0].wait_recv()
        start(b2[2][d])
    split_g(opposite)
    high, low = split(whole(opposite)[...])
    rhi[STEPS] = high
    rlo[STEPS] = low
    lax.fori_loop(0, slots, find, 0)
    take_v(1)
    take_v(3)
    p_of[0].wait_recv()
    split_r(1, rf[0])
    p_of[1].wait_recv()
    split_r(3, rf[2])
    lax.fori_loop(0, slots, count, 0)
    take_v(2)
    take_far(1)
    q_near[0].wait_recv()
    start(q_far[0])
    take_far(2)

    row_in = lax.broadcasted_iota(jnp.int32, (CHUNK, TILE), 0)
    col_in = lax.broadcasted_iota(jnp.int32, (CHUNK, TILE), 1)

    def dot(p, q):
        return lax.dot_general(p, q, (((1,), (1,)), ((), ())), preferred_element_type=jnp.float32)

    def one_piece(i, carry):
        k = i // SERVED % CAP
        p = i % SERVED * 2 + i // (SERVED * CAP)
        to = served(p // 2, p % 2)
        chunk = jnp.where(p % 2 == 0, gy, opposite)
        entry = send_tab[p * CAP + k]
        s = entry // 32
        j = entry // 4 % HALF_TILES
        rh = rhi[s]
        gh = ghi[j]
        value = dot(rh, gh) + dot(rh, glo[j]) + dot(rlo[s], gh)
        upper = row_in + chunk % 2 * CHUNK < col_in
        masked = jnp.logical_and(upper, entry // 2 % 2 > 0)
        value = jnp.where(masked, jnp.float32(0.0), value)
        rowwise = jnp.full((CHUNK, CHUNK), entry % 2, jnp.int32) > 0
        for c in range(2):
            part = value[:, c * CHUNK:(c + 1) * CHUNK]
            outs[p, k, c] = jnp.where(rowwise, part, part.T)

        @pl.when(p < PIECES - 2)
        def _():
            remote(
                outs.at[p, k], in_ref.at[chunk, k], x_send.at[p, k], x_recv.at[chunk, k], gx, to
            ).start()

        return carry

    lax.fori_loop(0, SERVED, one_piece, 0)
    q_near[1].wait_recv()
    start(q_far[1])

    @pl.when(core == 0)
    def _():
        to_partner(3, qf.at[1], qf.at[2]).start()

    @pl.when(core == 1)
    def _():
        to_partner(2, qf.at[1], qf.at[0]).start()

    split_r(STEPS + 2, qf[1])
    lax.fori_loop(SERVED, SERVED * CAP, one_piece, 0)
    for h in (0, 1):
        q_far[h].wait_recv()

    @pl.when(core == 1)
    def _():
        to_partner(3, qf.at[3], qf.at[2]).start()

    split_r(STEPS + 4, qf[3])
    p_of[2].wait_recv()
    split_r(STEPS + 1, qf[0])
    p_of[3].wait_recv()
    split_r(STEPS + 3, qf[2])
    lax.fori_loop(SERVED * CAP, PIECES * CAP, one_piece, 0)
    local = [
        pltpu.make_async_copy(outs.at[PIECES - 2 + n], in_ref.at[c], l_sem.at[n])
        for n, c in enumerate((gy, opposite))
    ]
    for copy in local:
        copy.start()
    for copy in copies + p_of:
        copy.wait_send()
    for copy in local:
        copy.wait()

    def sent(i, carry):
        remote(
            outs.at[i // CAP, i % CAP], in_ref.at[0, 0], x_send.at[i // CAP, i % CAP], x_recv.at[0, 0], ahead, gy
        ).wait_send()
        return carry

    lax.fori_loop(0, (PIECES - 2) * CAP, sent, 0)

    def arrived(i, carry):
        du = i // CAP // SIDE
        dv = i // CAP % SIDE
        chunk = at(du, dv)

        @pl.when(jnp.logical_or(du != dv, du % 2 > 0))
        def _():
            remote(
                outs.at[0, 0], in_ref.at[chunk, i % CAP], x_send.at[0, 0], x_recv.at[chunk, i % CAP], ahead, gy
            ).wait_recv()

        return carry

    lax.fori_loop(0, PLANE * CAP, arrived, 0)


def exchange(matrix_rows, tile_owner, tile_slot, slots):
    rows, width = matrix_rows.shape
    count = tile_owner.shape[0]
    lower_i, lower_j = np.tril_indices(TILE_COUNT)
    code = jnp.asarray(lower_i * TILE_COUNT + lower_j, jnp.int32)
    smem = pl.BlockSpec(memory_space=pltpu.SMEM)
    hbm = pl.BlockSpec(memory_space=pl.ANY)
    dma = pltpu.SemaphoreType.DMA
    return pl.pallas_call(
        exchange_kernel,
        out_shape=(
            jax.ShapeDtypeStruct((PLANE, CAP, 2, CHUNK, CHUNK), jnp.float32),
            jax.ShapeDtypeStruct((slots,), jnp.int32),
        ),
        in_specs=[smem, hbm, hbm, hbm, hbm],
        out_specs=(hbm, smem),
        scratch_shapes=[
            pltpu.VMEM((rows, width), jnp.float32),
            pltpu.VMEM((count,), jnp.int32),
            pltpu.VMEM((count,), jnp.int32),
            pltpu.VMEM((count,), jnp.int32),
            pltpu.VMEM((HALF_TILES, TILE, width), jnp.float32),
            pltpu.VMEM((HALF_TILES, TILE, width), jnp.bfloat16),
            pltpu.VMEM((HALF_TILES, TILE, width), jnp.bfloat16),
            pltpu.VMEM((4, CHUNK, width), jnp.float32),
            pltpu.VMEM((4, CHUNK, width), jnp.float32),
            pltpu.VMEM((2 * STEPS, CHUNK, width), jnp.bfloat16),
            pltpu.VMEM((2 * STEPS, CHUNK, width), jnp.bfloat16),
            pltpu.VMEM((PIECES, CAP, 2, CHUNK, CHUNK), jnp.float32),
            pltpu.SMEM((2 * ENTRIES,), jnp.int32),
            pltpu.SMEM((2 * ENTRIES,), jnp.int32),
            pltpu.SMEM((PIECES * CAP,), jnp.int32),
            pltpu.SMEM((slots,), jnp.int32),
            dma((2, 2)), dma((2, 2)), dma((2,)), dma((2,)),
            dma((4, 2, 2)), dma((4, 2, 2)), dma((4, 2)), dma((4, 2)),
            dma((2,)), dma((2,)), dma((4,)), dma((4,)), dma((4,)), dma((4,)),
            dma((PIECES, CAP)), dma((PLANE, CAP)), dma((4,)),
        ],
        compiler_params=pltpu.CompilerParams(
            collective_id=0, has_side_effects=True, vmem_limit_bytes=56 * 1024 * 1024
        ),
        name="exchange",
    )(tile_owner, tile_owner, tile_slot, code, matrix_rows)


def assemble_kernel(table, in_ref, out_ref, tiles, in_sem, out_sem):
    slots = tiles.shape[0]

    def pieces(q, act):
        entry = table[q]
        across = entry % 4 == 1
        source = entry // 4 % HALF_TILES * 2
        rank = entry // 32
        for h in range(2):
            for c in range(2):
                row = pl.multiple_of(jnp.where(across, h, c) * CHUNK, CHUNK)
                col = pl.multiple_of(jnp.where(across, c, h) * CHUNK, CHUNK)
                act(pltpu.make_async_copy(
                    in_ref.at[source + h, rank, c],
                    tiles.at[q, pl.ds(row, CHUNK), pl.ds(col, CHUNK)],
                    in_sem.at[q, 2 * h + c],
                ))

    def fetch(q, carry):
        present = table[q] % 4 > 0

        @pl.when(present)
        def _():
            pieces(q, lambda copy: copy.start())

        @pl.when(jnp.logical_not(present))
        def _():
            tiles[q] = jnp.zeros((TILE, TILE), jnp.float32)

        return carry

    def put(q, carry):
        @pl.when(table[q] % 4 > 0)
        def _():
            pieces(q, lambda copy: copy.wait())

        pltpu.make_async_copy(tiles.at[q], out_ref.at[q], out_sem.at[q]).start()
        return carry

    def finish(q, carry):
        pltpu.make_async_copy(tiles.at[q], out_ref.at[q], out_sem.at[q]).wait()
        return carry

    lax.fori_loop(0, slots, fetch, 0)
    lax.fori_loop(0, slots, put, 0)
    lax.fori_loop(0, slots, finish, 0)


def assemble(table, incoming):
    slots = table.shape[0]
    return pl.pallas_call(
        assemble_kernel,
        out_shape=jax.ShapeDtypeStruct((slots, TILE, TILE), jnp.float32),
        in_specs=[pl.BlockSpec(memory_space=pltpu.SMEM), pl.BlockSpec(memory_space=pl.ANY)],
        out_specs=pl.BlockSpec(memory_space=pl.ANY),
        scratch_shapes=[
            pltpu.VMEM((slots, TILE, TILE), jnp.float32),
            pltpu.SemaphoreType.DMA((slots, 4)),
            pltpu.SemaphoreType.DMA((slots,)),
        ],
        name="assemble",
    )(table, incoming)


def per_device(matrix_rows, tile_owner, tile_slot):
    devices = GROUPS * PLANE
    slots = (tile_owner.shape[0] + devices - 1) // devices
    incoming, table = exchange(matrix_rows, tile_owner, tile_slot, slots)
    return assemble(table, incoming)


def solution(mesh):
    placed = (P(("gx", "gy"), None), P(), P())
    return jax.shard_map(
        per_device,
        mesh=mesh,
        in_specs=placed,
        out_specs=P(("gx", "gy"), None, None),
        check_vma=False,
    )
```

```python
import jax
import jax.numpy as jnp
import numpy as np
from jax import lax
from jax.experimental import pallas as pl
from jax.experimental.pallas import tpu as pltpu
from jax.sharding import PartitionSpec as P

MESH = pl.DeviceIdType.MESH
SIDE = 4
PLANE = SIDE * SIDE
GROUPS = 8
HALF_TILES = 8
STEPS = 5
CAP = 3
CHUNK = 128
HALF = CHUNK // 2
TILE = 256
TILE_COUNT = 64
ENTRIES = 33
ORDER = ((2, 0), (0, 1), (1, 9), (0, 3), (3, 9), (1, 0), (3, 0), (0, 0))
SERVED = len(ORDER)
PIECES = 2 * SERVED


def entry_of(e, gx, r):
    quarter = HALF_TILES // 2
    middle = GROUPS // 2 - 1
    if e <= quarter:
        s, col = 0, (r - e + HALF_TILES) % HALF_TILES
        valid = r < quarter if e == quarter else None
        rowwise = col <= r
        source = gx
    elif e <= quarter + middle * HALF_TILES:
        s, col = 1 + (e - quarter - 1) // HALF_TILES, (e - quarter - 1) % HALF_TILES
        valid = None
        source = (gx - s + GROUPS) % GROUPS
        rowwise = source > gx
    else:
        s = middle + 1
        last = e - quarter - 1 - middle * HALF_TILES
        col = 2 * last + (r + jnp.where(gx >= GROUPS // 2, 1, 0)) % 2
        valid = None
        source = (gx - s + GROUPS) % GROUPS
        rowwise = source > gx
    near = source * HALF_TILES + r
    far = gx * HALF_TILES + col
    row_tile = jnp.where(rowwise, near, far)
    col_tile = jnp.where(rowwise, far, near)
    return s, col, valid, rowwise, row_tile, col_tile


def exchange_kernel(
    owner_smem, owner_any, slot_any, code_any, a_any, in_ref, table_ref,
    a_ref, owner_ref, slot_ref, code_ref,
    g, ghi, glo, rf, qf, rhi, rlo, outs, target_tab, entry_tab, send_tab, found_tab,
    a1_send, a1_recv, a2_send, a2_recv, b1_send, b1_recv, b2_send, b2_recv,
    z_send, z_recv, p_send, p_recv, q_send, q_recv, x_send, x_recv, l_sem,
):
    gx = lax.axis_index("gx")
    gy = lax.axis_index("gy")
    core = gx % 2
    y = gy // SIDE
    x = gy % SIDE
    u = jnp.where(core == 0, x, y)
    v = jnp.where(core == 0, y, x)
    stride_u = jnp.where(core == 0, 1, SIDE)
    stride_v = jnp.where(core == 0, SIDE, 1)

    def at(du, dv):
        return (u + du + SIDE) % SIDE * stride_u + (v + dv + SIDE) % SIDE * stride_v

    ahead = (gx + 2) % GROUPS
    behind = (gx + 6) % GROUPS
    partner = gx + 1 - 2 * core

    loads = [
        pltpu.make_async_copy(src, dst, l_sem.at[n])
        for n, (src, dst) in enumerate(
            ((a_any, a_ref), (owner_any, owner_ref), (slot_any, slot_ref), (code_any, code_ref))
        )
    ]
    for load in loads:
        load.start()

    barrier = pltpu.get_barrier_semaphore()
    for du, dv in ((1, 0), (3, 0), (0, 1), (0, 3)):
        pl.semaphore_signal(
            barrier, inc=1, device_id={"gx": gx, "gy": at(du, dv)}, device_id_type=MESH
        )
    for other in (ahead, behind, partner):
        pl.semaphore_signal(barrier, inc=1, device_id={"gx": other, "gy": gy}, device_id_type=MESH)
    loads[0].wait()
    pl.semaphore_wait(barrier, 7)

    def rows_of(c, h, size):
        return pl.ds(pl.multiple_of(c % 2 * CHUNK + h * HALF, HALF), size)

    def half(c, h):
        return g.at[c // 2, rows_of(c, h, HALF)]

    def whole(c):
        return g.at[c // 2, rows_of(c, 0, CHUNK)]

    def part(ref, n, h):
        return ref.at[n, pl.ds(h * HALF, HALF)]

    def own_half(h):
        return a_ref.at[pl.ds(h * HALF, HALF)]

    def remote(src, dst, send, recv, to_gx, to_gy):
        return pltpu.make_async_remote_copy(
            src_ref=src, dst_ref=dst, send_sem=send, recv_sem=recv,
            device_id={"gx": to_gx, "gy": to_gy}, device_id_type=MESH,
        )

    copies = []

    def start(copy):
        copy.start()
        copies.append(copy)

    me = gy
    a1 = [[
        remote(own_half(h), half(me, h), a1_send.at[d, p], a1_recv.at[d, p], gx, at(1 - 2 * d, 0))
        for p, h in enumerate((d, 1 - d))
    ] for d in (0, 1)]
    a2 = [
        remote(
            half(at(-1 + 2 * d, 0), d), half(at(-1 + 2 * d, 0), d),
            a2_send.at[d], a2_recv.at[d], gx, at(1 - 2 * d, 0),
        )
        for d in (0, 1)
    ]
    offs = (0, -1, 1, 2)
    b1 = [[[
        remote(
            own_half(h) if n == 0 else half(at(du, 0), h), half(at(du, 0), h),
            b1_send.at[n, d, p], b1_recv.at[n, d, p], gx, at(0, 1 - 2 * d),
        )
        for p, h in enumerate((d, 1 - d))
    ] for d in (0, 1)] for n, du in enumerate(offs)]
    b2 = [[
        remote(
            half(at(du, -1 + 2 * d), d), half(at(du, -1 + 2 * d), d),
            b2_send.at[n, d], b2_recv.at[n, d], gx, at(0, 1 - 2 * d),
        )
        for d in (0, 1)
    ] for n, du in enumerate(offs)]

    def along_z(n, src, dst, to):
        return remote(src, dst, z_send.at[n], z_recv.at[n], to, gy)

    z_near = along_z(0, a_ref, rf.at[1], ahead)
    z_far = along_z(1, rf.at[1], rf.at[3], ahead)

    def along_q(n, src, dst, to):
        return remote(src, dst, q_send.at[n], q_recv.at[n], to, gy)

    opposite = at(2, 2)
    q_near = [along_q(h, half(opposite, h), part(qf, 1, h), ahead) for h in (0, 1)]
    q_far = [along_q(2 + h, part(qf, 1, h), part(qf, 3, h), ahead) for h in (0, 1)]

    def to_partner(n, src, dst):
        return remote(src, dst, p_send.at[n], p_recv.at[n], partner, gy)

    p_of = [to_partner(n, a_ref, dst) for n, dst in enumerate((rf.at[0], rf.at[2], qf.at[0], qf.at[2]))]

    for p in (0, 1):
        for d in (0, 1):
            start(a1[d][p])
    for p in (0, 1):
        for d in (0, 1):
            start(b1[0][d][p])
    start(z_near)

    @pl.when(core == 0)
    def _():
        to_partner(0, a_ref, rf.at[0]).start()

    def split(value):
        high = value.astype(jnp.bfloat16)
        return high, (value - high.astype(jnp.float32)).astype(jnp.bfloat16)

    def split_g(c):
        block = c // 2
        rows = rows_of(c, 0, CHUNK)
        high, low = split(g[block, rows, :])
        ghi[block, rows, :] = high
        glo[block, rows, :] = low

    def split_r(n, value):
        high, low = split(value)
        rhi[n] = high
        rlo[n] = low

    for cls, chunk in enumerate((gy, opposite)):
        class_r = chunk // 2
        for e in range(ENTRIES):
            s, col, valid, rowwise, row_tile, col_tile = entry_of(e, gx, class_r)
            owner = owner_smem[row_tile * (row_tile + 1) // 2 + col_tile] % PLANE
            target_tab[cls * ENTRIES + e] = owner if valid is None else jnp.where(valid, owner, -1)
            diag = jnp.where(row_tile == col_tile, 2, 0)
            step = s + STEPS * cls
            entry_tab[cls * ENTRIES + e] = step * 32 + col * 4 + diag + jnp.where(rowwise, 1, 0)

    def served(n, cls):
        du = jnp.int32(0)
        dv = jnp.int32(0)
        for m, (one, two) in enumerate(ORDER):
            du = jnp.where(n == m, one, du)
            dv = jnp.where(n == m, two, dv)
        side = jnp.where((u + 2 * cls) % SIDE < 2, 1, 3)
        return at(du, jnp.where(dv == 9, side, dv))

    def fill(p, carry):
        to = served(p // 2, p % 2)
        base = p % 2 * ENTRIES
        kept = [jnp.int32(0)] * CAP
        for e in range(ENTRIES):
            hit = target_tab[base + e] == to
            fresh = entry_tab[base + e]
            kept = [jnp.where(hit, b, a) for a, b in zip(kept, [fresh] + kept[:-1])]
        for k in range(CAP):
            send_tab[p * CAP + k] = kept[k]
        return carry

    lax.fori_loop(0, PIECES, fill, 0)
    split_r(0, a_ref[...])
    block, rows = me // 2, rows_of(me, 0, CHUNK)
    ghi[block, rows, :] = rhi[0]
    glo[block, rows, :] = rlo[0]

    for load in loads[1:]:
        load.wait()
    mine = owner_ref[...] == gx * PLANE + gy
    slots = table_ref.shape[0]

    def find(q, carry):
        hit = jnp.logical_and(mine, slot_ref[...] == q)
        found = jnp.max(jnp.where(hit, code_ref[...], -1))
        row_tile = jnp.maximum(found, 0) // TILE_COUNT
        col_tile = jnp.maximum(found, 0) % TILE_COUNT
        group_a, inner_i = row_tile // HALF_TILES, row_tile % HALF_TILES
        group_b, inner_j = col_tile // HALF_TILES, col_tile % HALF_TILES
        gap = group_a - group_b
        even = (inner_i + inner_j) % 2 == 0
        across = jnp.logical_or(gap > GROUPS // 2, jnp.logical_and(gap == GROUPS // 2, even))
        within = inner_i - inner_j < HALF_TILES // 2
        rowwise = jnp.logical_or(jnp.logical_and(gap == 0, within), jnp.logical_and(gap > 0, across))
        class_r = jnp.where(rowwise, inner_i, inner_j)
        col = jnp.where(rowwise, inner_j, inner_i)
        s = (gx - jnp.where(rowwise, group_a, group_b) + GROUPS) % GROUPS
        place = s * HALF_TILES + jnp.where(s == 0, (class_r - col + HALF_TILES) % HALF_TILES, col)
        found_tab[q] = jnp.where(found >= 0, class_r * 64 + place, -1)
        table_ref[q] = jnp.where(found >= 0, jnp.where(rowwise, 1, 2), 0) + class_r * 4
        return carry

    def count(q, carry):
        own = found_tab[q]
        later = jnp.int32(0)
        for other in range(slots):
            code = found_tab[other]
            same = jnp.logical_and(code // 64 == own // 64, code > own)
            later = later + jnp.where(same, 1, 0)
        table_ref[q] = table_ref[q] + 32 * jnp.minimum(later, CAP - 1)
        return carry

    def take_v(n):
        for d in (0, 1):
            b1[n][d][1].wait_recv()
            split_g(at(offs[n], -1 + 2 * d))

    def take_far(n):
        for d in (0, 1):
            b2[n][d].wait_recv()
        split_g(at(offs[n], 2))

    for d in (0, 1):
        a1[d][0].wait_recv()
        start(a2[d])
    for d in (0, 1):
        a1[d][1].wait_recv()
    for d in (0, 1):
        start(b1[1][d][0])
    for d in (0, 1):
        split_g(at(-1 + 2 * d, 0))
    for d in (0, 1):
        a2[d].wait_recv()
        start(b1[3][d][0])
    for d in (0, 1):
        b1[0][d][0].wait_recv()
        start(b2[0][d])
    for d in (0, 1):
        start(b1[3][d][1])
    split_g(at(2, 0))
    for d in (0, 1):
        b1[3][d][0].wait_recv()
        start(b2[3][d])
    for d in (0, 1):
        start(b1[1][d][1])
    for p in (0, 1):
        for d in (0, 1):
            start(b1[2][d][p])
    for d in (0, 1):
        b1[1][d][0].wait_recv()
        start(b2[1][d])
    z_near.wait_recv()
    start(z_far)

    @pl.when(core == 0)
    def _():
        to_partner(1, rf.at[1], rf.at[2]).start()

    @pl.when(core == 1)
    def _():
        to_partner(0, rf.at[1], rf.at[0]).start()

    take_v(0)
    split_r(2, rf[1])
    z_far.wait_recv()

    @pl.when(core == 1)
    def _():
        to_partner(1, rf.at[3], rf.at[2]).start()

    split_r(4, rf[3])
    take_far(0)
    for d in (0, 1):
        b2[3][d].wait_recv()
    for h in (0, 1):
        start(q_near[h])

    @pl.when(core == 0)
    def _():
        to_partner(2, whole(opposite), qf.at[0]).start()

    for d in (0, 1):
        b1[2][d][0].wait_recv()
        start(b2[2][d])
    split_g(opposite)
    high, low = split(whole(opposite)[...])
    rhi[STEPS] = high
    rlo[STEPS] = low
    lax.fori_loop(0, slots, find, 0)
    take_v(1)
    take_v(3)
    p_of[0].wait_recv()
    split_r(1, rf[0])
    p_of[1].wait_recv()
    split_r(3, rf[2])
    lax.fori_loop(0, slots, count, 0)
    take_v(2)
    take_far(1)
    q_near[0].wait_recv()
    start(q_far[0])
    take_far(2)

    row_in = lax.broadcasted_iota(jnp.int32, (CHUNK, TILE), 0)
    col_in = lax.broadcasted_iota(jnp.int32, (CHUNK, TILE), 1)

    def dot(p, q):
        return lax.dot_general(p, q, (((1,), (1,)), ((), ())), preferred_element_type=jnp.float32)

    def one_piece(i, carry):
        k = i // SERVED % CAP
        p = i % SERVED * 2 + i // (SERVED * CAP)
        to = served(p // 2, p % 2)
        chunk = jnp.where(p % 2 == 0, gy, opposite)
        entry = send_tab[p * CAP + k]
        s = entry // 32
        j = entry // 4 % HALF_TILES
        rh = rhi[s]
        gh = ghi[j]
        value = dot(rh, gh) + dot(rh, glo[j]) + dot(rlo[s], gh)
        upper = row_in + chunk % 2 * CHUNK < col_in
        masked = jnp.logical_and(upper, entry // 2 % 2 > 0)
        value = jnp.where(masked, jnp.float32(0.0), value)
        rowwise = jnp.full((CHUNK, CHUNK), entry % 2, jnp.int32) > 0
        for c in range(2):
            part = value[:, c * CHUNK:(c + 1) * CHUNK]
            outs[p, k, c] = jnp.where(rowwise, part, part.T)

        @pl.when(p < PIECES - 2)
        def _():
            remote(
                outs.at[p, k], in_ref.at[chunk, k], x_send.at[p, k], x_recv.at[chunk, k], gx, to
            ).start()

        return carry

    lax.fori_loop(0, SERVED, one_piece, 0)
    q_near[1].wait_recv()
    start(q_far[1])

    @pl.when(core == 0)
    def _():
        to_partner(3, qf.at[1], qf.at[2]).start()

    @pl.when(core == 1)
    def _():
        to_partner(2, qf.at[1], qf.at[0]).start()

    split_r(STEPS + 2, qf[1])
    lax.fori_loop(SERVED, SERVED * CAP, one_piece, 0)
    for h in (0, 1):
        q_far[h].wait_recv()

    @pl.when(core == 1)
    def _():
        to_partner(3, qf.at[3], qf.at[2]).start()

    split_r(STEPS + 4, qf[3])
    p_of[2].wait_recv()
    split_r(STEPS + 1, qf[0])
    p_of[3].wait_recv()
    split_r(STEPS + 3, qf[2])
    lax.fori_loop(SERVED * CAP, PIECES * CAP, one_piece, 0)
    local = [
        pltpu.make_async_copy(outs.at[PIECES - 2 + n], in_ref.at[c], l_sem.at[n])
        for n, c in enumerate((gy, opposite))
    ]
    for copy in local:
        copy.start()
    for copy in copies + p_of:
        copy.wait_send()
    for copy in local:
        copy.wait()

    def sent(i, carry):
        remote(
            outs.at[i // CAP, i % CAP], in_ref.at[0, 0], x_send.at[i // CAP, i % CAP], x_recv.at[0, 0], ahead, gy
        ).wait_send()
        return carry

    lax.fori_loop(0, (PIECES - 2) * CAP, sent, 0)

    def arrived(i, carry):
        du = i // CAP // SIDE
        dv = i // CAP % SIDE
        chunk = at(du, dv)

        @pl.when(jnp.logical_or(du != dv, du % 2 > 0))
        def _():
            remote(
                outs.at[0, 0], in_ref.at[chunk, i % CAP], x_send.at[0, 0], x_recv.at[chunk, i % CAP], ahead, gy
            ).wait_recv()

        return carry

    lax.fori_loop(0, PLANE * CAP, arrived, 0)


def exchange(matrix_rows, tile_owner, tile_slot, slots):
    rows, width = matrix_rows.shape
    count = tile_owner.shape[0]
    lower_i, lower_j = np.tril_indices(TILE_COUNT)
    code = jnp.asarray(lower_i * TILE_COUNT + lower_j, jnp.int32)
    smem = pl.BlockSpec(memory_space=pltpu.SMEM)
    hbm = pl.BlockSpec(memory_space=pltpu.HBM)
    dma = pltpu.SemaphoreType.DMA
    return pl.pallas_call(
        exchange_kernel,
        out_shape=(
            jax.ShapeDtypeStruct((PLANE, CAP, 2, CHUNK, CHUNK), jnp.float32),
            jax.ShapeDtypeStruct((slots,), jnp.int32),
        ),
        in_specs=[smem, hbm, hbm, hbm, hbm],
        out_specs=(pl.BlockSpec(memory_space=pltpu.VMEM), smem),
        scratch_shapes=[
            pltpu.VMEM((rows, width), jnp.float32),
            pltpu.VMEM((count,), jnp.int32),
            pltpu.VMEM((count,), jnp.int32),
            pltpu.VMEM((count,), jnp.int32),
            pltpu.VMEM((HALF_TILES, TILE, width), jnp.float32),
            pltpu.VMEM((HALF_TILES, TILE, width), jnp.bfloat16),
            pltpu.VMEM((HALF_TILES, TILE, width), jnp.bfloat16),
            pltpu.VMEM((4, CHUNK, width), jnp.float32),
            pltpu.VMEM((4, CHUNK, width), jnp.float32),
            pltpu.VMEM((2 * STEPS, CHUNK, width), jnp.bfloat16),
            pltpu.VMEM((2 * STEPS, CHUNK, width), jnp.bfloat16),
            pltpu.VMEM((PIECES, CAP, 2, CHUNK, CHUNK), jnp.float32),
            pltpu.SMEM((2 * ENTRIES,), jnp.int32),
            pltpu.SMEM((2 * ENTRIES,), jnp.int32),
            pltpu.SMEM((PIECES * CAP,), jnp.int32),
            pltpu.SMEM((slots,), jnp.int32),
            dma((2, 2)), dma((2, 2)), dma((2,)), dma((2,)),
            dma((4, 2, 2)), dma((4, 2, 2)), dma((4, 2)), dma((4, 2)),
            dma((2,)), dma((2,)), dma((4,)), dma((4,)), dma((4,)), dma((4,)),
            dma((PIECES, CAP)), dma((PLANE, CAP)), dma((4,)),
        ],
        compiler_params=pltpu.CompilerParams(
            collective_id=0, has_side_effects=True, vmem_limit_bytes=42 * 1024 * 1024
        ),
        name="exchange",
    )(tile_owner, *(pltpu.with_memory_space_constraint(x, pltpu.HBM) for x in (tile_owner, tile_slot, code, matrix_rows)))


def assemble_kernel(table, in_ref, out_ref, blank, out_sem):
    slots = table.shape[0]

    def quarters(q, act):
        entry = table[q]
        across = entry % 4 == 1
        source = entry // 4 % HALF_TILES * 2
        for h in range(2):
            for c in range(2):
                row = pl.multiple_of(jnp.where(across, h, c) * CHUNK, CHUNK)
                col = pl.multiple_of(jnp.where(across, c, h) * CHUNK, CHUNK)
                place = out_ref.at[q, pl.ds(row, CHUNK), pl.ds(col, CHUNK)]
                act(pltpu.make_async_copy(in_ref.at[source + h, entry // 32, c], place, out_sem.at[q, 2 * h + c]))

    def clear(q):
        return pltpu.make_async_copy(blank, out_ref.at[q], out_sem.at[q, 0])

    def put(q, carry):
        present = table[q] % 4 > 0

        @pl.when(present)
        def _():
            quarters(q, lambda copy: copy.start())

        @pl.when(jnp.logical_not(present))
        def _():
            blank[...] = jnp.zeros(blank.shape, jnp.float32)
            clear(q).start()

        return carry

    def finish(q, carry):
        present = table[q] % 4 > 0

        @pl.when(present)
        def _():
            quarters(q, lambda copy: copy.wait())

        @pl.when(jnp.logical_not(present))
        def _():
            clear(q).wait()

        return carry

    lax.fori_loop(0, slots, put, 0)
    lax.fori_loop(0, slots, finish, 0)


def assemble(table, incoming):
    slots = table.shape[0]
    return pl.pallas_call(
        assemble_kernel,
        out_shape=jax.ShapeDtypeStruct((slots, TILE, TILE), jnp.float32),
        in_specs=[pl.BlockSpec(memory_space=pltpu.SMEM), pl.BlockSpec(memory_space=pltpu.VMEM)],
        out_specs=pl.BlockSpec(memory_space=pl.ANY),
        scratch_shapes=[
            pltpu.VMEM((TILE, TILE), jnp.float32),
            pltpu.SemaphoreType.DMA((slots, 4)),
        ],
        compiler_params=pltpu.CompilerParams(vmem_limit_bytes=16 * 1024 * 1024),
        name="assemble",
    )(table, incoming)


def per_device(matrix_rows, tile_owner, tile_slot):
    devices = GROUPS * PLANE
    slots = (tile_owner.shape[0] + devices - 1) // devices
    incoming, table = exchange(matrix_rows, tile_owner, tile_slot, slots)
    return assemble(table, incoming)


def solution(mesh):
    placed = (P(("gx", "gy"), None), P(), P())
    return jax.shard_map(
        per_device,
        mesh=mesh,
        in_specs=placed,
        out_specs=P(("gx", "gy"), None, None),
        check_vma=False,
    )
```

```python
import jax
import jax.numpy as jnp
import numpy as np
from jax import lax
from jax.experimental import pallas as pl
from jax.experimental.pallas import tpu as pltpu
from jax.sharding import PartitionSpec as P

MESH = pl.DeviceIdType.MESH
SIDE = 4
PLANE = SIDE * SIDE
GROUPS = 8
HALF_TILES = 8
STEPS = 5
CAP = 3
CHUNK = 128
HALF = CHUNK // 2
TILE = 256
TILE_COUNT = 64
ENTRIES = 33
ORDER = ((2, 0), (0, 1), (1, 9), (0, 3), (3, 9), (1, 0), (3, 0), (0, 0))
SERVED = len(ORDER)
PIECES = 2 * SERVED
LEAVING = SERVED - 1


def entry_of(e, gx, r):
    quarter = HALF_TILES // 2
    middle = GROUPS // 2 - 1
    if e <= quarter:
        s, col = 0, (r - e + HALF_TILES) % HALF_TILES
        valid = r < quarter if e == quarter else None
        rowwise = col <= r
        source = gx
    elif e <= quarter + middle * HALF_TILES:
        s, col = 1 + (e - quarter - 1) // HALF_TILES, (e - quarter - 1) % HALF_TILES
        valid = None
        source = (gx - s + GROUPS) % GROUPS
        rowwise = source > gx
    else:
        s = middle + 1
        last = e - quarter - 1 - middle * HALF_TILES
        col = 2 * last + (r + jnp.where(gx >= GROUPS // 2, 1, 0)) % 2
        valid = None
        source = (gx - s + GROUPS) % GROUPS
        rowwise = source > gx
    near = source * HALF_TILES + r
    far = gx * HALF_TILES + col
    row_tile = jnp.where(rowwise, near, far)
    col_tile = jnp.where(rowwise, far, near)
    return s, col, valid, rowwise, row_tile, col_tile


def exchange_kernel(
    owner_smem, owner_any, slot_any, code_any, a_any, in_ref, table_ref,
    a_ref, owner_ref, slot_ref, code_ref,
    g, ghi, glo, rf, qf, rhi, rlo, outs, target_tab, entry_tab, send_tab, found_tab,
    a1_send, a1_recv, a2_send, a2_recv, b1_send, b1_recv, b2_send, b2_recv,
    z_send, z_recv, p_send, p_recv, q_send, q_recv, x_send, x_recv, l_sem,
):
    gx = lax.axis_index("gx")
    gy = lax.axis_index("gy")
    core = gx % 2
    y = gy // SIDE
    x = gy % SIDE
    u = jnp.where(core == 0, x, y)
    v = jnp.where(core == 0, y, x)
    stride_u = jnp.where(core == 0, 1, SIDE)
    stride_v = jnp.where(core == 0, SIDE, 1)

    def at(du, dv):
        return (u + du + SIDE) % SIDE * stride_u + (v + dv + SIDE) % SIDE * stride_v

    ahead = (gx + 2) % GROUPS
    behind = (gx + 6) % GROUPS
    partner = gx + 1 - 2 * core

    loads = [
        pltpu.make_async_copy(src, dst, l_sem.at[n])
        for n, (src, dst) in enumerate(
            ((a_any, a_ref), (owner_any, owner_ref), (slot_any, slot_ref), (code_any, code_ref))
        )
    ]
    for load in loads:
        load.start()

    barrier = pltpu.get_barrier_semaphore()
    for du, dv in ((1, 0), (3, 0), (0, 1), (0, 3)):
        pl.semaphore_signal(
            barrier, inc=1, device_id={"gx": gx, "gy": at(du, dv)}, device_id_type=MESH
        )
    for other in (ahead, behind, partner):
        pl.semaphore_signal(barrier, inc=1, device_id={"gx": other, "gy": gy}, device_id_type=MESH)
    loads[0].wait()
    pl.semaphore_wait(barrier, 7)

    def rows_of(c, h, size):
        return pl.ds(pl.multiple_of(c % 2 * CHUNK + h * HALF, HALF), size)

    def half(c, h):
        return g.at[c // 2, rows_of(c, h, HALF)]

    def whole(c):
        return g.at[c // 2, rows_of(c, 0, CHUNK)]

    def part(ref, n, h):
        return ref.at[n, pl.ds(h * HALF, HALF)]

    def own_half(h):
        return a_ref.at[pl.ds(h * HALF, HALF)]

    def remote(src, dst, send, recv, to_gx, to_gy):
        return pltpu.make_async_remote_copy(
            src_ref=src, dst_ref=dst, send_sem=send, recv_sem=recv,
            device_id={"gx": to_gx, "gy": to_gy}, device_id_type=MESH,
        )

    copies = []

    def start(copy):
        copy.start()
        copies.append(copy)

    me = gy
    a1 = [[
        remote(own_half(h), half(me, h), a1_send.at[d, p], a1_recv.at[d, p], gx, at(1 - 2 * d, 0))
        for p, h in enumerate((d, 1 - d))
    ] for d in (0, 1)]
    a2 = [
        remote(
            half(at(-1 + 2 * d, 0), d), half(at(-1 + 2 * d, 0), d),
            a2_send.at[d], a2_recv.at[d], gx, at(1 - 2 * d, 0),
        )
        for d in (0, 1)
    ]
    offs = (0, -1, 1, 2)
    b1 = [[[
        remote(
            own_half(h) if n == 0 else half(at(du, 0), h), half(at(du, 0), h),
            b1_send.at[n, d, p], b1_recv.at[n, d, p], gx, at(0, 1 - 2 * d),
        )
        for p, h in enumerate((d, 1 - d))
    ] for d in (0, 1)] for n, du in enumerate(offs)]
    b2 = [[
        remote(
            half(at(du, -1 + 2 * d), d), half(at(du, -1 + 2 * d), d),
            b2_send.at[n, d], b2_recv.at[n, d], gx, at(0, 1 - 2 * d),
        )
        for d in (0, 1)
    ] for n, du in enumerate(offs)]

    def along_z(n, src, dst, to):
        return remote(src, dst, z_send.at[n], z_recv.at[n], to, gy)

    z_near = along_z(0, a_ref, rf.at[1], ahead)
    z_far = along_z(1, rf.at[1], rf.at[3], ahead)

    def along_q(n, src, dst, to):
        return remote(src, dst, q_send.at[n], q_recv.at[n], to, gy)

    opposite = at(2, 2)
    q_near = [along_q(h, half(opposite, h), part(qf, 1, h), ahead) for h in (0, 1)]
    q_far = [along_q(2 + h, part(qf, 1, h), part(qf, 3, h), ahead) for h in (0, 1)]

    def to_partner(n, src, dst):
        return remote(src, dst, p_send.at[n], p_recv.at[n], partner, gy)

    p_of = [to_partner(n, a_ref, dst) for n, dst in enumerate((rf.at[0], rf.at[2], qf.at[0], qf.at[2]))]

    for p in (0, 1):
        for d in (0, 1):
            start(a1[d][p])
    for p in (0, 1):
        for d in (0, 1):
            start(b1[0][d][p])
    start(z_near)

    @pl.when(core == 0)
    def _():
        to_partner(0, a_ref, rf.at[0]).start()

    def split(value):
        high = value.astype(jnp.bfloat16)
        return high, (value - high.astype(jnp.float32)).astype(jnp.bfloat16)

    def split_g(c):
        block = c // 2
        rows = rows_of(c, 0, CHUNK)
        high, low = split(g[block, rows, :])
        ghi[block, rows, :] = high
        glo[block, rows, :] = low

    def split_r(n, value):
        high, low = split(value)
        rhi[n] = high
        rlo[n] = low

    for cls, chunk in enumerate((gy, opposite)):
        class_r = chunk // 2
        for e in range(ENTRIES):
            s, col, valid, rowwise, row_tile, col_tile = entry_of(e, gx, class_r)
            owner = owner_smem[row_tile * (row_tile + 1) // 2 + col_tile] % PLANE
            target_tab[cls * ENTRIES + e] = owner if valid is None else jnp.where(valid, owner, -1)
            diag = jnp.where(row_tile == col_tile, 2, 0)
            step = s + STEPS * cls
            entry_tab[cls * ENTRIES + e] = step * 32 + col * 4 + diag + jnp.where(rowwise, 1, 0)

    def served(n, cls):
        du = jnp.int32(0)
        dv = jnp.int32(0)
        for m, (one, two) in enumerate(ORDER):
            du = jnp.where(n == m, one, du)
            dv = jnp.where(n == m, two, dv)
        side = jnp.where((u + 2 * cls) % SIDE < 2, 1, 3)
        return at(du, jnp.where(dv == 9, side, dv))

    def fill(p, carry):
        to = served(p // 2, p % 2)
        base = p % 2 * ENTRIES
        kept = [jnp.int32(0)] * CAP
        for e in range(ENTRIES):
            hit = target_tab[base + e] == to
            fresh = entry_tab[base + e]
            kept = [jnp.where(hit, b, a) for a, b in zip(kept, [fresh] + kept[:-1])]
        for k in range(CAP):
            send_tab[p * CAP + k] = kept[k]
        return carry

    lax.fori_loop(0, PIECES, fill, 0)
    split_r(0, a_ref[...])
    block, rows = me // 2, rows_of(me, 0, CHUNK)
    ghi[block, rows, :] = rhi[0]
    glo[block, rows, :] = rlo[0]

    for load in loads[1:]:
        load.wait()
    mine = owner_ref[...] == gx * PLANE + gy
    slots = table_ref.shape[0]

    def find(q, carry):
        hit = jnp.logical_and(mine, slot_ref[...] == q)
        found = jnp.max(jnp.where(hit, code_ref[...], -1))
        row_tile = jnp.maximum(found, 0) // TILE_COUNT
        col_tile = jnp.maximum(found, 0) % TILE_COUNT
        group_a, inner_i = row_tile // HALF_TILES, row_tile % HALF_TILES
        group_b, inner_j = col_tile // HALF_TILES, col_tile % HALF_TILES
        gap = group_a - group_b
        even = (inner_i + inner_j) % 2 == 0
        across = jnp.logical_or(gap > GROUPS // 2, jnp.logical_and(gap == GROUPS // 2, even))
        within = inner_i - inner_j < HALF_TILES // 2
        rowwise = jnp.logical_or(jnp.logical_and(gap == 0, within), jnp.logical_and(gap > 0, across))
        class_r = jnp.where(rowwise, inner_i, inner_j)
        col = jnp.where(rowwise, inner_j, inner_i)
        s = (gx - jnp.where(rowwise, group_a, group_b) + GROUPS) % GROUPS
        place = s * HALF_TILES + jnp.where(s == 0, (class_r - col + HALF_TILES) % HALF_TILES, col)
        found_tab[q] = jnp.where(found >= 0, class_r * 64 + place, -1)
        table_ref[q] = jnp.where(found >= 0, jnp.where(rowwise, 1, 2), 0) + class_r * 4
        return carry

    def count(q, carry):
        own = found_tab[q]
        later = jnp.int32(0)
        for other in range(slots):
            code = found_tab[other]
            same = jnp.logical_and(code // 64 == own // 64, code > own)
            later = later + jnp.where(same, 1, 0)
        table_ref[q] = table_ref[q] + 32 * jnp.minimum(later, CAP - 1)
        return carry

    def take_v(n):
        for d in (0, 1):
            b1[n][d][1].wait_recv()
            split_g(at(offs[n], -1 + 2 * d))

    def take_far(n):
        for d in (0, 1):
            b2[n][d].wait_recv()
        split_g(at(offs[n], 2))

    for d in (0, 1):
        a1[d][0].wait_recv()
        start(a2[d])
    for d in (0, 1):
        a1[d][1].wait_recv()
    for d in (0, 1):
        start(b1[1][d][0])
    for d in (0, 1):
        split_g(at(-1 + 2 * d, 0))
    for d in (0, 1):
        a2[d].wait_recv()
        start(b1[3][d][0])
    for d in (0, 1):
        b1[0][d][0].wait_recv()
        start(b2[0][d])
    for d in (0, 1):
        start(b1[3][d][1])
    split_g(at(2, 0))
    for d in (0, 1):
        b1[3][d][0].wait_recv()
        start(b2[3][d])
    for d in (0, 1):
        start(b1[1][d][1])
    for p in (0, 1):
        for d in (0, 1):
            start(b1[2][d][p])
    for d in (0, 1):
        b1[1][d][0].wait_recv()
        start(b2[1][d])
    z_near.wait_recv()
    start(z_far)

    @pl.when(core == 0)
    def _():
        to_partner(1, rf.at[1], rf.at[2]).start()

    @pl.when(core == 1)
    def _():
        to_partner(0, rf.at[1], rf.at[0]).start()

    take_v(0)
    split_r(2, rf[1])
    z_far.wait_recv()

    @pl.when(core == 1)
    def _():
        to_partner(1, rf.at[3], rf.at[2]).start()

    split_r(4, rf[3])
    take_far(0)
    for d in (0, 1):
        b2[3][d].wait_recv()
    for h in (0, 1):
        start(q_near[h])

    @pl.when(core == 0)
    def _():
        to_partner(2, whole(opposite), qf.at[0]).start()

    for d in (0, 1):
        b1[2][d][0].wait_recv()
        start(b2[2][d])
    split_g(opposite)
    high, low = split(whole(opposite)[...])
    rhi[STEPS] = high
    rlo[STEPS] = low
    lax.fori_loop(0, slots, find, 0)
    take_v(1)
    take_v(3)
    p_of[0].wait_recv()
    split_r(1, rf[0])
    p_of[1].wait_recv()
    split_r(3, rf[2])
    lax.fori_loop(0, slots, count, 0)
    take_v(2)
    take_far(1)
    q_near[0].wait_recv()
    start(q_far[0])
    take_far(2)

    row_in = lax.broadcasted_iota(jnp.int32, (CHUNK, TILE), 0)
    col_in = lax.broadcasted_iota(jnp.int32, (CHUNK, TILE), 1)

    def dot(p, q):
        return lax.dot_general(p, q, (((1,), (1,)), ((), ())), preferred_element_type=jnp.float32)

    def one_piece(i, carry):
        away = i < 2 * LEAVING * CAP
        n = jnp.where(away, i % LEAVING, LEAVING)
        k = jnp.where(away, i // LEAVING % CAP, i % CAP)
        p = n * 2 + jnp.where(away, i // (LEAVING * CAP), (i - 2 * LEAVING * CAP) // CAP)
        to = served(p // 2, p % 2)
        chunk = jnp.where(p % 2 == 0, gy, opposite)
        entry = send_tab[p * CAP + k]
        s = entry // 32
        j = entry // 4 % HALF_TILES
        rh = rhi[s]
        gh = ghi[j]
        value = dot(rh, gh) + dot(rh, glo[j]) + dot(rlo[s], gh)
        upper = row_in + chunk % 2 * CHUNK < col_in
        masked = jnp.logical_and(upper, entry // 2 % 2 > 0)
        value = jnp.where(masked, jnp.float32(0.0), value)
        rowwise = jnp.full((CHUNK, CHUNK), entry % 2, jnp.int32) > 0
        for c in range(2):
            part = value[:, c * CHUNK:(c + 1) * CHUNK]
            outs[p, k, c] = jnp.where(rowwise, part, part.T)

        @pl.when(away)
        def _():
            remote(outs.at[p, k], in_ref.at[chunk, k], x_send, x_recv, gx, to).start()

        return carry

    lax.fori_loop(0, LEAVING, one_piece, 0)
    q_near[1].wait_recv()
    start(q_far[1])

    @pl.when(core == 0)
    def _():
        to_partner(3, qf.at[1], qf.at[2]).start()

    @pl.when(core == 1)
    def _():
        to_partner(2, qf.at[1], qf.at[0]).start()

    split_r(STEPS + 2, qf[1])
    lax.fori_loop(LEAVING, LEAVING * CAP, one_piece, 0)
    for h in (0, 1):
        q_far[h].wait_recv()

    @pl.when(core == 1)
    def _():
        to_partner(3, qf.at[3], qf.at[2]).start()

    split_r(STEPS + 4, qf[3])
    p_of[2].wait_recv()
    split_r(STEPS + 1, qf[0])
    p_of[3].wait_recv()
    split_r(STEPS + 3, qf[2])
    lax.fori_loop(LEAVING * CAP, PIECES * CAP, one_piece, 0)
    local = [
        pltpu.make_async_copy(outs.at[PIECES - 2 + n], in_ref.at[c], l_sem.at[n])
        for n, c in enumerate((gy, opposite))
    ]
    for copy in local:
        copy.start()
    for copy in copies + p_of:
        copy.wait_send()
    for copy in local:
        copy.wait()

    everything = remote(outs.at[pl.ds(0, 2 * LEAVING)], in_ref.at[pl.ds(0, 2 * LEAVING)], x_send, x_recv, ahead, gy)
    everything.wait_send()
    everything.wait_recv()


def exchange(matrix_rows, tile_owner, tile_slot, slots):
    rows, width = matrix_rows.shape
    count = tile_owner.shape[0]
    lower_i, lower_j = np.tril_indices(TILE_COUNT)
    code = jnp.asarray(lower_i * TILE_COUNT + lower_j, jnp.int32)
    smem = pl.BlockSpec(memory_space=pltpu.SMEM)
    hbm = pl.BlockSpec(memory_space=pltpu.HBM)
    dma = pltpu.SemaphoreType.DMA
    return pl.pallas_call(
        exchange_kernel,
        out_shape=(
            jax.ShapeDtypeStruct((PLANE, CAP, 2, CHUNK, CHUNK), jnp.float32),
            jax.ShapeDtypeStruct((slots,), jnp.int32),
        ),
        in_specs=[smem, hbm, hbm, hbm, hbm],
        out_specs=(pl.BlockSpec(memory_space=pltpu.VMEM), smem),
        scratch_shapes=[
            pltpu.VMEM((rows, width), jnp.float32),
            pltpu.VMEM((count,), jnp.int32),
            pltpu.VMEM((count,), jnp.int32),
            pltpu.VMEM((count,), jnp.int32),
            pltpu.VMEM((HALF_TILES, TILE, width), jnp.float32),
            pltpu.VMEM((HALF_TILES, TILE, width), jnp.bfloat16),
            pltpu.VMEM((HALF_TILES, TILE, width), jnp.bfloat16),
            pltpu.VMEM((4, CHUNK, width), jnp.float32),
            pltpu.VMEM((4, CHUNK, width), jnp.float32),
            pltpu.VMEM((2 * STEPS, CHUNK, width), jnp.bfloat16),
            pltpu.VMEM((2 * STEPS, CHUNK, width), jnp.bfloat16),
            pltpu.VMEM((PIECES, CAP, 2, CHUNK, CHUNK), jnp.float32),
            pltpu.SMEM((2 * ENTRIES,), jnp.int32),
            pltpu.SMEM((2 * ENTRIES,), jnp.int32),
            pltpu.SMEM((PIECES * CAP,), jnp.int32),
            pltpu.SMEM((slots,), jnp.int32),
            dma((2, 2)), dma((2, 2)), dma((2,)), dma((2,)),
            dma((4, 2, 2)), dma((4, 2, 2)), dma((4, 2)), dma((4, 2)),
            dma((2,)), dma((2,)), dma((4,)), dma((4,)), dma((4,)), dma((4,)),
            dma(()), dma(()), dma((4,)),
        ],
        compiler_params=pltpu.CompilerParams(
            collective_id=0, has_side_effects=True, vmem_limit_bytes=42 * 1024 * 1024
        ),
        name="exchange",
    )(tile_owner, *(pltpu.with_memory_space_constraint(x, pltpu.HBM) for x in (tile_owner, tile_slot, code, matrix_rows)))


def assemble_kernel(table, in_ref, out_ref, blank, out_sem):
    slots = table.shape[0]

    def quarters(q, act):
        entry = table[q]
        across = entry % 4 == 1
        source = entry // 4 % HALF_TILES * 2
        for h in range(2):
            for c in range(2):
                row = pl.multiple_of(jnp.where(across, h, c) * CHUNK, CHUNK)
                col = pl.multiple_of(jnp.where(across, c, h) * CHUNK, CHUNK)
                place = out_ref.at[q, pl.ds(row, CHUNK), pl.ds(col, CHUNK)]
                act(pltpu.make_async_copy(in_ref.at[source + h, entry // 32, c], place, out_sem.at[q, 2 * h + c]))

    def clear(q):
        return pltpu.make_async_copy(blank, out_ref.at[q], out_sem.at[q, 0])

    def put(q, carry):
        present = table[q] % 4 > 0

        @pl.when(present)
        def _():
            quarters(q, lambda copy: copy.start())

        @pl.when(jnp.logical_not(present))
        def _():
            blank[...] = jnp.zeros(blank.shape, jnp.float32)
            clear(q).start()

        return carry

    def finish(q, carry):
        present = table[q] % 4 > 0

        @pl.when(present)
        def _():
            quarters(q, lambda copy: copy.wait())

        @pl.when(jnp.logical_not(present))
        def _():
            clear(q).wait()

        return carry

    lax.fori_loop(0, slots, put, 0)
    lax.fori_loop(0, slots, finish, 0)


def assemble(table, incoming):
    slots = table.shape[0]
    return pl.pallas_call(
        assemble_kernel,
        out_shape=jax.ShapeDtypeStruct((slots, TILE, TILE), jnp.float32),
        in_specs=[pl.BlockSpec(memory_space=pltpu.SMEM), pl.BlockSpec(memory_space=pltpu.VMEM)],
        out_specs=pl.BlockSpec(memory_space=pl.ANY),
        scratch_shapes=[
            pltpu.VMEM((TILE, TILE), jnp.float32),
            pltpu.SemaphoreType.DMA((slots, 4)),
        ],
        compiler_params=pltpu.CompilerParams(vmem_limit_bytes=16 * 1024 * 1024),
        name="assemble",
    )(table, incoming)


def per_device(matrix_rows, tile_owner, tile_slot):
    devices = GROUPS * PLANE
    slots = (tile_owner.shape[0] + devices - 1) // devices
    incoming, table = exchange(matrix_rows, tile_owner, tile_slot, slots)
    return assemble(table, incoming)


def solution(mesh):
    placed = (P(("gx", "gy"), None), P(), P())
    return jax.shard_map(
        per_device,
        mesh=mesh,
        in_specs=placed,
        out_specs=P(("gx", "gy"), None, None),
        check_vma=False,
    )
```

```python
import jax
import jax.numpy as jnp
import numpy as np
from jax import lax
from jax.experimental import pallas as pl
from jax.experimental.pallas import tpu as pltpu
from jax.sharding import PartitionSpec as P

MESH = pl.DeviceIdType.MESH
SIDE = 4
PLANE = SIDE * SIDE
GROUPS = 8
HALF_TILES = 8
STEPS = 5
CAP = 3
CHUNK = 128
HALF = CHUNK // 2
TILE = 256
TILE_COUNT = 64
ENTRIES = 33
ORDER = ((2, 0), (0, 1), (1, 9), (0, 3), (3, 9), (1, 0), (3, 0), (0, 0))
SERVED = len(ORDER)
PIECES = 2 * SERVED
LEAVING = SERVED - 1


def entry_of(e, gx, r):
    quarter = HALF_TILES // 2
    middle = GROUPS // 2 - 1
    if e <= quarter:
        s, col = 0, (r - e + HALF_TILES) % HALF_TILES
        valid = r < quarter if e == quarter else None
        rowwise = col <= r
        source = gx
    elif e <= quarter + middle * HALF_TILES:
        s, col = 1 + (e - quarter - 1) // HALF_TILES, (e - quarter - 1) % HALF_TILES
        valid = None
        source = (gx - s + GROUPS) % GROUPS
        rowwise = source > gx
    else:
        s = middle + 1
        last = e - quarter - 1 - middle * HALF_TILES
        col = 2 * last + (r + jnp.where(gx >= GROUPS // 2, 1, 0)) % 2
        valid = None
        source = (gx - s + GROUPS) % GROUPS
        rowwise = source > gx
    near = source * HALF_TILES + r
    far = gx * HALF_TILES + col
    row_tile = jnp.where(rowwise, near, far)
    col_tile = jnp.where(rowwise, far, near)
    return s, col, valid, rowwise, row_tile, col_tile


def exchange_kernel(
    owner_smem, owner_any, slot_any, code_any, a_any, in_ref, table_ref,
    a_ref, owner_ref, slot_ref, code_ref,
    g, ghi, glo, rf, qf, rows_ref, outs, target_tab, entry_tab, send_tab, found_tab,
    a1_send, a1_recv, a2_send, a2_recv, b1_send, b1_recv, b2_send, b2_recv,
    z_send, z_recv, p_send, p_recv, q_send, q_recv, x_send, x_recv, l_sem,
):
    gx = lax.axis_index("gx")
    gy = lax.axis_index("gy")
    core = gx % 2
    y = gy // SIDE
    x = gy % SIDE
    u = jnp.where(core == 0, x, y)
    v = jnp.where(core == 0, y, x)
    stride_u = jnp.where(core == 0, 1, SIDE)
    stride_v = jnp.where(core == 0, SIDE, 1)

    def at(du, dv):
        return (u + du + SIDE) % SIDE * stride_u + (v + dv + SIDE) % SIDE * stride_v

    ahead = (gx + 2) % GROUPS
    behind = (gx + 6) % GROUPS
    partner = gx + 1 - 2 * core

    loads = [
        pltpu.make_async_copy(src, dst, l_sem.at[n])
        for n, (src, dst) in enumerate(
            ((a_any, a_ref), (owner_any, owner_ref), (slot_any, slot_ref), (code_any, code_ref))
        )
    ]
    barrier = pltpu.get_barrier_semaphore()
    for du, dv in ((1, 0), (3, 0), (0, 1), (0, 3)):
        pl.semaphore_signal(
            barrier, inc=1, device_id={"gx": gx, "gy": at(du, dv)}, device_id_type=MESH
        )
    for other in (ahead, behind, partner):
        pl.semaphore_signal(barrier, inc=1, device_id={"gx": other, "gy": gy}, device_id_type=MESH)
    for load in loads:
        load.start()
    loads[0].wait()
    pl.semaphore_wait(barrier, 7)

    def rows_of(c, h, size):
        return pl.ds(pl.multiple_of(c % 2 * CHUNK + h * HALF, HALF), size)

    def half(c, h):
        return g.at[c // 2, rows_of(c, h, HALF)]

    def whole(c):
        return g.at[c // 2, rows_of(c, 0, CHUNK)]

    def part(ref, n, h):
        return ref.at[n, pl.ds(h * HALF, HALF)]

    def own_half(h):
        return a_ref.at[pl.ds(h * HALF, HALF)]

    def remote(src, dst, send, recv, to_gx, to_gy):
        return pltpu.make_async_remote_copy(
            src_ref=src, dst_ref=dst, send_sem=send, recv_sem=recv,
            device_id={"gx": to_gx, "gy": to_gy}, device_id_type=MESH,
        )

    copies = []

    def start(copy):
        copy.start()
        copies.append(copy)

    me = gy
    a1 = [[
        remote(own_half(h), half(me, h), a1_send.at[d, p], a1_recv.at[d, p], gx, at(1 - 2 * d, 0))
        for p, h in enumerate((d, 1 - d))
    ] for d in (0, 1)]
    a2 = [
        remote(
            half(at(-1 + 2 * d, 0), d), half(at(-1 + 2 * d, 0), d),
            a2_send.at[d], a2_recv.at[d], gx, at(1 - 2 * d, 0),
        )
        for d in (0, 1)
    ]
    offs = (0, -1, 1, 2)
    b1 = [[[
        remote(
            own_half(h) if n == 0 else half(at(du, 0), h), half(at(du, 0), h),
            b1_send.at[n, d, p], b1_recv.at[n, d, p], gx, at(0, 1 - 2 * d),
        )
        for p, h in enumerate((d, 1 - d))
    ] for d in (0, 1)] for n, du in enumerate(offs)]
    b2 = [[
        remote(
            half(at(du, -1 + 2 * d), d), half(at(du, -1 + 2 * d), d),
            b2_send.at[n, d], b2_recv.at[n, d], gx, at(0, 1 - 2 * d),
        )
        for d in (0, 1)
    ] for n, du in enumerate(offs)]

    def along_z(n, src, dst, to):
        return remote(src, dst, z_send.at[n], z_recv.at[n], to, gy)

    z_near = along_z(0, a_ref, rf.at[1], ahead)
    z_far = along_z(1, rf.at[1], rf.at[3], ahead)

    def along_q(n, src, dst, to):
        return remote(src, dst, q_send.at[n], q_recv.at[n], to, gy)

    opposite = at(2, 2)
    q_near = [along_q(h, half(opposite, h), part(qf, 1, h), ahead) for h in (0, 1)]
    q_far = [along_q(2 + h, part(qf, 1, h), part(qf, 3, h), ahead) for h in (0, 1)]

    def to_partner(n, src, dst):
        return remote(src, dst, p_send.at[n], p_recv.at[n], partner, gy)

    p_of = [to_partner(n, a_ref, dst) for n, dst in enumerate((rf.at[0], rf.at[2], qf.at[0], qf.at[2]))]

    for p in (0, 1):
        for d in (0, 1):
            start(a1[d][p])
    for p in (0, 1):
        for d in (0, 1):
            start(b1[0][d][p])
    start(z_near)

    @pl.when(core == 0)
    def _():
        to_partner(0, a_ref, rf.at[0]).start()

    def split(value):
        high = value.astype(jnp.bfloat16)
        return high, (value - high.astype(jnp.float32)).astype(jnp.bfloat16)

    def split_g(c):
        block = c // 2
        rows = rows_of(c, 0, CHUNK)
        high, low = split(g[block, rows, :])
        ghi[block, rows, :] = high
        glo[block, rows, :] = low

    def split_r(n, value):
        high, low = split(value)
        rows_ref[n, :CHUNK] = high
        rows_ref[n, CHUNK:] = low

    for cls, chunk in enumerate((gy, opposite)):
        class_r = chunk // 2
        for e in range(ENTRIES):
            s, col, valid, rowwise, row_tile, col_tile = entry_of(e, gx, class_r)
            owner = owner_smem[row_tile * (row_tile + 1) // 2 + col_tile] % PLANE
            target_tab[cls * ENTRIES + e] = owner if valid is None else jnp.where(valid, owner, -1)
            diag = jnp.where(row_tile == col_tile, 2, 0)
            step = s + STEPS * cls
            entry_tab[cls * ENTRIES + e] = step * 32 + col * 4 + diag + jnp.where(rowwise, 1, 0)

    def served(n, cls):
        du = jnp.int32(0)
        dv = jnp.int32(0)
        for m, (one, two) in enumerate(ORDER):
            du = jnp.where(n == m, one, du)
            dv = jnp.where(n == m, two, dv)
        side = jnp.where((u + 2 * cls) % SIDE < 2, 1, 3)
        return at(du, jnp.where(dv == 9, side, dv))

    def fill(p, carry):
        to = served(p // 2, p % 2)
        base = p % 2 * ENTRIES
        kept = [jnp.int32(0)] * CAP
        for e in range(ENTRIES):
            hit = target_tab[base + e] == to
            fresh = entry_tab[base + e]
            kept = [jnp.where(hit, b, a) for a, b in zip(kept, [fresh] + kept[:-1])]
        for k in range(CAP):
            send_tab[p * CAP + k] = kept[k]
        return carry

    lax.fori_loop(0, PIECES, fill, 0)
    split_r(0, a_ref[...])
    block, rows = me // 2, rows_of(me, 0, CHUNK)
    ghi[block, rows, :] = rows_ref[0, :CHUNK]
    glo[block, rows, :] = rows_ref[0, CHUNK:]

    for load in loads[1:]:
        load.wait()
    mine = owner_ref[...] == gx * PLANE + gy
    slots = table_ref.shape[0]

    def find(q, carry):
        hit = jnp.logical_and(mine, slot_ref[...] == q)
        found = jnp.max(jnp.where(hit, code_ref[...], -1))
        row_tile = jnp.maximum(found, 0) // TILE_COUNT
        col_tile = jnp.maximum(found, 0) % TILE_COUNT
        group_a, inner_i = row_tile // HALF_TILES, row_tile % HALF_TILES
        group_b, inner_j = col_tile // HALF_TILES, col_tile % HALF_TILES
        gap = group_a - group_b
        even = (inner_i + inner_j) % 2 == 0
        across = jnp.logical_or(gap > GROUPS // 2, jnp.logical_and(gap == GROUPS // 2, even))
        within = inner_i - inner_j < HALF_TILES // 2
        rowwise = jnp.logical_or(jnp.logical_and(gap == 0, within), jnp.logical_and(gap > 0, across))
        class_r = jnp.where(rowwise, inner_i, inner_j)
        col = jnp.where(rowwise, inner_j, inner_i)
        s = (gx - jnp.where(rowwise, group_a, group_b) + GROUPS) % GROUPS
        place = s * HALF_TILES + jnp.where(s == 0, (class_r - col + HALF_TILES) % HALF_TILES, col)
        found_tab[q] = jnp.where(found >= 0, class_r * 64 + place, -1)
        table_ref[q] = jnp.where(found >= 0, jnp.where(rowwise, 1, 2), 0) + class_r * 4
        return carry

    def count(q, carry):
        own = found_tab[q]
        later = jnp.int32(0)
        for other in range(slots):
            code = found_tab[other]
            same = jnp.logical_and(code // 64 == own // 64, code > own)
            later = later + jnp.where(same, 1, 0)
        table_ref[q] = table_ref[q] + 32 * jnp.minimum(later, CAP - 1)
        return carry

    def take_v(n):
        for d in (0, 1):
            b1[n][d][1].wait_recv()
            split_g(at(offs[n], -1 + 2 * d))

    def take_far(n):
        for d in (0, 1):
            b2[n][d].wait_recv()
        split_g(at(offs[n], 2))

    for d in (0, 1):
        a1[d][0].wait_recv()
        start(a2[d])
    for d in (0, 1):
        a1[d][1].wait_recv()
    for d in (0, 1):
        start(b1[1][d][0])
    for d in (0, 1):
        a2[d].wait_recv()
        start(b1[3][d][0])
    for d in (0, 1):
        b1[0][d][0].wait_recv()
        start(b2[0][d])
    for d in (0, 1):
        start(b1[2][d][0])
    for d in (0, 1):
        split_g(at(-1 + 2 * d, 0))
    split_g(at(2, 0))
    for d in (0, 1):
        b1[3][d][0].wait_recv()
        start(b2[3][d])
    for d in (0, 1):
        b1[1][d][0].wait_recv()
        start(b2[1][d])
    for n in (3, 1, 2):
        for d in (0, 1):
            start(b1[n][d][1])
    z_near.wait_recv()
    start(z_far)

    @pl.when(core == 0)
    def _():
        to_partner(1, rf.at[1], rf.at[2]).start()

    @pl.when(core == 1)
    def _():
        to_partner(0, rf.at[1], rf.at[0]).start()

    take_v(0)
    split_r(2, rf[1])
    z_far.wait_recv()

    @pl.when(core == 1)
    def _():
        to_partner(1, rf.at[3], rf.at[2]).start()

    split_r(4, rf[3])
    take_far(0)
    for d in (0, 1):
        b2[3][d].wait_recv()
    for h in (0, 1):
        start(q_near[h])

    @pl.when(core == 0)
    def _():
        to_partner(2, whole(opposite), qf.at[0]).start()

    for d in (0, 1):
        b1[2][d][0].wait_recv()
        start(b2[2][d])
    split_g(opposite)
    split_r(STEPS, whole(opposite)[...])
    lax.fori_loop(0, slots, find, 0)
    take_v(1)
    take_v(3)
    p_of[0].wait_recv()
    split_r(1, rf[0])
    p_of[1].wait_recv()
    split_r(3, rf[2])
    lax.fori_loop(0, slots, count, 0)
    take_v(2)
    take_far(1)
    q_near[0].wait_recv()
    start(q_far[0])
    take_far(2)

    row_in = lax.broadcasted_iota(jnp.int32, (CHUNK, TILE), 0)
    col_in = lax.broadcasted_iota(jnp.int32, (CHUNK, TILE), 1)

    def dot(p, q):
        return lax.dot_general(p, q, (((1,), (1,)), ((), ())), preferred_element_type=jnp.float32)

    def one_piece(i, carry):
        away = i < 2 * LEAVING * CAP
        n = jnp.where(away, i % LEAVING, LEAVING)
        k = jnp.where(away, i // LEAVING % CAP, i % CAP)
        p = n * 2 + jnp.where(away, i // (LEAVING * CAP), (i - 2 * LEAVING * CAP) // CAP)
        to = served(p // 2, p % 2)
        chunk = jnp.where(p % 2 == 0, gy, opposite)
        entry = send_tab[p * CAP + k]
        s = entry // 32
        j = entry // 4 % HALF_TILES
        both = dot(rows_ref[s], ghi[j])
        value = both[:CHUNK] + both[CHUNK:] + dot(rows_ref[s, :CHUNK], glo[j])
        upper = row_in + chunk % 2 * CHUNK < col_in
        masked = jnp.logical_and(upper, entry // 2 % 2 > 0)
        value = jnp.where(masked, jnp.float32(0.0), value)
        rowwise = jnp.full((CHUNK, CHUNK), entry % 2, jnp.int32) > 0
        for c in range(2):
            part = value[:, c * CHUNK:(c + 1) * CHUNK]
            outs[p, k, c] = jnp.where(rowwise, part, part.T)

        @pl.when(away)
        def _():
            remote(outs.at[p, k], in_ref.at[chunk, k], x_send, x_recv, gx, to).start()

        return carry

    lax.fori_loop(0, LEAVING, one_piece, 0)
    q_near[1].wait_recv()
    start(q_far[1])

    @pl.when(core == 0)
    def _():
        to_partner(3, qf.at[1], qf.at[2]).start()

    @pl.when(core == 1)
    def _():
        to_partner(2, qf.at[1], qf.at[0]).start()

    split_r(STEPS + 2, qf[1])
    lax.fori_loop(LEAVING, LEAVING * CAP, one_piece, 0)
    for h in (0, 1):
        q_far[h].wait_recv()

    @pl.when(core == 1)
    def _():
        to_partner(3, qf.at[3], qf.at[2]).start()

    split_r(STEPS + 4, qf[3])
    p_of[2].wait_recv()
    split_r(STEPS + 1, qf[0])
    p_of[3].wait_recv()
    split_r(STEPS + 3, qf[2])
    lax.fori_loop(LEAVING * CAP, PIECES * CAP, one_piece, 0)
    local = [
        pltpu.make_async_copy(outs.at[PIECES - 2 + n], in_ref.at[c], l_sem.at[n])
        for n, c in enumerate((gy, opposite))
    ]
    for copy in local:
        copy.start()
    for copy in copies + p_of:
        copy.wait_send()
    for copy in local:
        copy.wait()

    everything = remote(outs.at[pl.ds(0, 2 * LEAVING)], in_ref.at[pl.ds(0, 2 * LEAVING)], x_send, x_recv, ahead, gy)
    everything.wait_send()
    everything.wait_recv()


def exchange(matrix_rows, tile_owner, tile_slot, slots):
    rows, width = matrix_rows.shape
    count = tile_owner.shape[0]
    lower_i, lower_j = np.tril_indices(TILE_COUNT)
    code = jnp.asarray(lower_i * TILE_COUNT + lower_j, jnp.int32)
    smem = pl.BlockSpec(memory_space=pltpu.SMEM)
    hbm = pl.BlockSpec(memory_space=pltpu.HBM)
    dma = pltpu.SemaphoreType.DMA
    return pl.pallas_call(
        exchange_kernel,
        out_shape=(
            jax.ShapeDtypeStruct((PLANE, CAP, 2, CHUNK, CHUNK), jnp.float32),
            jax.ShapeDtypeStruct((slots,), jnp.int32),
        ),
        in_specs=[smem, hbm, hbm, hbm, hbm],
        out_specs=(pl.BlockSpec(memory_space=pltpu.VMEM), smem),
        scratch_shapes=[
            pltpu.VMEM((rows, width), jnp.float32),
            pltpu.VMEM((count,), jnp.int32),
            pltpu.VMEM((count,), jnp.int32),
            pltpu.VMEM((count,), jnp.int32),
            pltpu.VMEM((HALF_TILES, TILE, width), jnp.float32),
            pltpu.VMEM((HALF_TILES, TILE, width), jnp.bfloat16),
            pltpu.VMEM((HALF_TILES, TILE, width), jnp.bfloat16),
            pltpu.VMEM((4, CHUNK, width), jnp.float32),
            pltpu.VMEM((4, CHUNK, width), jnp.float32),
            pltpu.VMEM((2 * STEPS, 2 * CHUNK, width), jnp.bfloat16),
            pltpu.VMEM((PIECES, CAP, 2, CHUNK, CHUNK), jnp.float32),
            pltpu.SMEM((2 * ENTRIES,), jnp.int32),
            pltpu.SMEM((2 * ENTRIES,), jnp.int32),
            pltpu.SMEM((PIECES * CAP,), jnp.int32),
            pltpu.SMEM((slots,), jnp.int32),
            dma((2, 2)), dma((2, 2)), dma((2,)), dma((2,)),
            dma((4, 2, 2)), dma((4, 2, 2)), dma((4, 2)), dma((4, 2)),
            dma((2,)), dma((2,)), dma((4,)), dma((4,)), dma((4,)), dma((4,)),
            dma(()), dma(()), dma((4,)),
        ],
        compiler_params=pltpu.CompilerParams(
            collective_id=0, has_side_effects=True, vmem_limit_bytes=42 * 1024 * 1024
        ),
        name="exchange",
    )(tile_owner, *(pltpu.with_memory_space_constraint(x, pltpu.HBM) for x in (tile_owner, tile_slot, code, matrix_rows)))


def assemble_kernel(table, in_ref, out_ref, blank, out_sem):
    slots = table.shape[0]

    def quarters(q, act):
        entry = table[q]
        across = entry % 4 == 1
        source = entry // 4 % HALF_TILES * 2
        for h in range(2):
            for c in range(2):
                row = pl.multiple_of(jnp.where(across, h, c) * CHUNK, CHUNK)
                col = pl.multiple_of(jnp.where(across, c, h) * CHUNK, CHUNK)
                place = out_ref.at[q, pl.ds(row, CHUNK), pl.ds(col, CHUNK)]
                act(pltpu.make_async_copy(in_ref.at[source + h, entry // 32, c], place, out_sem.at[q, 2 * h + c]))

    def clear(q):
        return pltpu.make_async_copy(blank, out_ref.at[q], out_sem.at[q, 0])

    def put(q, carry):
        present = table[q] % 4 > 0

        @pl.when(present)
        def _():
            quarters(q, lambda copy: copy.start())

        @pl.when(jnp.logical_not(present))
        def _():
            blank[...] = jnp.zeros(blank.shape, jnp.float32)
            clear(q).start()

        return carry

    def finish(q, carry):
        present = table[q] % 4 > 0

        @pl.when(present)
        def _():
            quarters(q, lambda copy: copy.wait())

        @pl.when(jnp.logical_not(present))
        def _():
            clear(q).wait()

        return carry

    lax.fori_loop(0, slots, put, 0)
    lax.fori_loop(0, slots, finish, 0)


def assemble(table, incoming):
    slots = table.shape[0]
    return pl.pallas_call(
        assemble_kernel,
        out_shape=jax.ShapeDtypeStruct((slots, TILE, TILE), jnp.float32),
        in_specs=[pl.BlockSpec(memory_space=pltpu.SMEM), pl.BlockSpec(memory_space=pltpu.VMEM)],
        out_specs=pl.BlockSpec(memory_space=pl.ANY),
        scratch_shapes=[
            pltpu.VMEM((TILE, TILE), jnp.float32),
            pltpu.SemaphoreType.DMA((slots, 4)),
        ],
        compiler_params=pltpu.CompilerParams(vmem_limit_bytes=16 * 1024 * 1024),
        name="assemble",
    )(table, incoming)


def per_device(matrix_rows, tile_owner, tile_slot):
    devices = GROUPS * PLANE
    slots = (tile_owner.shape[0] + devices - 1) // devices
    incoming, table = exchange(matrix_rows, tile_owner, tile_slot, slots)
    return assemble(table, incoming)


def solution(mesh):
    placed = (P(("gx", "gy"), None), P(), P())
    return jax.shard_map(
        per_device,
        mesh=mesh,
        in_specs=placed,
        out_specs=P(("gx", "gy"), None, None),
        check_vma=False,
    )
```

```python
import jax
import jax.numpy as jnp
import numpy as np
from jax import lax
from jax.experimental import pallas as pl
from jax.experimental.pallas import tpu as pltpu
from jax.sharding import PartitionSpec as P

MESH = pl.DeviceIdType.MESH
SIDE = 4
PLANE = SIDE * SIDE
GROUPS = 8
HALF_TILES = 8
STEPS = 5
CAP = 3
CHUNK = 128
HALF = CHUNK // 2
TILE = 256
TILE_COUNT = 64
ENTRIES = 33
ORDER = ((2, 0), (0, 1), (1, 9), (0, 3), (3, 9), (1, 0), (3, 0), (0, 0))
SERVED = len(ORDER)
PIECES = 2 * SERVED
LEAVING = SERVED - 1


def entry_of(e, gx, r):
    quarter = HALF_TILES // 2
    middle = GROUPS // 2 - 1
    if e <= quarter:
        s, col = 0, (r - e + HALF_TILES) % HALF_TILES
        valid = r < quarter if e == quarter else None
        rowwise = col <= r
        source = gx
    elif e <= quarter + middle * HALF_TILES:
        s, col = 1 + (e - quarter - 1) // HALF_TILES, (e - quarter - 1) % HALF_TILES
        valid = None
        source = (gx - s + GROUPS) % GROUPS
        rowwise = source > gx
    else:
        s = middle + 1
        last = e - quarter - 1 - middle * HALF_TILES
        col = 2 * last + (r + jnp.where(gx >= GROUPS // 2, 1, 0)) % 2
        valid = None
        source = (gx - s + GROUPS) % GROUPS
        rowwise = source > gx
    near = source * HALF_TILES + r
    far = gx * HALF_TILES + col
    row_tile = jnp.where(rowwise, near, far)
    col_tile = jnp.where(rowwise, far, near)
    return s, col, valid, rowwise, row_tile, col_tile


def exchange_kernel(
    owner_smem, owner_any, slot_any, code_any, a_any, in_ref, table_ref,
    a_ref, owner_ref, slot_ref, code_ref,
    g, ghi, glo, rf, qf, rows_ref, outs, target_tab, entry_tab, send_tab, found_tab,
    a1_send, a1_recv, a2_send, a2_recv, b1_send, b1_recv, b2_send, b2_recv,
    z_send, z_recv, p_send, p_recv, q_send, q_recv, x_send, x_recv, l_sem,
):
    gx = lax.axis_index("gx")
    gy = lax.axis_index("gy")
    core = gx % 2
    y = gy // SIDE
    x = gy % SIDE
    u = jnp.where(core == 0, x, y)
    v = jnp.where(core == 0, y, x)
    stride_u = jnp.where(core == 0, 1, SIDE)
    stride_v = jnp.where(core == 0, SIDE, 1)

    def at(du, dv):
        return (u + du + SIDE) % SIDE * stride_u + (v + dv + SIDE) % SIDE * stride_v

    ahead = (gx + 2) % GROUPS
    behind = (gx + 6) % GROUPS
    partner = gx + 1 - 2 * core

    loads = [
        pltpu.make_async_copy(src, dst, l_sem.at[n])
        for n, (src, dst) in enumerate(
            ((a_any, a_ref), (owner_any, owner_ref), (slot_any, slot_ref), (code_any, code_ref))
        )
    ]
    barrier = pltpu.get_barrier_semaphore()
    for du, dv in ((1, 0), (3, 0), (0, 1), (0, 3)):
        pl.semaphore_signal(
            barrier, inc=1, device_id={"gx": gx, "gy": at(du, dv)}, device_id_type=MESH
        )
    for other in (ahead, behind, partner):
        pl.semaphore_signal(barrier, inc=1, device_id={"gx": other, "gy": gy}, device_id_type=MESH)
    for load in loads:
        load.start()
    loads[0].wait()
    pl.semaphore_wait(barrier, 7)

    def rows_of(c, h, size):
        return pl.ds(pl.multiple_of(c % 2 * CHUNK + h * HALF, HALF), size)

    def half(c, h):
        return g.at[c // 2, rows_of(c, h, HALF)]

    def whole(c):
        return g.at[c // 2, rows_of(c, 0, CHUNK)]

    def part(ref, n, h):
        return ref.at[n, pl.ds(h * HALF, HALF)]

    def own_half(h):
        return a_ref.at[pl.ds(h * HALF, HALF)]

    def remote(src, dst, send, recv, to_gx, to_gy):
        return pltpu.make_async_remote_copy(
            src_ref=src, dst_ref=dst, send_sem=send, recv_sem=recv,
            device_id={"gx": to_gx, "gy": to_gy}, device_id_type=MESH,
        )

    copies = []

    def start(copy):
        copy.start()
        copies.append(copy)

    me = gy
    a1 = [[
        remote(own_half(h), half(me, h), a1_send.at[d, p], a1_recv.at[d, p], gx, at(1 - 2 * d, 0))
        for p, h in enumerate((d, 1 - d))
    ] for d in (0, 1)]
    a2 = [
        remote(
            half(at(-1 + 2 * d, 0), d), half(at(-1 + 2 * d, 0), d),
            a2_send.at[d], a2_recv.at[d], gx, at(1 - 2 * d, 0),
        )
        for d in (0, 1)
    ]
    offs = (0, -1, 1, 2)
    b1 = [[[
        remote(
            own_half(h) if n == 0 else half(at(du, 0), h), half(at(du, 0), h),
            b1_send.at[n, d, p], b1_recv.at[n, d, p], gx, at(0, 1 - 2 * d),
        )
        for p, h in enumerate((d, 1 - d))
    ] for d in (0, 1)] for n, du in enumerate(offs)]
    b2 = [[
        remote(
            half(at(du, -1 + 2 * d), d), half(at(du, -1 + 2 * d), d),
            b2_send.at[n, d], b2_recv.at[n, d], gx, at(0, 1 - 2 * d),
        )
        for d in (0, 1)
    ] for n, du in enumerate(offs)]

    def along_z(n, src, dst, to):
        return remote(src, dst, z_send.at[n], z_recv.at[n], to, gy)

    z_near = along_z(0, a_ref, rf.at[1], ahead)
    z_far = along_z(1, rf.at[1], rf.at[3], ahead)

    def along_q(n, src, dst, to):
        return remote(src, dst, q_send.at[n], q_recv.at[n], to, gy)

    opposite = at(2, 2)
    q_near = [along_q(h, half(opposite, h), part(qf, 1, h), ahead) for h in (0, 1)]
    q_far = [along_q(2 + h, part(qf, 1, h), part(qf, 3, h), ahead) for h in (0, 1)]

    def to_partner(n, src, dst):
        return remote(src, dst, p_send.at[n], p_recv.at[n], partner, gy)

    p_of = [to_partner(n, a_ref, dst) for n, dst in enumerate((rf.at[0], rf.at[2], qf.at[0], qf.at[2]))]

    for p in (0, 1):
        for d in (0, 1):
            start(a1[d][p])
    for p in (0, 1):
        for d in (0, 1):
            start(b1[0][d][p])
    start(z_near)

    @pl.when(core == 0)
    def _():
        to_partner(0, a_ref, rf.at[0]).start()

    def split(value):
        high = value.astype(jnp.bfloat16)
        return high, (value - high.astype(jnp.float32)).astype(jnp.bfloat16)

    def split_g(c):
        block = c // 2
        rows = rows_of(c, 0, CHUNK)
        high, low = split(g[block, rows, :])
        ghi[block, rows, :] = high
        glo[block, rows, :] = low

    def split_r(n, value):
        high, low = split(value)
        rows_ref[n, :CHUNK] = high
        rows_ref[n, CHUNK:] = low

    for cls, chunk in enumerate((gy, opposite)):
        class_r = chunk // 2
        for e in range(ENTRIES):
            s, col, valid, rowwise, row_tile, col_tile = entry_of(e, gx, class_r)
            owner = owner_smem[row_tile * (row_tile + 1) // 2 + col_tile] % PLANE
            target_tab[cls * ENTRIES + e] = owner if valid is None else jnp.where(valid, owner, -1)
            diag = jnp.where(row_tile == col_tile, 2, 0)
            step = s + STEPS * cls
            entry_tab[cls * ENTRIES + e] = step * 32 + col * 4 + diag + jnp.where(rowwise, 1, 0)

    def served(n, cls):
        du = jnp.int32(0)
        dv = jnp.int32(0)
        for m, (one, two) in enumerate(ORDER):
            du = jnp.where(n == m, one, du)
            dv = jnp.where(n == m, two, dv)
        side = jnp.where((u + 2 * cls) % SIDE < 2, 1, 3)
        return at(du, jnp.where(dv == 9, side, dv))

    def fill(p, carry):
        to = served(p // 2, p % 2)
        base = p % 2 * ENTRIES
        kept = [jnp.int32(0)] * CAP
        for e in range(ENTRIES):
            hit = target_tab[base + e] == to
            fresh = entry_tab[base + e]
            kept = [jnp.where(hit, b, a) for a, b in zip(kept, [fresh] + kept[:-1])]
        for k in range(CAP):
            send_tab[p * CAP + k] = kept[k]
        return carry

    lax.fori_loop(0, PIECES, fill, 0)
    split_r(0, a_ref[...])
    block, rows = me // 2, rows_of(me, 0, CHUNK)
    ghi[block, rows, :] = rows_ref[0, :CHUNK]
    glo[block, rows, :] = rows_ref[0, CHUNK:]

    for load in loads[1:]:
        load.wait()
    mine = owner_ref[...] == gx * PLANE + gy
    slots = table_ref.shape[0]

    def find(q, carry):
        hit = jnp.logical_and(mine, slot_ref[...] == q)
        found = jnp.max(jnp.where(hit, code_ref[...], -1))
        row_tile = jnp.maximum(found, 0) // TILE_COUNT
        col_tile = jnp.maximum(found, 0) % TILE_COUNT
        group_a, inner_i = row_tile // HALF_TILES, row_tile % HALF_TILES
        group_b, inner_j = col_tile // HALF_TILES, col_tile % HALF_TILES
        gap = group_a - group_b
        even = (inner_i + inner_j) % 2 == 0
        across = jnp.logical_or(gap > GROUPS // 2, jnp.logical_and(gap == GROUPS // 2, even))
        within = inner_i - inner_j < HALF_TILES // 2
        rowwise = jnp.logical_or(jnp.logical_and(gap == 0, within), jnp.logical_and(gap > 0, across))
        class_r = jnp.where(rowwise, inner_i, inner_j)
        col = jnp.where(rowwise, inner_j, inner_i)
        s = (gx - jnp.where(rowwise, group_a, group_b) + GROUPS) % GROUPS
        place = s * HALF_TILES + jnp.where(s == 0, (class_r - col + HALF_TILES) % HALF_TILES, col)
        found_tab[q] = jnp.where(found >= 0, class_r * 64 + place, -1)
        table_ref[q] = jnp.where(found >= 0, jnp.where(rowwise, 1, 2), 0) + class_r * 4
        return carry

    def count(q, carry):
        own = found_tab[q]
        later = jnp.int32(0)
        for other in range(slots):
            code = found_tab[other]
            same = jnp.logical_and(code // 64 == own // 64, code > own)
            later = later + jnp.where(same, 1, 0)
        table_ref[q] = table_ref[q] + 32 * jnp.minimum(later, CAP - 1)
        return carry

    def take_v(n):
        for d in (0, 1):
            b1[n][d][1].wait_recv()
            split_g(at(offs[n], -1 + 2 * d))

    def take_far(n):
        for d in (0, 1):
            b2[n][d].wait_recv()
        split_g(at(offs[n], 2))

    for d in (0, 1):
        a1[d][0].wait_recv()
        start(a2[d])
    for d in (0, 1):
        a1[d][1].wait_recv()
    for d in (0, 1):
        start(b1[1][d][0])
    for d in (0, 1):
        a2[d].wait_recv()
        start(b1[3][d][0])
    for d in (0, 1):
        b1[0][d][0].wait_recv()
        start(b2[0][d])
    for d in (0, 1):
        start(b1[2][d][0])
    for d in (0, 1):
        split_g(at(-1 + 2 * d, 0))
    split_g(at(2, 0))
    for d in (0, 1):
        b1[3][d][0].wait_recv()
        start(b2[3][d])
    for d in (0, 1):
        b1[1][d][0].wait_recv()
        start(b2[1][d])
    for n in (3, 1, 2):
        for d in (0, 1):
            start(b1[n][d][1])
    z_near.wait_recv()
    start(z_far)

    @pl.when(core == 0)
    def _():
        to_partner(1, rf.at[1], rf.at[2]).start()

    @pl.when(core == 1)
    def _():
        to_partner(0, rf.at[1], rf.at[0]).start()

    take_v(0)
    split_r(2, rf[1])
    z_far.wait_recv()

    @pl.when(core == 1)
    def _():
        to_partner(1, rf.at[3], rf.at[2]).start()

    split_r(4, rf[3])
    take_far(0)
    for d in (0, 1):
        b2[3][d].wait_recv()
    for h in (0, 1):
        start(q_near[h])

    @pl.when(core == 0)
    def _():
        to_partner(2, whole(opposite), qf.at[0]).start()

    for d in (0, 1):
        b1[2][d][0].wait_recv()
        start(b2[2][d])
    split_g(opposite)
    split_r(STEPS, whole(opposite)[...])
    lax.fori_loop(0, slots, find, 0)
    take_v(1)
    take_v(3)
    p_of[0].wait_recv()
    split_r(1, rf[0])
    p_of[1].wait_recv()
    split_r(3, rf[2])
    lax.fori_loop(0, slots, count, 0)
    take_v(2)
    take_far(1)
    q_near[0].wait_recv()
    start(q_far[0])
    take_far(2)

    row_in = lax.broadcasted_iota(jnp.int32, (CHUNK, TILE), 0)
    col_in = lax.broadcasted_iota(jnp.int32, (CHUNK, TILE), 1)

    def dot(p, q):
        return lax.dot_general(p, q, (((1,), (1,)), ((), ())), preferred_element_type=jnp.float32)

    def one_piece(i, carry):
        away = i < 2 * LEAVING * CAP
        n = jnp.where(away, i % LEAVING, LEAVING)
        k = jnp.where(away, i // LEAVING % CAP, i % CAP)
        p = n * 2 + jnp.where(away, i // (LEAVING * CAP), (i - 2 * LEAVING * CAP) // CAP)
        to = served(p // 2, p % 2)
        chunk = jnp.where(p % 2 == 0, gy, opposite)
        entry = send_tab[p * CAP + k]
        s = entry // 32
        j = entry // 4 % HALF_TILES
        both = dot(rows_ref[s], ghi[j])
        value = both[:CHUNK] + both[CHUNK:] + dot(rows_ref[s, :CHUNK], glo[j])
        upper = row_in + chunk % 2 * CHUNK < col_in
        masked = jnp.logical_and(upper, entry // 2 % 2 > 0)
        value = jnp.where(masked, jnp.float32(0.0), value)
        rowwise = jnp.full((CHUNK, CHUNK), entry % 2, jnp.int32) > 0
        for c in range(2):
            part = value[:, c * CHUNK:(c + 1) * CHUNK]
            outs[p, k, c] = jnp.where(rowwise, part, part.T)

        @pl.when(away)
        def _():
            remote(outs.at[p, k], in_ref.at[chunk, k], x_send, x_recv, gx, to).start()

        return carry

    lax.fori_loop(0, LEAVING, one_piece, 0)
    q_near[1].wait_recv()
    start(q_far[1])

    @pl.when(core == 0)
    def _():
        to_partner(3, qf.at[1], qf.at[2]).start()

    @pl.when(core == 1)
    def _():
        to_partner(2, qf.at[1], qf.at[0]).start()

    split_r(STEPS + 2, qf[1])
    lax.fori_loop(LEAVING, LEAVING * CAP, one_piece, 0)
    for h in (0, 1):
        q_far[h].wait_recv()

    @pl.when(core == 1)
    def _():
        to_partner(3, qf.at[3], qf.at[2]).start()

    split_r(STEPS + 4, qf[3])
    p_of[2].wait_recv()
    split_r(STEPS + 1, qf[0])
    p_of[3].wait_recv()
    split_r(STEPS + 3, qf[2])
    lax.fori_loop(LEAVING * CAP, PIECES * CAP, one_piece, 0)
    local = [
        pltpu.make_async_copy(outs.at[PIECES - 2 + n], in_ref.at[c], l_sem.at[n])
        for n, c in enumerate((gy, opposite))
    ]
    for copy in local:
        copy.start()
    for copy in copies + p_of:
        copy.wait_send()
    for copy in local:
        copy.wait()

    everything = remote(outs.at[pl.ds(0, 2 * LEAVING)], in_ref.at[pl.ds(0, 2 * LEAVING)], x_send, x_recv, ahead, gy)
    everything.wait_send()
    everything.wait_recv()


def exchange(matrix_rows, tile_owner, tile_slot, slots):
    rows, width = matrix_rows.shape
    count = tile_owner.shape[0]
    lower_i, lower_j = np.tril_indices(TILE_COUNT)
    code = jnp.asarray(lower_i * TILE_COUNT + lower_j, jnp.int32)
    smem = pl.BlockSpec(memory_space=pltpu.SMEM)
    hbm = pl.BlockSpec(memory_space=pltpu.HBM)
    dma = pltpu.SemaphoreType.DMA
    return pl.pallas_call(
        exchange_kernel,
        out_shape=(
            jax.ShapeDtypeStruct((PLANE, CAP, 2, CHUNK, CHUNK), jnp.float32),
            jax.ShapeDtypeStruct((slots,), jnp.int32),
        ),
        in_specs=[smem, hbm, hbm, hbm, hbm],
        out_specs=(pl.BlockSpec(memory_space=pltpu.VMEM), smem),
        scratch_shapes=[
            pltpu.VMEM((rows, width), jnp.float32),
            pltpu.VMEM((count,), jnp.int32),
            pltpu.VMEM((count,), jnp.int32),
            pltpu.VMEM((count,), jnp.int32),
            pltpu.VMEM((HALF_TILES, TILE, width), jnp.float32),
            pltpu.VMEM((HALF_TILES, TILE, width), jnp.bfloat16),
            pltpu.VMEM((HALF_TILES, TILE, width), jnp.bfloat16),
            pltpu.VMEM((4, CHUNK, width), jnp.float32),
            pltpu.VMEM((4, CHUNK, width), jnp.float32),
            pltpu.VMEM((2 * STEPS, 2 * CHUNK, width), jnp.bfloat16),
            pltpu.VMEM((PIECES, CAP, 2, CHUNK, CHUNK), jnp.float32),
            pltpu.SMEM((2 * ENTRIES,), jnp.int32),
            pltpu.SMEM((2 * ENTRIES,), jnp.int32),
            pltpu.SMEM((PIECES * CAP,), jnp.int32),
            pltpu.SMEM((slots,), jnp.int32),
            dma((2, 2)), dma((2, 2)), dma((2,)), dma((2,)),
            dma((4, 2, 2)), dma((4, 2, 2)), dma((4, 2)), dma((4, 2)),
            dma((2,)), dma((2,)), dma((4,)), dma((4,)), dma((4,)), dma((4,)),
            dma(()), dma(()), dma((4,)),
        ],
        compiler_params=pltpu.CompilerParams(
            collective_id=0, has_side_effects=True, vmem_limit_bytes=42 * 1024 * 1024
        ),
        name="exchange",
    )(tile_owner, *(pltpu.with_memory_space_constraint(x, pltpu.HBM) for x in (tile_owner, tile_slot, code, matrix_rows)))


def assemble_kernel(table, in_ref, out_ref, blank, out_sem):
    slots = table.shape[0]

    def quarters(q, act):
        entry = table[q]
        across = entry % 4 == 1
        source = entry // 4 % HALF_TILES * 2
        for h in range(2):
            for c in range(2):
                row = pl.multiple_of(jnp.where(across, h, c) * CHUNK, CHUNK)
                col = pl.multiple_of(jnp.where(across, c, h) * CHUNK, CHUNK)
                place = out_ref.at[q, pl.ds(row, CHUNK), pl.ds(col, CHUNK)]
                act(pltpu.make_async_copy(in_ref.at[source + h, entry // 32, c], place, out_sem.at[q, 2 * h + c]), h)

    def clear(q):
        return pltpu.make_async_copy(blank, out_ref.at[q], out_sem.at[q, 0])

    def put(q, carry):
        present = table[q] % 4 > 0

        @pl.when(present)
        def _():
            quarters(q, lambda copy, thread: copy.start(priority=thread))

        @pl.when(jnp.logical_not(present))
        def _():
            blank[...] = jnp.zeros(blank.shape, jnp.float32)
            clear(q).start()

        return carry

    def finish(q, carry):
        present = table[q] % 4 > 0

        @pl.when(present)
        def _():
            quarters(q, lambda copy, thread: copy.wait())

        @pl.when(jnp.logical_not(present))
        def _():
            clear(q).wait()

        return carry

    lax.fori_loop(0, slots, put, 0)
    lax.fori_loop(0, slots, finish, 0)


def assemble(table, incoming):
    slots = table.shape[0]
    return pl.pallas_call(
        assemble_kernel,
        out_shape=jax.ShapeDtypeStruct((slots, TILE, TILE), jnp.float32),
        in_specs=[pl.BlockSpec(memory_space=pltpu.SMEM), pl.BlockSpec(memory_space=pltpu.VMEM)],
        out_specs=pl.BlockSpec(memory_space=pl.ANY),
        scratch_shapes=[
            pltpu.VMEM((TILE, TILE), jnp.float32),
            pltpu.SemaphoreType.DMA((slots, 4)),
        ],
        compiler_params=pltpu.CompilerParams(vmem_limit_bytes=16 * 1024 * 1024),
        name="assemble",
    )(table, incoming)


def per_device(matrix_rows, tile_owner, tile_slot):
    devices = GROUPS * PLANE
    slots = (tile_owner.shape[0] + devices - 1) // devices
    incoming, table = exchange(matrix_rows, tile_owner, tile_slot, slots)
    return assemble(table, incoming)


def solution(mesh):
    placed = (P(("gx", "gy"), None), P(), P())
    return jax.shard_map(
        per_device,
        mesh=mesh,
        in_specs=placed,
        out_specs=P(("gx", "gy"), None, None),
        check_vma=False,
    )
```

```python
import jax
import jax.numpy as jnp
import numpy as np
from jax import lax
from jax.experimental import pallas as pl
from jax.experimental.pallas import tpu as pltpu
from jax.sharding import PartitionSpec as P

MESH = pl.DeviceIdType.MESH
SIDE = 4
PLANE = SIDE * SIDE
GROUPS = 8
HALF_TILES = 8
STEPS = 5
CAP = 3
CHUNK = 128
HALF = CHUNK // 2
TILE = 256
TILE_COUNT = 64
ENTRIES = 33
ORDER = ((2, 0), (0, 1), (1, 9), (0, 3), (3, 9), (1, 0), (3, 0), (0, 0))
SERVED = len(ORDER)
PIECES = 2 * SERVED
LEAVING = SERVED - 1


def entry_of(e, gx, r):
    quarter = HALF_TILES // 2
    middle = GROUPS // 2 - 1
    if e <= quarter:
        s, col = 0, (r - e + HALF_TILES) % HALF_TILES
        valid = r < quarter if e == quarter else None
        rowwise = col <= r
        source = gx
    elif e <= quarter + middle * HALF_TILES:
        s, col = 1 + (e - quarter - 1) // HALF_TILES, (e - quarter - 1) % HALF_TILES
        valid = None
        source = (gx - s + GROUPS) % GROUPS
        rowwise = source > gx
    else:
        s = middle + 1
        last = e - quarter - 1 - middle * HALF_TILES
        col = 2 * last + (r + jnp.where(gx >= GROUPS // 2, 1, 0)) % 2
        valid = None
        source = (gx - s + GROUPS) % GROUPS
        rowwise = source > gx
    near = source * HALF_TILES + r
    far = gx * HALF_TILES + col
    row_tile = jnp.where(rowwise, near, far)
    col_tile = jnp.where(rowwise, far, near)
    return s, col, valid, rowwise, row_tile, col_tile


def exchange_kernel(
    owner_smem, owner_any, slot_any, code_any, a_any, in_ref, table_ref,
    a_ref, owner_ref, slot_ref, code_ref,
    g, ghi, glo, rf, qf, rows_ref, outs, target_tab, entry_tab, send_tab, found_tab,
    a1_send, a1_recv, a2_send, a2_recv, b1_send, b1_recv, b2_send, b2_recv,
    z_send, z_recv, p_send, p_recv, q_send, q_recv, x_send, x_recv, l_sem,
):
    gx = lax.axis_index("gx")
    gy = lax.axis_index("gy")
    core = gx % 2
    y = gy // SIDE
    x = gy % SIDE
    u = jnp.where(core == 0, x, y)
    v = jnp.where(core == 0, y, x)
    stride_u = jnp.where(core == 0, 1, SIDE)
    stride_v = jnp.where(core == 0, SIDE, 1)

    def at(du, dv):
        return (u + du + SIDE) % SIDE * stride_u + (v + dv + SIDE) % SIDE * stride_v

    ahead = (gx + 2) % GROUPS
    behind = (gx + 6) % GROUPS
    partner = gx + 1 - 2 * core

    loads = [
        pltpu.make_async_copy(src, dst, l_sem.at[n])
        for n, (src, dst) in enumerate(
            ((a_any, a_ref), (owner_any, owner_ref), (slot_any, slot_ref), (code_any, code_ref))
        )
    ]
    barrier = pltpu.get_barrier_semaphore()
    for du, dv in ((1, 0), (3, 0), (0, 1), (0, 3)):
        pl.semaphore_signal(
            barrier, inc=1, device_id={"gx": gx, "gy": at(du, dv)}, device_id_type=MESH
        )
    for other in (ahead, behind, partner):
        pl.semaphore_signal(barrier, inc=1, device_id={"gx": other, "gy": gy}, device_id_type=MESH)
    for load in loads:
        load.start()
    loads[0].wait()
    pl.semaphore_wait(barrier, 7)

    def rows_of(c, h, size):
        return pl.ds(pl.multiple_of(c % 2 * CHUNK + h * HALF, HALF), size)

    def half(c, h):
        return g.at[c // 2, rows_of(c, h, HALF)]

    def whole(c):
        return g.at[c // 2, rows_of(c, 0, CHUNK)]

    def part(ref, n, h):
        return ref.at[n, pl.ds(h * HALF, HALF)]

    def own_half(h):
        return a_ref.at[pl.ds(h * HALF, HALF)]

    def remote(src, dst, send, recv, to_gx, to_gy):
        return pltpu.make_async_remote_copy(
            src_ref=src, dst_ref=dst, send_sem=send, recv_sem=recv,
            device_id={"gx": to_gx, "gy": to_gy}, device_id_type=MESH,
        )

    copies = []

    def start(copy):
        copy.start()
        copies.append(copy)

    me = gy
    a1 = [[
        remote(own_half(h), half(me, h), a1_send.at[d, p], a1_recv.at[d, p], gx, at(1 - 2 * d, 0))
        for p, h in enumerate((d, 1 - d))
    ] for d in (0, 1)]
    a2 = [
        remote(
            half(at(-1 + 2 * d, 0), d), half(at(-1 + 2 * d, 0), d),
            a2_send.at[d], a2_recv.at[d], gx, at(1 - 2 * d, 0),
        )
        for d in (0, 1)
    ]
    offs = (0, -1, 1, 2)
    b1 = [[[
        remote(
            own_half(h) if n == 0 else half(at(du, 0), h), half(at(du, 0), h),
            b1_send.at[n, d, p], b1_recv.at[n, d, p], gx, at(0, 1 - 2 * d),
        )
        for p, h in enumerate((d, 1 - d))
    ] for d in (0, 1)] for n, du in enumerate(offs)]
    b2 = [[
        remote(
            half(at(du, -1 + 2 * d), d), half(at(du, -1 + 2 * d), d),
            b2_send.at[n, d], b2_recv.at[n, d], gx, at(0, 1 - 2 * d),
        )
        for d in (0, 1)
    ] for n, du in enumerate(offs)]

    def along_z(n, src, dst, to):
        return remote(src, dst, z_send.at[n], z_recv.at[n], to, gy)

    z_near = along_z(0, a_ref, rf.at[1], ahead)
    z_far = along_z(1, rf.at[1], rf.at[3], ahead)

    def along_q(n, src, dst, to):
        return remote(src, dst, q_send.at[n], q_recv.at[n], to, gy)

    opposite = at(2, 2)
    q_near = [along_q(h, half(opposite, h), part(qf, 1, h), ahead) for h in (0, 1)]
    q_far = [along_q(2 + h, part(qf, 1, h), part(qf, 3, h), ahead) for h in (0, 1)]

    def to_partner(n, src, dst):
        return remote(src, dst, p_send.at[n], p_recv.at[n], partner, gy)

    p_of = [to_partner(n, a_ref, dst) for n, dst in enumerate((rf.at[0], rf.at[2], qf.at[0], qf.at[2]))]

    for p in (0, 1):
        for d in (0, 1):
            start(a1[d][p])
    for p in (0, 1):
        for d in (0, 1):
            start(b1[0][d][p])
    start(z_near)

    @pl.when(core == 0)
    def _():
        to_partner(0, a_ref, rf.at[0]).start()

    def split(value):
        high = value.astype(jnp.bfloat16)
        return high, (value - high.astype(jnp.float32)).astype(jnp.bfloat16)

    def split_g(c):
        block = c // 2
        rows = rows_of(c, 0, CHUNK)
        high, low = split(g[block, rows, :])
        ghi[block, rows, :] = high
        glo[block, rows, :] = low

    def split_r(n, value):
        high, low = split(value)
        rows_ref[n, :CHUNK] = high
        rows_ref[n, CHUNK:] = low

    for cls, chunk in enumerate((gy, opposite)):
        class_r = chunk // 2
        for e in range(ENTRIES):
            s, col, valid, rowwise, row_tile, col_tile = entry_of(e, gx, class_r)
            owner = owner_smem[row_tile * (row_tile + 1) // 2 + col_tile] % PLANE
            target_tab[cls * ENTRIES + e] = owner if valid is None else jnp.where(valid, owner, -1)
            diag = jnp.where(row_tile == col_tile, 2, 0)
            step = s + STEPS * cls
            entry_tab[cls * ENTRIES + e] = step * 32 + col * 4 + diag + jnp.where(rowwise, 1, 0)

    def served(n, cls):
        du = jnp.int32(0)
        dv = jnp.int32(0)
        for m, (one, two) in enumerate(ORDER):
            du = jnp.where(n == m, one, du)
            dv = jnp.where(n == m, two, dv)
        side = jnp.where((u + 2 * cls) % SIDE < 2, 1, 3)
        return at(du, jnp.where(dv == 9, side, dv))

    def fill(p, carry):
        to = served(p // 2, p % 2)
        base = p % 2 * ENTRIES
        kept = [jnp.int32(0)] * CAP
        for e in range(ENTRIES):
            hit = target_tab[base + e] == to
            fresh = entry_tab[base + e]
            kept = [jnp.where(hit, b, a) for a, b in zip(kept, [fresh] + kept[:-1])]
        for k in range(CAP):
            send_tab[p * CAP + k] = kept[k]
        return carry

    lax.fori_loop(0, PIECES, fill, 0)
    split_r(0, a_ref[...])
    block, rows = me // 2, rows_of(me, 0, CHUNK)
    ghi[block, rows, :] = rows_ref[0, :CHUNK]
    glo[block, rows, :] = rows_ref[0, CHUNK:]

    for load in loads[1:]:
        load.wait()
    mine = owner_ref[...] == gx * PLANE + gy
    slots = table_ref.shape[0]

    def find(q, carry):
        hit = jnp.logical_and(mine, slot_ref[...] == q)
        found = jnp.max(jnp.where(hit, code_ref[...], -1))
        row_tile = jnp.maximum(found, 0) // TILE_COUNT
        col_tile = jnp.maximum(found, 0) % TILE_COUNT
        group_a, inner_i = row_tile // HALF_TILES, row_tile % HALF_TILES
        group_b, inner_j = col_tile // HALF_TILES, col_tile % HALF_TILES
        gap = group_a - group_b
        even = (inner_i + inner_j) % 2 == 0
        across = jnp.logical_or(gap > GROUPS // 2, jnp.logical_and(gap == GROUPS // 2, even))
        within = inner_i - inner_j < HALF_TILES // 2
        rowwise = jnp.logical_or(jnp.logical_and(gap == 0, within), jnp.logical_and(gap > 0, across))
        class_r = jnp.where(rowwise, inner_i, inner_j)
        col = jnp.where(rowwise, inner_j, inner_i)
        s = (gx - jnp.where(rowwise, group_a, group_b) + GROUPS) % GROUPS
        place = s * HALF_TILES + jnp.where(s == 0, (class_r - col + HALF_TILES) % HALF_TILES, col)
        found_tab[q] = jnp.where(found >= 0, class_r * 64 + place, -1)
        table_ref[q] = jnp.where(found >= 0, jnp.where(rowwise, 1, 2), 0) + class_r * 4
        return carry

    def count(q, carry):
        own = found_tab[q]
        later = jnp.int32(0)
        for other in range(slots):
            code = found_tab[other]
            same = jnp.logical_and(code // 64 == own // 64, code > own)
            later = later + jnp.where(same, 1, 0)
        table_ref[q] = table_ref[q] + 32 * jnp.minimum(later, CAP - 1)
        return carry

    def take_v(n):
        for d in (0, 1):
            b1[n][d][1].wait_recv()
            split_g(at(offs[n], -1 + 2 * d))

    def take_far(n):
        for d in (0, 1):
            b2[n][d].wait_recv()
        split_g(at(offs[n], 2))

    for d in (0, 1):
        a1[d][0].wait_recv()
        start(a2[d])
    for d in (0, 1):
        a1[d][1].wait_recv()
    for d in (0, 1):
        start(b1[1][d][0])
    for d in (0, 1):
        a2[d].wait_recv()
        start(b1[3][d][0])
    for d in (0, 1):
        b1[0][d][0].wait_recv()
        start(b2[0][d])
    for d in (0, 1):
        start(b1[2][d][0])
    for d in (0, 1):
        split_g(at(-1 + 2 * d, 0))
    split_g(at(2, 0))
    for d in (0, 1):
        b1[3][d][0].wait_recv()
        start(b2[3][d])
    for d in (0, 1):
        b1[1][d][0].wait_recv()
        start(b2[1][d])
    for n in (3, 1, 2):
        for d in (0, 1):
            start(b1[n][d][1])
    z_near.wait_recv()
    start(z_far)

    @pl.when(core == 0)
    def _():
        to_partner(1, rf.at[1], rf.at[2]).start()

    @pl.when(core == 1)
    def _():
        to_partner(0, rf.at[1], rf.at[0]).start()

    take_v(0)
    split_r(2, rf[1])
    z_far.wait_recv()

    @pl.when(core == 1)
    def _():
        to_partner(1, rf.at[3], rf.at[2]).start()

    split_r(4, rf[3])
    take_far(0)
    for d in (0, 1):
        b2[3][d].wait_recv()
    for h in (0, 1):
        start(q_near[h])

    @pl.when(core == 0)
    def _():
        to_partner(2, whole(opposite), qf.at[0]).start()

    for d in (0, 1):
        b1[2][d][0].wait_recv()
        start(b2[2][d])
    split_g(opposite)
    split_r(STEPS, whole(opposite)[...])
    lax.fori_loop(0, slots, find, 0)
    take_v(1)
    take_v(3)
    p_of[0].wait_recv()
    split_r(1, rf[0])
    p_of[1].wait_recv()
    split_r(3, rf[2])
    lax.fori_loop(0, slots, count, 0)
    take_v(2)
    take_far(1)
    q_near[0].wait_recv()
    start(q_far[0])
    take_far(2)

    row_in = lax.broadcasted_iota(jnp.int32, (CHUNK, TILE), 0)
    col_in = lax.broadcasted_iota(jnp.int32, (CHUNK, TILE), 1)

    def dot(p, q):
        return lax.dot_general(p, q, (((1,), (1,)), ((), ())), preferred_element_type=jnp.float32)

    def one_piece(i, carry):
        away = i < 2 * LEAVING * CAP
        n = jnp.where(away, i % LEAVING, LEAVING)
        k = jnp.where(away, i // LEAVING % CAP, i % CAP)
        p = n * 2 + jnp.where(away, i // (LEAVING * CAP), (i - 2 * LEAVING * CAP) // CAP)
        to = served(p // 2, p % 2)
        chunk = jnp.where(p % 2 == 0, gy, opposite)
        entry = send_tab[p * CAP + k]
        s = entry // 32
        j = entry // 4 % HALF_TILES
        both = dot(rows_ref[s], ghi[j])
        value = both[:CHUNK] + both[CHUNK:] + dot(rows_ref[s, :CHUNK], glo[j])
        upper = row_in + chunk % 2 * CHUNK < col_in
        masked = jnp.logical_and(upper, entry // 2 % 2 > 0)
        value = jnp.where(masked, jnp.float32(0.0), value)
        rowwise = jnp.full((CHUNK, CHUNK), entry % 2, jnp.int32) > 0
        for c in range(2):
            part = value[:, c * CHUNK:(c + 1) * CHUNK]
            outs[p, k, c] = jnp.where(rowwise, part, part.T)

        @pl.when(away)
        def _():
            remote(outs.at[p, k], in_ref.at[chunk, k], x_send, x_recv, gx, to).start()

        return carry

    lax.fori_loop(0, LEAVING, one_piece, 0)
    q_near[1].wait_recv()
    start(q_far[1])

    @pl.when(core == 0)
    def _():
        to_partner(3, qf.at[1], qf.at[2]).start()

    @pl.when(core == 1)
    def _():
        to_partner(2, qf.at[1], qf.at[0]).start()

    split_r(STEPS + 2, qf[1])
    lax.fori_loop(LEAVING, LEAVING * CAP, one_piece, 0)
    for h in (0, 1):
        q_far[h].wait_recv()

    @pl.when(core == 1)
    def _():
        to_partner(3, qf.at[3], qf.at[2]).start()

    split_r(STEPS + 4, qf[3])
    p_of[2].wait_recv()
    split_r(STEPS + 1, qf[0])
    p_of[3].wait_recv()
    split_r(STEPS + 3, qf[2])
    lax.fori_loop(LEAVING * CAP, PIECES * CAP, one_piece, 0)
    local = [
        pltpu.make_async_copy(outs.at[PIECES - 2 + n], in_ref.at[c], l_sem.at[n])
        for n, c in enumerate((gy, opposite))
    ]
    for copy in local:
        copy.start()
    for copy in copies + p_of:
        copy.wait_send()
    for copy in local:
        copy.wait()

    everything = remote(outs.at[pl.ds(0, 2 * LEAVING)], in_ref.at[pl.ds(0, 2 * LEAVING)], x_send, x_recv, ahead, gy)
    everything.wait_send()
    everything.wait_recv()


def exchange(matrix_rows, tile_owner, tile_slot, slots):
    rows, width = matrix_rows.shape
    count = tile_owner.shape[0]
    lower_i, lower_j = np.tril_indices(TILE_COUNT)
    code = jnp.asarray(lower_i * TILE_COUNT + lower_j, jnp.int32)
    smem = pl.BlockSpec(memory_space=pltpu.SMEM)
    hbm = pl.BlockSpec(memory_space=pltpu.HBM)
    dma = pltpu.SemaphoreType.DMA
    return pl.pallas_call(
        exchange_kernel,
        out_shape=(
            jax.ShapeDtypeStruct((PLANE, CAP, 2, CHUNK, CHUNK), jnp.float32),
            jax.ShapeDtypeStruct((slots,), jnp.int32),
        ),
        in_specs=[smem, hbm, hbm, hbm, hbm],
        out_specs=(pl.BlockSpec(memory_space=pltpu.VMEM), smem),
        scratch_shapes=[
            pltpu.VMEM((rows, width), jnp.float32),
            pltpu.VMEM((count,), jnp.int32),
            pltpu.VMEM((count,), jnp.int32),
            pltpu.VMEM((count,), jnp.int32),
            pltpu.VMEM((HALF_TILES, TILE, width), jnp.float32),
            pltpu.VMEM((HALF_TILES, TILE, width), jnp.bfloat16),
            pltpu.VMEM((HALF_TILES, TILE, width), jnp.bfloat16),
            pltpu.VMEM((4, CHUNK, width), jnp.float32),
            pltpu.VMEM((4, CHUNK, width), jnp.float32),
            pltpu.VMEM((2 * STEPS, 2 * CHUNK, width), jnp.bfloat16),
            pltpu.VMEM((PIECES, CAP, 2, CHUNK, CHUNK), jnp.float32),
            pltpu.SMEM((2 * ENTRIES,), jnp.int32),
            pltpu.SMEM((2 * ENTRIES,), jnp.int32),
            pltpu.SMEM((PIECES * CAP,), jnp.int32),
            pltpu.SMEM((slots,), jnp.int32),
            dma((2, 2)), dma((2, 2)), dma((2,)), dma((2,)),
            dma((4, 2, 2)), dma((4, 2, 2)), dma((4, 2)), dma((4, 2)),
            dma((2,)), dma((2,)), dma((4,)), dma((4,)), dma((4,)), dma((4,)),
            dma(()), dma(()), dma((4,)),
        ],
        compiler_params=pltpu.CompilerParams(
            collective_id=0, has_side_effects=True, vmem_limit_bytes=42 * 1024 * 1024
        ),
        name="exchange",
    )(tile_owner, *(pltpu.with_memory_space_constraint(x, pltpu.HBM) for x in (tile_owner, tile_slot, code, matrix_rows)))


def assemble_kernel(table, in_ref, out_ref, blank, out_sem):
    slots = table.shape[0]

    def quarters(q, act):
        entry = table[q]
        across = entry % 4 == 1
        source = entry // 4 % HALF_TILES * 2
        for h in range(2):
            for c in range(2):
                row = pl.multiple_of(jnp.where(across, h, c) * CHUNK, CHUNK)
                col = pl.multiple_of(jnp.where(across, c, h) * CHUNK, CHUNK)
                place = out_ref.at[q, pl.ds(row, CHUNK), pl.ds(col, CHUNK)]
                act(pltpu.make_async_copy(in_ref.at[source + h, entry // 32, c], place, out_sem))

    def clear(q):
        return pltpu.make_async_copy(blank, out_ref.at[q], out_sem)

    def put(q, carry):
        present = table[q] % 4 > 0

        @pl.when(present)
        def _():
            quarters(q, lambda copy: copy.start())

        @pl.when(jnp.logical_not(present))
        def _():
            blank[...] = jnp.zeros(blank.shape, jnp.float32)
            clear(q).start()

        return carry

    lax.fori_loop(0, slots, put, 0)
    pltpu.make_async_copy(out_ref, out_ref, out_sem).wait()


def assemble(table, incoming):
    slots = table.shape[0]
    return pl.pallas_call(
        assemble_kernel,
        out_shape=jax.ShapeDtypeStruct((slots, TILE, TILE), jnp.float32),
        in_specs=[pl.BlockSpec(memory_space=pltpu.SMEM), pl.BlockSpec(memory_space=pltpu.VMEM)],
        out_specs=pl.BlockSpec(memory_space=pl.ANY),
        scratch_shapes=[
            pltpu.VMEM((TILE, TILE), jnp.float32),
            pltpu.SemaphoreType.DMA(()),
        ],
        compiler_params=pltpu.CompilerParams(vmem_limit_bytes=16 * 1024 * 1024),
        name="assemble",
    )(table, incoming)


def per_device(matrix_rows, tile_owner, tile_slot):
    devices = GROUPS * PLANE
    slots = (tile_owner.shape[0] + devices - 1) // devices
    incoming, table = exchange(matrix_rows, tile_owner, tile_slot, slots)
    return assemble(table, incoming)


def solution(mesh):
    placed = (P(("gx", "gy"), None), P(), P())
    return jax.shard_map(
        per_device,
        mesh=mesh,
        in_specs=placed,
        out_specs=P(("gx", "gy"), None, None),
        check_vma=False,
    )
```
